16 devices in a mesh: sp: 16 (over z, y, x, core).
Axes of the slice: x: 2, y: 2, z: 2, core: 2. Of those that a mesh axis runs over, the one named last changes fastest.
Arguments:
- x: bfloat16 [4, 2048, 1024], P(None, 'sp')
- d_y: bfloat16 [4, 2048, 1024], P(None, 'sp')
- ln_gamma: bfloat16 [1024], replicated
- ln_beta: bfloat16 [1024], replicated
- w_qkv: bfloat16 [1024, 3072], replicated
- b_qkv: bfloat16 [3072], replicated
- w_out: bfloat16 [1024, 1024], replicated
- b_out: bfloat16 [1024], replicated
- head_kind: int32 [16], replicated
Outputs:
- output 1: bfloat16 [4, 2048, 1024], P(None, 'sp')
- output 2: bfloat16 [4, 2048, 1024], P(None, 'sp')
- output 3: float32 [1024], replicated
- output 4: float32 [1024], replicated
- output 5: float32 [1024, 3072], replicated
- output 6: float32 [3072], replicated
- output 7: float32 [1024, 1024], replicated
- output 8: float32 [1024], replicated
All inputs are finite; a program needn't handle non-finite values.
Results may differ from the reference program's by a relative error of at most 0.0134294.
Values are sent between devices in bfloat16 or wider.
A program may use at most 1 GiB of HBM per device.

```python
import math
import jax
import jax.numpy as jnp
from jax import lax

BATCH_SIZE = 4
SEQ_LEN = 2048
D_MODEL = 1024
NUM_HEADS = 16
HEAD_DIM = D_MODEL // NUM_HEADS
BAND_WIDTH = SEQ_LEN // 4
QUERY_BLOCK = min(128, SEQ_LEN)
SCORE_SCALE = 1.0 / math.sqrt(HEAD_DIM)
LN_EPS = 1e-5
NEG_BIG = -1e30


def setup_inputs(seed: int = 0) -> dict:
    key_list = jax.random.split(jax.random.key(seed), 9)
    tok_shape = (BATCH_SIZE, SEQ_LEN, D_MODEL)
    w_scale = 1.0 / math.sqrt(D_MODEL)
    qkv_gain = jnp.array([1.7, 1.7, 1.0], jnp.float32)
    x_val = jax.random.normal(key_list[0], tok_shape, jnp.float32)
    dy_val = jax.random.normal(key_list[1], tok_shape, jnp.float32)
    gamma_val = 1.0 + 0.3 * jax.random.normal(key_list[2], (D_MODEL,), jnp.float32)
    beta_val = 0.3 * jax.random.normal(key_list[3], (D_MODEL,), jnp.float32)
    wqkv_val = jax.random.normal(key_list[4], (D_MODEL, 3, D_MODEL), jnp.float32) * qkv_gain[None, :, None] * w_scale
    bqkv_val = 0.5 * jax.random.normal(key_list[5], (3 * D_MODEL,), jnp.float32)
    wout_val = jax.random.normal(key_list[6], (D_MODEL, D_MODEL), jnp.float32) * w_scale
    bout_val = 0.5 * jax.random.normal(key_list[7], (D_MODEL,), jnp.float32)
    kind_val = (jax.random.permutation(key_list[8], NUM_HEADS) < NUM_HEADS // 2).astype(jnp.int32)
    return {
        "x": x_val.astype(jnp.bfloat16),
        "d_y": dy_val.astype(jnp.bfloat16),
        "ln_gamma": gamma_val.astype(jnp.bfloat16),
        "ln_beta": beta_val.astype(jnp.bfloat16),
        "w_qkv": wqkv_val.reshape(D_MODEL, 3 * D_MODEL).astype(jnp.bfloat16),
        "b_qkv": bqkv_val.astype(jnp.bfloat16),
        "w_out": wout_val.astype(jnp.bfloat16),
        "b_out": bout_val.astype(jnp.bfloat16),
        "head_kind": kind_val,
    }


def bf16_cast(values):
    return values.astype(jnp.bfloat16).astype(jnp.float32)


def layer_norm(x_rows, gamma_f, beta_f):
    row_mean = jnp.mean(x_rows, axis=-1, keepdims=True)
    centred = x_rows - row_mean
    row_var = jnp.mean(centred * centred, axis=-1, keepdims=True)
    return centred * lax.rsqrt(row_var + LN_EPS) * gamma_f + beta_f


def head_attention(q_head, k_head, v_head, banded):
    key_pos = jnp.arange(SEQ_LEN)[None, :]

    def query_block(q_start):
        q_part = lax.dynamic_slice_in_dim(q_head, q_start, QUERY_BLOCK, axis=1)
        logits = jnp.einsum("bqd,bkd->bqk", q_part, k_head) * SCORE_SCALE
        query_pos = q_start + jnp.arange(QUERY_BLOCK)[:, None]
        allowed = (key_pos <= query_pos) & ((banded == 0) | (key_pos > query_pos - BAND_WIDTH))
        attn_prob = jax.nn.softmax(jnp.where(allowed[None], logits, NEG_BIG), axis=-1)
        return bf16_cast(jnp.einsum("bqk,bkd->bqd", bf16_cast(attn_prob), v_head))

    return lax.map(jax.checkpoint(query_block), jnp.arange(SEQ_LEN // QUERY_BLOCK) * QUERY_BLOCK)


def block_forward(x_f, gamma_f, beta_f, wqkv_f, bqkv_f, wout_f, bout_f, head_kind):
    h_norm = bf16_cast(layer_norm(x_f, gamma_f, beta_f))
    qkv_tok = bf16_cast(jnp.dot(h_norm, wqkv_f, preferred_element_type=jnp.float32) + bqkv_f)
    qkv_head = jnp.transpose(qkv_tok.reshape(BATCH_SIZE, SEQ_LEN, 3, NUM_HEADS, HEAD_DIM), (2, 3, 0, 1, 4))

    def one_head(head_items):
        return head_attention(head_items[0], head_items[1], head_items[2], head_items[3])

    attn_heads = lax.map(one_head, (qkv_head[0], qkv_head[1], qkv_head[2], head_kind))
    attn_tok = jnp.transpose(attn_heads, (2, 1, 3, 0, 4)).reshape(BATCH_SIZE, SEQ_LEN, D_MODEL)
    return x_f + jnp.dot(attn_tok, wout_f, preferred_element_type=jnp.float32) + bout_f


def reference(x, d_y, ln_gamma, ln_beta, w_qkv, b_qkv, w_out, b_out, head_kind):
    def block_fn(x_f, gamma_f, beta_f, wqkv_f, bqkv_f, wout_f, bout_f):
        return block_forward(x_f, gamma_f, beta_f, wqkv_f, bqkv_f, wout_f, bout_f, head_kind)

    primal_list = [item_arr.astype(jnp.float32) for item_arr in (x, ln_gamma, ln_beta, w_qkv, b_qkv, w_out, b_out)]
    y_full, pull_back = jax.vjp(block_fn, *primal_list)
    grad_list = pull_back(d_y.astype(jnp.float32))
    return (y_full.astype(jnp.bfloat16), grad_list[0].astype(jnp.bfloat16), grad_list[1], grad_list[2], grad_list[3], grad_list[4], grad_list[5], grad_list[6])
```

```python
import functools
import math

import jax
import jax.numpy as jnp
from jax import lax
from jax.experimental import pallas as pl
from jax.experimental.pallas import tpu as pltpu
from jax.sharding import PartitionSpec as P

LN_EPS = 1e-5
NEG_BIG = -1e30
BF = jnp.bfloat16
F32 = jnp.float32
QB = 256
L = 128
W3 = 384
T = 512
D = 1024
DR = 1032
S = 2048
D3 = 3072
VMEM_CAP = 60 * D * D


def dot_nn(a, b):
    return lax.dot_general(a, b, (((1,), (0,)), ((), ())), preferred_element_type=F32)


def dot_nt(a, b):
    return lax.dot_general(a, b, (((1,), (1,)), ((), ())), preferred_element_type=F32)


def dot_tn(a, b):
    return lax.dot_general(a, b, (((0,), (0,)), ((), ())), preferred_element_type=F32)


def swap_halves(a):
    return jnp.concatenate([a[:, 64:], a[:, :64]], axis=1)


def pair_halves(a, a_half, b, b_half):
    lane = lax.broadcasted_iota(jnp.int32, a.shape, 1)
    a = jnp.where(a_half == 1, swap_halves(a), a)
    b = jnp.where(b_half == 0, swap_halves(b), b)
    return jnp.where(lane < 64, a, b)


def pre_kernel(perm_ref, x_ref, dy_ref, gamma_ref, beta_ref, wout_ref, h_ref, do_ref, wp_ref):
    for c in range(8):
        wp_ref[c * L:c * L + 64] = wout_ref[perm_ref[c]]
        wp_ref[c * L + 64:c * L + L] = wout_ref[perm_ref[8 + c]]
    gamma = gamma_ref[...].astype(F32)
    beta = beta_ref[...].astype(F32)
    for b in range(4):
        xf = x_ref[b].astype(F32)
        cen = xf - jnp.mean(xf, axis=-1, keepdims=True)
        var = jnp.mean(cen * cen, axis=-1, keepdims=True)
        h_ref[b] = (cen * lax.rsqrt(var + LN_EPS) * gamma + beta).astype(BF)
    dy = dy_ref[...].reshape(T, D)
    for c in range(4):
        d = dot_nt(dy, wp_ref[c * QB:(c + 1) * QB]).astype(BF)
        for u in range(2):
            do_ref[2 * c + u] = d[:, u * L:(u + 1) * L].reshape(4, L, L)


def pre_call(perm, x, dy, gamma, beta, wout):
    vm = pl.BlockSpec(memory_space=pltpu.VMEM)
    return pl.pallas_call(
        pre_kernel,
        out_shape=(jax.ShapeDtypeStruct((4, L, D), BF), jax.ShapeDtypeStruct((8, 4, L, L), BF)),
        in_specs=[pl.BlockSpec(memory_space=pltpu.SMEM)] + [vm] * 5,
        out_specs=(vm, vm),
        scratch_shapes=[pltpu.VMEM((D, D), BF)],
        compiler_params=pltpu.CompilerParams(vmem_limit_bytes=VMEM_CAP),
        cost_estimate=pl.CostEstimate(flops=2 * T * D * D, bytes_accessed=8 << 20, transcendentals=0),
        name="pre",
    )(perm, x, dy, gamma, beta, wout)


def attn_kernel(sel_ref, hg_ref, dog_ref, *refs):
    w_refs, bias_refs = refs[:6], refs[6:12]
    send_ref, dwp_ref = refs[12:14]
    w_ref, bias_ref, qkv_ref, dqkv_ref, qt_ref, dot_ref, dkt_ref, dvt_ref = refs[14:22]
    scr = (refs[22:25], refs[25:28])
    b = pl.program_id(0)
    f_half, g_half = sel_ref[1], sel_ref[3]

    @pl.when(b == 0)
    def _():
        for t in range(3):
            w_ref[:, t * L:(t + 1) * L] = pair_halves(w_refs[2 * t][...], f_half, w_refs[2 * t + 1][...], g_half)
            bf = bias_refs[2 * t][0].astype(F32)
            bg = bias_refs[2 * t + 1][0].astype(F32)
            bias_ref[:, t * L:(t + 1) * L] = pair_halves(bf, f_half, bg, g_half)
        dwp_ref[...] = jnp.zeros_like(dwp_ref)

    def qkv_step(r, carry):
        rows = hg_ref[pl.ds(2 * r, 2), 0].reshape(T, D)
        out = dot_nn(rows, w_ref[...]) + bias_ref[0:1, :]
        qkv_ref[pl.ds(pl.multiple_of(r * T, T), T), :] = out.astype(BF)
        return carry

    lax.fori_loop(0, 4, qkv_step, 0)
    for i in range(8):
        qs = qkv_ref[i * QB:(i + 1) * QB, 0:L] * BF(0.125)
        qt_ref[:, i * QB:(i + 1) * QB] = qs.T
        do = dog_ref[2 * i:2 * i + 2, 0].reshape(QB, L)
        dot_ref[:, i * QB:(i + 1) * QB] = do.T
    dkt_ref[...] = jnp.zeros_like(dkt_ref)
    dvt_ref[...] = jnp.zeros_like(dvt_ref)
    lane = lax.broadcasted_iota(jnp.int32, (QB, L), 1)
    row_i = lax.broadcasted_iota(jnp.int32, (QB, QB), 0)
    col_i = lax.broadcasted_iota(jnp.int32, (QB, QB), 1)

    def head_block(i, hd):
        s_ref, p_ref, ds_ref = scr[hd]
        first = 0 if hd == 0 else max(0, i - 2)
        blocks = range(first, i + 1)
        mine = (lane < 64) if hd == 0 else (lane >= 64)
        qi = qkv_ref[i * QB:(i + 1) * QB, 0:L] * BF(0.125)
        doi = dog_ref[2 * i:2 * i + 2, 0].reshape(QB, L)
        qm = jnp.where(mine, qi, BF(0))
        dom = jnp.where(mine, doi, BF(0))
        mx = None
        for kb in blocks:
            s = dot_nt(qm, qkv_ref[kb * QB:(kb + 1) * QB, L:QB])
            if kb == i:
                s = jnp.where(col_i <= row_i, s, NEG_BIG)
            if hd == 1 and kb == i - 2:
                s = jnp.where(col_i > row_i, s, NEG_BIG)
            s_ref[:, (kb - first) * QB:(kb - first + 1) * QB] = s
            cur = jnp.maximum(s[:, :L], s[:, L:])
            mx = cur if mx is None else jnp.maximum(mx, cur)
        m = jnp.max(mx, axis=1, keepdims=True)
        ls = None
        for kb in blocks:
            o_ = (kb - first) * QB
            e = jnp.exp(s_ref[:, o_:o_ + QB] - m)
            s_ref[:, o_:o_ + QB] = e
            cur = e[:, :L] + e[:, L:]
            ls = cur if ls is None else ls + cur
        rl = 1.0 / jnp.sum(ls, axis=1, keepdims=True)
        acc = None
        for kb in blocks:
            o_ = (kb - first) * QB
            p_ = s_ref[:, o_:o_ + QB] * rl
            s_ref[:, o_:o_ + QB] = p_
            pb = p_.astype(BF)
            p_ref[:, o_:o_ + QB] = pb
            cur = dot_nn(pb, qkv_ref[kb * QB:(kb + 1) * QB, QB:W3])
            acc = cur if acc is None else acc + cur
        dsum = jnp.sum(dom.astype(F32) * acc, axis=1, keepdims=True)
        dq = None
        for kb in blocks:
            o_ = (kb - first) * QB
            dp = dot_nt(dom, qkv_ref[kb * QB:(kb + 1) * QB, QB:W3]).astype(BF).astype(F32)
            ds = (s_ref[:, o_:o_ + QB] * (dp - dsum)).astype(BF)
            ds_ref[:, o_:o_ + QB] = ds
            cur = dot_nn(ds, qkv_ref[kb * QB:(kb + 1) * QB, L:QB])
            dq = cur if dq is None else dq + cur
        hr = slice(hd * 64, hd * 64 + 64)
        n = len(blocks) * QB
        dotb = dot_ref[hr, i * QB:(i + 1) * QB]
        qtb = qt_ref[hr, i * QB:(i + 1) * QB]
        dvt_ref[hr, first * QB:first * QB + n] += dot_nn(dotb, p_ref[:, :n])
        dkt_ref[hr, first * QB:first * QB + n] += dot_nn(qtb, ds_ref[:, :n])
        return acc, dq * 0.125

    for i in range(8):
        of, dqf = head_block(i, 0)
        og, dqg = head_block(i, 1)
        o = jnp.where(lane < 64, of, og).astype(BF)
        dq = jnp.where(lane < 64, dqf, dqg).astype(BF)
        for u in range(2):
            send_ref[2 * i + u, 0, 0] = o[u * L:(u + 1) * L]
            send_ref[2 * i + u, 0, 1] = dq[u * L:(u + 1) * L]
        dqkv_ref[i * QB:(i + 1) * QB, 0:L] = dq

    for t, src in ((1, dkt_ref), (2, dvt_ref)):
        for j in range(16):
            d = src[:, j * L:(j + 1) * L].T.astype(BF)
            send_ref[j, 0, 1 + t] = d
            dqkv_ref[j * L:(j + 1) * L, t * L:(t + 1) * L] = d

    def dw_step(r, carry):
        cols = pl.ds(pl.multiple_of(r * QB, QB), QB)
        hc = hg_ref[:, 0, :, cols].reshape(S, QB)
        dwp_ref[cols, :] += dot_tn(hc, dqkv_ref[...])
        return carry

    lax.fori_loop(0, 4, dw_step, 0)
    dwp_ref[D:1025, :] += jnp.sum(dqkv_ref[...].astype(F32), axis=0, keepdims=True)


def attn_call(sel, hg, dog, w_qkv, b_qkv3):
    full = lambda b, s: (0, b, 0, 0)
    in_specs = [pl.BlockSpec((8, 1, QB, D), full), pl.BlockSpec((16, 1, L, L), full)]
    for t in range(3):
        for u in range(2):
            in_specs.append(pl.BlockSpec((D, L), lambda b, s, t=t, u=u: (0, t * 8 + s[2 * u])))
    for t in range(3):
        for u in range(2):
            in_specs.append(pl.BlockSpec((1, 8, L), lambda b, s, t=t, u=u: (t * 8 + s[2 * u], 0, 0)))
    flash = [pltpu.VMEM((QB, S), F32), pltpu.VMEM((QB, S), BF), pltpu.VMEM((QB, S), BF)]
    band = [pltpu.VMEM((QB, 768), F32), pltpu.VMEM((QB, 768), BF), pltpu.VMEM((QB, 768), BF)]
    return pl.pallas_call(
        attn_kernel,
        grid_spec=pltpu.PrefetchScalarGridSpec(
            num_scalar_prefetch=1,
            grid=(2,),
            in_specs=in_specs,
            out_specs=[
                pl.BlockSpec((16, 1, 4, L, L), lambda b, s: (0, b, 0, 0, 0)),
                pl.BlockSpec((DR, W3), lambda b, s: (0, 0)),
            ],
            scratch_shapes=[
                pltpu.VMEM((D, W3), BF), pltpu.VMEM((8, W3), F32),
                pltpu.VMEM((S, W3), BF), pltpu.VMEM((S, W3), BF),
                pltpu.VMEM((L, S), BF), pltpu.VMEM((L, S), BF),
                pltpu.VMEM((L, S), F32), pltpu.VMEM((L, S), F32),
            ] + flash + band,
        ),
        out_shape=[jax.ShapeDtypeStruct((16, 2, 4, L, L), BF), jax.ShapeDtypeStruct((DR, W3), F32)],
        compiler_params=pltpu.CompilerParams(vmem_limit_bytes=VMEM_CAP, dimension_semantics=("arbitrary",)),
        cost_estimate=pl.CostEstimate(flops=40 * 10**9, bytes_accessed=20 << 20, transcendentals=0),
        name="attn",
    )(sel, hg, dog, *([w_qkv] * 6), *([b_qkv3] * 6))


def gather_heads(recv_ref, pos_ref, arr, b, m):
    pa, pb = pos_ref[2 * m], pos_ref[2 * m + 1]
    k, j = b // 2, b % 2
    a = recv_ref[2 * (pa % 8) + k, j, arr]
    c = recv_ref[2 * (pb % 8) + k, j, arr]
    return pair_halves(a, pa // 8, c, pb // 8)


def post_kernel(pos_ref, recv_ref, x_ref, dy_ref, gamma_ref, bout_ref, wqkv_ref, wout_ref,
                y_ref, dx_ref, dwout_ref, small_ref, o_ref, dqkv_ref):
    for b in range(4):
        for m in range(8):
            o_ref[b * L:(b + 1) * L, m * L:(m + 1) * L] = gather_heads(recv_ref, pos_ref, 0, b, m)
            for t in range(3):
                dqkv_ref[b * L:(b + 1) * L, t * D + m * L:t * D + (m + 1) * L] = gather_heads(
                    recv_ref, pos_ref, 1 + t, b, m)
    gamma = gamma_ref[...].astype(F32)
    bout = bout_ref[...].astype(F32)
    dy_all = dy_ref[...].reshape(T, D)
    for c in range(4):
        dwout_ref[c * QB:(c + 1) * QB] = dot_tn(o_ref[:, c * QB:(c + 1) * QB], dy_all)
    dg = jnp.zeros((1, D), F32)
    db = jnp.zeros((1, D), F32)
    dbo = jnp.zeros((1, D), F32)
    for b in range(4):
        rows = slice(b * L, (b + 1) * L)
        xf = x_ref[b].astype(F32)
        dyf = dy_ref[b].astype(F32)
        y_ref[b] = (xf + dot_nn(o_ref[rows], wout_ref[...]) + bout).astype(BF)
        cen = xf - jnp.mean(xf, axis=-1, keepdims=True)
        rstd = lax.rsqrt(jnp.mean(cen * cen, axis=-1, keepdims=True) + LN_EPS)
        xhat = cen * rstd
        dh = dot_nt(dqkv_ref[rows], wqkv_ref[...]).astype(BF).astype(F32)
        dg += jnp.sum(dh * xhat, axis=0, keepdims=True)
        db += jnp.sum(dh, axis=0, keepdims=True)
        dbo += jnp.sum(dyf, axis=0, keepdims=True)
        dxh = dh * gamma
        m1 = jnp.mean(dxh, axis=-1, keepdims=True)
        m2 = jnp.mean(dxh * xhat, axis=-1, keepdims=True)
        dx_ref[b] = (dyf + rstd * (dxh - m1 - xhat * m2)).astype(BF)
    small_ref[...] = jnp.zeros_like(small_ref)
    small_ref[0:1] = dg
    small_ref[1:2] = db
    small_ref[2:3] = dbo


def post_call(pos, recv, x, dy, gamma, bout, wqkv, wout):
    vm = pl.BlockSpec(memory_space=pltpu.VMEM)
    tok = jax.ShapeDtypeStruct((4, L, D), BF)
    return pl.pallas_call(
        post_kernel,
        out_shape=(tok, tok, jax.ShapeDtypeStruct((D, D), F32), jax.ShapeDtypeStruct((8, D), F32)),
        in_specs=[pl.BlockSpec(memory_space=pltpu.SMEM)] + [vm] * 7,
        out_specs=(vm,) * 4,
        scratch_shapes=[pltpu.VMEM((T, D), BF), pltpu.VMEM((T, D3), BF)],
        compiler_params=pltpu.CompilerParams(vmem_limit_bytes=VMEM_CAP),
        cost_estimate=pl.CostEstimate(flops=10 * 10**9, bytes_accessed=24 << 20, transcendentals=0),
        name="post",
    )(pos, recv, x, dy, gamma, bout, wqkv, wout)


def unpack_kernel(pos_ref, dw_ref, out_ref):
    r = pl.program_id(1)
    m = r % 8
    pa, pb = pos_ref[2 * m], pos_ref[2 * m + 1]
    a = dw_ref[pa % 8]
    c = dw_ref[pb % 8]
    out_ref[...] = pair_halves(a, pa // 8, c, pb // 8)


def unpack_call(pos, dwg):
    return pl.pallas_call(
        unpack_kernel,
        grid_spec=pltpu.PrefetchScalarGridSpec(
            num_scalar_prefetch=1,
            grid=(3, 8),
            in_specs=[pl.BlockSpec((8, DR, L), lambda t, m, s: (0, 0, t))],
            out_specs=pl.BlockSpec((DR, L), lambda t, m, s: (0, t * 8 + m)),
        ),
        out_shape=jax.ShapeDtypeStruct((DR, D3), F32),
        compiler_params=pltpu.CompilerParams(vmem_limit_bytes=VMEM_CAP),
        name="unpack",
    )(pos, dwg)


def solution(mesh):
    tok_spec = P(None, "sp", None)

    def local_block(x, d_y, ln_gamma, ln_beta, w_qkv, b_qkv, w_out, b_out, head_kind):
        me = lax.axis_index("sp")
        chip, core = me // 2, me % 2
        idx = jnp.arange(16, dtype=jnp.int32)
        same_before = (head_kind[None, :] == head_kind[:, None]) & (idx[None, :] < idx[:, None])
        pos = jnp.sum(same_before.astype(jnp.int32), axis=1) + 8 * head_kind
        perm = jnp.sum(jnp.where(pos[None, :] == idx[:, None], idx[None, :], 0), axis=1)
        f, g = perm[chip], perm[8 + chip]
        sel = jnp.stack([f // 2, f % 2, g // 2, g % 2])
        gamma2, beta2, bout2 = (v.reshape(1, D) for v in (ln_gamma, ln_beta, b_out))
        h, do = pre_call(perm, x, d_y, gamma2, beta2, w_out.reshape(16, 64, D))
        h2 = h.reshape(2, 2, L, D)
        mine = jnp.where(core == 0, h2[0], h2[1])
        other = jnp.where(core == 0, h2[1], h2[0])
        got = lax.ppermute(other, "sp", [(d, d ^ 1) for d in range(16)])
        blk = jnp.stack([jnp.where(core == 0, mine, got), jnp.where(core == 0, got, mine)], axis=1)
        blk = blk.reshape(2, QB, D)
        hg = lax.all_gather(blk, "sp", axis_index_groups=[list(range(0, 16, 2)), list(range(1, 16, 2))])
        dog = lax.all_to_all(do.reshape(16, 2, L, L), "sp", 0, 0, tiled=True)
        b3 = jnp.broadcast_to(b_qkv.reshape(24, 1, L), (24, 8, L))
        send, dwp = attn_call(sel, hg, dog, w_qkv, b3)
        recv = lax.all_to_all(send, "sp", 0, 0, tiled=True)
        y, dx, dwout, small = post_call(pos, recv, x, d_y, gamma2, bout2, w_qkv, w_out)
        dwg = lax.all_gather(dwp, "sp").reshape(8, 2, DR, W3)
        dw = unpack_call(pos, dwg[:, 0] + dwg[:, 1])
        dwout, small = lax.psum((dwout, small), "sp")
        return y, dx, small[0], small[1], dw[:D], dw[D], dwout, small[2]

    return jax.shard_map(
        local_block, mesh=mesh,
        in_specs=(tok_spec, tok_spec, P(), P(), P(), P(), P(), P(), P()),
        out_specs=(tok_spec, tok_spec, P(), P(), P(), P(), P(), P()), check_vma=False)
```

```python
import functools
import math

import jax
import jax.numpy as jnp
from jax import lax
from jax.experimental import pallas as pl
from jax.experimental.pallas import tpu as pltpu
from jax.sharding import PartitionSpec as P

LN_EPS = 1e-5
NEG_BIG = -1e30
BF = jnp.bfloat16
F32 = jnp.float32
QB = 256
L = 128
W3 = 384
T = 512
D = 1024
DR = 1040
HR = 520
N = 16
R3, R4, R8 = range(3), range(4), range(8)
MESH = pl.DeviceIdType.MESH
H_ROWS = (0, 176, 352, 512)
W_ROWS = (0, 176, 352, 520)
O_ROWS = (0, 24, 48, 64)
S = 2048
D3 = 3072
VMEM_CAP = 60 * D * D


def dot_nn(a, b):
    return lax.dot_general(a, b, (((1,), (0,)), ((), ())), preferred_element_type=F32)


def dot_nt(a, b):
    return lax.dot_general(a, b, (((1,), (1,)), ((), ())), preferred_element_type=F32)


def dot_tn(a, b):
    return lax.dot_general(a, b, (((0,), (0,)), ((), ())), preferred_element_type=F32)


def swap_halves(a):
    return jnp.concatenate([a[:, 64:], a[:, :64]], axis=1)


def pair_halves(a, a_half, b, b_half):
    lane = lax.broadcasted_iota(jnp.int32, a.shape, 1)
    a = jnp.where(a_half == 1, swap_halves(a), a)
    b = jnp.where(b_half == 0, swap_halves(b), b)
    return jnp.where(lane < 64, a, b)


class Place:
    def __init__(self):
        self.me = lax.axis_index("sp")
        self.core, self.chip = self.me % 2, self.me // 2
        self.sib = self.me + 1 - 2 * self.core
        bits = (self.chip % 2, self.chip // 2 % 2, self.chip // 4)
        self.step = [(1 - 2 * v) * w for v, w in zip(bits, (1, 2, 4))]

    def chip_at(self, axes):
        out = self.chip
        for a in axes:
            out = out + self.step[a]
        return out

    def next_dev(self, axis):
        return self.me + 2 * self.step[axis]


def rcopy(src, dst, send, recv, dev):
    return pltpu.make_async_remote_copy(
        src_ref=src, dst_ref=dst, send_sem=send, recv_sem=recv, device_id=(dev,), device_id_type=MESH)


def subsets(axes):
    out = [()]
    for a in axes:
        out += [v + (a,) for v in out]
    return out


class Tree:
    def __init__(self, place, own, slot, send, recv):
        self.place, self.own, self.slot, self.send, self.recv = place, own, slot, send, recv
        self.entries = []
        for s in R3:
            for p in R3:
                order = [(p + j) % 3 for j in R3]
                for sub in subsets(order[:s]):
                    self.entries.append((p, order[s], sub))

    def copy(self, e):
        p, axis, sub = e
        i = self.entries.index(e)
        at = self.slot(self.place.chip_at(sub), p)
        return rcopy(at if sub else self.own(p), at, self.send.at[i], self.recv.at[i], self.place.next_dev(axis))

    def start_own(self):
        for e in self.entries:
            if not e[2]:
                self.copy(e).start()

    def arrive(self, e):
        p, axis, sub = e
        got = sub + (axis,)
        chip = self.place.chip_at(got)
        at = self.slot(chip, p)
        i = self.entries.index(e)
        rcopy(at, at, self.send.at[i], self.recv.at[i], self.place.next_dev(axis)).wait_recv()
        for n in self.entries:
            if n[0] == p and n[2] == got:
                self.copy(n).start()
        return chip, p

    def level(self, s):
        return [e for e in self.entries if len(e[2]) <= s and (e[1] - e[0]) % 3 == s]

    def finish(self):
        for e in self.entries:
            self.copy(e).wait_send()


def barrier_signal(place):
    sem = pltpu.get_barrier_semaphore()
    for r in range(1, N):
        pl.semaphore_signal(sem, inc=1, device_id=((place.me + r) % N,), device_id_type=MESH)


def barrier_wait():
    pl.semaphore_wait(pltpu.get_barrier_semaphore(), N - 1)


def head_places(kind_ref):
    pos, zeros, ones = [], 0, 8
    for n in range(N):
        k = kind_ref[n]
        pos.append(jnp.where(k == 0, zeros, ones))
        zeros, ones = zeros + 1 - k, ones + k
    return pos


def exchange(place, src, dst, send, recv):
    out = []
    for r in range(1, N):
        to = (place.me + r) % N
        cp = rcopy(src(to), dst(place.me), send.at[r], recv.at[r], to)
        cp.start()
        out.append(cp)
    return out


def exchange_wait(place, dst, send, recv):
    for r in range(1, N):
        at = dst((place.me + N - r) % N)
        rcopy(at, at, send.at[r], recv.at[r], place.me).wait_recv()


def pre_kernel(kind_ref, x_ref, dy_ref, gamma_ref, beta_ref, wout_hbm, hg_ref, dog_ref, sel_ref,
               blk_ref, out_ref, wout_ref, wp_ref, do_ref, loc_sem, sib_send, sib_recv, ag_send, ag_recv, do_send, do_recv):
    pc = Place()
    barrier_signal(pc)
    w_in = pltpu.make_async_copy(wout_hbm, wout_ref, loc_sem.at[0])
    w_in.start()
    gamma = gamma_ref[...].reshape(1, D).astype(F32)
    beta = beta_ref[...].reshape(1, D).astype(F32)

    def norm(xb):
        xf = xb.astype(F32)
        cen = xf - jnp.mean(xf, axis=-1, keepdims=True)
        var = jnp.mean(cen * cen, axis=-1, keepdims=True)
        return (cen * lax.rsqrt(var + LN_EPS) * gamma + beta).astype(BF)

    for j in range(2):
        out_ref[j] = norm(x_ref[2 * (1 - pc.core) + j])
    for j in range(2):
        blk_ref[j, pc.core] = norm(x_ref[2 * pc.core + j])
    barrier_wait()
    sib = [rcopy(out_ref.at[j], blk_ref.at[j, pc.core], sib_send.at[j], sib_recv.at[j], pc.sib) for j in range(2)]
    for cp in sib:
        cp.start()
    pos = head_places(kind_ref)
    perm = []
    for j in range(N):
        v = 0
        for n in range(1, N):
            v = v + jnp.where(pos[n] == j, n, 0)
        perm.append(v)
    f = g = 0
    for c in R8:
        f = f + jnp.where(pc.chip == c, perm[c], 0)
        g = g + jnp.where(pc.chip == c, perm[8 + c], 0)
    for i, v in enumerate((f // 2, f % 2, g // 2, g % 2)):
        sel_ref[i] = v
    for j in range(2):
        rcopy(blk_ref.at[j, 1 - pc.core], blk_ref.at[j, 1 - pc.core], sib_send.at[j], sib_recv.at[j], pc.sib).wait_recv()

    def rows(p):
        return pl.ds(H_ROWS[p], H_ROWS[p + 1] - H_ROWS[p])

    flat = blk_ref.reshape(T, D)
    tree = Tree(pc, lambda p: flat.at[rows(p)], lambda c, p: hg_ref.at[c, rows(p)], ag_send, ag_recv)
    tree.start_own()
    local = pltpu.make_async_copy(flat, hg_ref.at[pc.chip], loc_sem.at[1])
    local.start()
    w_in.wait()
    for c in R8:
        wp_ref[c * L:c * L + 64] = wout_ref[perm[c]]
        wp_ref[c * L + 64:c * L + L] = wout_ref[perm[8 + c]]
    dy = dy_ref[...].reshape(T, D)
    for c in R4:
        d = dot_nt(dy, wp_ref[c * QB:(c + 1) * QB]).astype(BF)
        for u in range(2):
            do_ref[2 * c + u] = d[:, u * L:(u + 1) * L].reshape(4, L, L)
    for e in tree.level(0):
        tree.arrive(e)
    mine = do_ref.reshape(N, 2, L, L)
    copies = exchange(pc, lambda t: mine.at[t], lambda t: dog_ref.at[t], do_send, do_recv)
    keep = pltpu.make_async_copy(mine.at[pc.me], dog_ref.at[pc.me], loc_sem.at[2])
    keep.start()
    for s in (1, 2):
        for e in tree.level(s):
            tree.arrive(e)
    exchange_wait(pc, lambda t: dog_ref.at[t], do_send, do_recv)
    local.wait()
    keep.wait()
    tree.finish()
    for cp in copies + sib:
        cp.wait_send()


def pre_call(kind, x, dy, gamma, beta, wout):
    vm, sm, hb = (pl.BlockSpec(memory_space=m) for m in (pltpu.VMEM, pltpu.SMEM, pl.ANY))
    sem = pltpu.SemaphoreType.DMA
    return pl.pallas_call(
        pre_kernel,
        out_shape=(jax.ShapeDtypeStruct((8, T, D), BF), jax.ShapeDtypeStruct((N, 2, L, L), BF),
                   jax.ShapeDtypeStruct((4,), jnp.int32)),
        in_specs=[sm, vm, vm, vm, vm, hb],
        out_specs=(hb, hb, sm),
        scratch_shapes=[
            pltpu.VMEM((2, 2, L, D), BF), pltpu.VMEM((2, L, D), BF), pltpu.VMEM((N, 64, D), BF),
            pltpu.VMEM((D, D), BF), pltpu.VMEM((8, 4, L, L), BF),
            sem((3,)), sem((2,)), sem((2,)), sem((21,)), sem((21,)), sem((N,)), sem((N,))],
        compiler_params=pltpu.CompilerParams(vmem_limit_bytes=VMEM_CAP, collective_id=0, has_side_effects=True),
        name="pre",
    )(kind, x, dy, gamma, beta, wout)


def attn_kernel(sel_ref, hg_ref, dog_ref, *refs):
    w_refs, bias_refs = refs[:6], refs[6:12]
    so_ref, sd_ref, dwp_ref = refs[12:15]
    w_ref, bias_ref, qkv_ref, dqkv_ref, qt_ref, dot_ref, dkt_ref, dvt_ref = refs[15:23]
    scr = (refs[23:26], refs[26:29])
    b = pl.program_id(0)
    f_half, g_half = sel_ref[1], sel_ref[3]

    @pl.when(b == 0)
    def _():
        for t in R3:
            w_ref[:, t * L:(t + 1) * L] = pair_halves(w_refs[2 * t][...], f_half, w_refs[2 * t + 1][...], g_half)
            bf = bias_refs[2 * t][0].astype(F32)
            bg = bias_refs[2 * t + 1][0].astype(F32)
            bias_ref[:, t * L:(t + 1) * L] = pair_halves(bf, f_half, bg, g_half)
        dwp_ref[...] = jnp.zeros_like(dwp_ref)

    def qkv_step(r, carry):
        rows = hg_ref[pl.ds(2 * r, 2), 0].reshape(T, D)
        out = dot_nn(rows, w_ref[...]) + bias_ref[0:1, :]
        qkv_ref[pl.ds(pl.multiple_of(r * T, T), T), :] = out.astype(BF)
        return carry

    lax.fori_loop(0, 4, qkv_step, 0)
    for i in R8:
        qs = qkv_ref[i * QB:(i + 1) * QB, 0:L] * BF(0.125)
        qt_ref[:, i * QB:(i + 1) * QB] = qs.T
        do = dog_ref[2 * i:2 * i + 2, 0].reshape(QB, L)
        dot_ref[:, i * QB:(i + 1) * QB] = do.T
    dkt_ref[...] = jnp.zeros_like(dkt_ref)
    dvt_ref[...] = jnp.zeros_like(dvt_ref)
    lane = lax.broadcasted_iota(jnp.int32, (QB, L), 1)
    row_i = lax.broadcasted_iota(jnp.int32, (QB, QB), 0)
    col_i = lax.broadcasted_iota(jnp.int32, (QB, QB), 1)

    def head_block(i, hd):
        s_ref, p_ref, ds_ref = scr[hd]
        first = 0 if hd == 0 else max(0, i - 2)
        blocks = range(first, i + 1)
        mine = (lane < 64) if hd == 0 else (lane >= 64)
        qi = qkv_ref[i * QB:(i + 1) * QB, 0:L] * BF(0.125)
        doi = dog_ref[2 * i:2 * i + 2, 0].reshape(QB, L)
        qm = jnp.where(mine, qi, BF(0))
        dom = jnp.where(mine, doi, BF(0))
        mx = None
        for kb in blocks:
            s = dot_nt(qm, qkv_ref[kb * QB:(kb + 1) * QB, L:QB])
            if kb == i:
                s = jnp.where(col_i <= row_i, s, NEG_BIG)
            if hd == 1 and kb == i - 2:
                s = jnp.where(col_i > row_i, s, NEG_BIG)
            s_ref[:, (kb - first) * QB:(kb - first + 1) * QB] = s
            cur = jnp.maximum(s[:, :L], s[:, L:])
            mx = cur if mx is None else jnp.maximum(mx, cur)
        m = jnp.max(mx, axis=1, keepdims=True)
        ls = None
        for kb in blocks:
            o_ = (kb - first) * QB
            e = jnp.exp(s_ref[:, o_:o_ + QB] - m)
            s_ref[:, o_:o_ + QB] = e
            cur = e[:, :L] + e[:, L:]
            ls = cur if ls is None else ls + cur
        rl = 1.0 / jnp.sum(ls, axis=1, keepdims=True)
        acc = None
        for kb in blocks:
            o_ = (kb - first) * QB
            p_ = s_ref[:, o_:o_ + QB] * rl
            s_ref[:, o_:o_ + QB] = p_
            pb = p_.astype(BF)
            p_ref[:, o_:o_ + QB] = pb
            cur = dot_nn(pb, qkv_ref[kb * QB:(kb + 1) * QB, QB:W3])
            acc = cur if acc is None else acc + cur
        dsum = jnp.sum(dom.astype(F32) * acc, axis=1, keepdims=True)
        dq = None
        for kb in blocks:
            o_ = (kb - first) * QB
            dp = dot_nt(dom, qkv_ref[kb * QB:(kb + 1) * QB, QB:W3]).astype(BF).astype(F32)
            ds = (s_ref[:, o_:o_ + QB] * (dp - dsum)).astype(BF)
            ds_ref[:, o_:o_ + QB] = ds
            cur = dot_nn(ds, qkv_ref[kb * QB:(kb + 1) * QB, L:QB])
            dq = cur if dq is None else dq + cur
        hr = slice(hd * 64, hd * 64 + 64)
        n = len(blocks) * QB
        dotb = dot_ref[hr, i * QB:(i + 1) * QB]
        qtb = qt_ref[hr, i * QB:(i + 1) * QB]
        dvt_ref[hr, first * QB:first * QB + n] += dot_nn(dotb, p_ref[:, :n])
        dkt_ref[hr, first * QB:first * QB + n] += dot_nn(qtb, ds_ref[:, :n])
        return acc, dq * 0.125

    for i in R8:
        of, dqf = head_block(i, 0)
        og, dqg = head_block(i, 1)
        o = jnp.where(lane < 64, of, og).astype(BF)
        dq = jnp.where(lane < 64, dqf, dqg).astype(BF)
        for u in range(2):
            so_ref[2 * i + u, 0] = o[u * L:(u + 1) * L]
            sd_ref[2 * i + u, 0, 0] = dq[u * L:(u + 1) * L]
        dqkv_ref[i * QB:(i + 1) * QB, 0:L] = dq

    for t, src in ((1, dkt_ref), (2, dvt_ref)):
        for j in range(16):
            d = src[:, j * L:(j + 1) * L].T.astype(BF)
            sd_ref[j, 0, t] = d
            dqkv_ref[j * L:(j + 1) * L, t * L:(t + 1) * L] = d

    def dw_step(r, carry):
        cols = pl.ds(pl.multiple_of(r * QB, QB), QB)
        hc = hg_ref[:, 0, :, cols].reshape(S, QB)
        dwp_ref[cols, :] += dot_tn(hc, dqkv_ref[...])
        return carry

    lax.fori_loop(0, 4, dw_step, 0)
    dwp_ref[D:1025, :] += jnp.sum(dqkv_ref[...].astype(F32), axis=0, keepdims=True)


def attn_call(sel, hg, dog, w_qkv, b_qkv3):
    full = lambda b, s: (0, b, 0, 0)
    in_specs = [pl.BlockSpec((8, 1, QB, D), full), pl.BlockSpec((16, 1, L, L), full)]
    for t in R3:
        for u in range(2):
            in_specs.append(pl.BlockSpec((D, L), lambda b, s, t=t, u=u: (0, t * 8 + s[2 * u])))
    for t in R3:
        for u in range(2):
            in_specs.append(pl.BlockSpec((1, 8, L), lambda b, s, t=t, u=u: (t * 8 + s[2 * u], 0, 0)))
    flash = [pltpu.VMEM((QB, S), F32), pltpu.VMEM((QB, S), BF), pltpu.VMEM((QB, S), BF)]
    band = [pltpu.VMEM((QB, 768), F32), pltpu.VMEM((QB, 768), BF), pltpu.VMEM((QB, 768), BF)]
    return pl.pallas_call(
        attn_kernel,
        grid_spec=pltpu.PrefetchScalarGridSpec(
            num_scalar_prefetch=1,
            grid=(2,),
            in_specs=in_specs,
            out_specs=[
                pl.BlockSpec((N, 1, L, L), full),
                pl.BlockSpec((N, 1, 3, L, L), lambda b, s: (0, b, 0, 0, 0)),
                pl.BlockSpec((DR, W3), lambda b, s: (0, 0)),
            ],
            scratch_shapes=[
                pltpu.VMEM((D, W3), BF), pltpu.VMEM((8, W3), F32),
                pltpu.VMEM((S, W3), BF), pltpu.VMEM((S, W3), BF),
                pltpu.VMEM((L, S), BF), pltpu.VMEM((L, S), BF),
                pltpu.VMEM((L, S), F32), pltpu.VMEM((L, S), F32),
            ] + flash + band,
        ),
        out_shape=[jax.ShapeDtypeStruct((N, 2, L, L), BF), jax.ShapeDtypeStruct((N, 2, 3, L, L), BF),
                   jax.ShapeDtypeStruct((DR, W3), F32)],
        compiler_params=pltpu.CompilerParams(vmem_limit_bytes=VMEM_CAP, dimension_semantics=("arbitrary",)),
        cost_estimate=pl.CostEstimate(flops=40 * 10**9, bytes_accessed=20 << 20, transcendentals=0),
        name="attn",
    )(sel, hg, dog, *([w_qkv] * 6), *([b_qkv3] * 6))


def gather_heads(recv_at, pos, b, m):
    pa, pb = pos[2 * m], pos[2 * m + 1]
    k, j = b // 2, b % 2
    a = recv_at(2 * (pa % 8) + k, j)
    c = recv_at(2 * (pb % 8) + k, j)
    return pair_halves(a, pa // 8, c, pb // 8)


def post_kernel(kind_ref, so_hbm, sd_hbm, dwp_ref, x_ref, dy_ref, gamma_ref, bout_ref, wqkv_hbm, wout_hbm,
                y_ref, dx_ref, small_ref, dwg_ref, dwo_ref,
                ro_ref, rd_ref, o_ref, dqkv_ref, wqkv_ref, wout_ref, dwx_ref, dws_ref, part_ref, px_ref, acc_ref,
                rs0_ref, rs1_ref, rs2_ref, sm_ref,
                loc, o_send, o_recv, d_send, d_recv, s_send, s_recv, x_send, x_recv,
                w_send, w_recv, g_send, g_recv, ws_send, ws_recv, gs_send, gs_recv, r_send, r_recv):
    pc = Place()
    barrier_signal(pc)
    loads = [pltpu.make_async_copy(so_hbm.at[pc.me], ro_ref.at[pc.me], loc.at[0]),
             pltpu.make_async_copy(sd_hbm.at[pc.me], rd_ref.at[pc.me], loc.at[1]),
             pltpu.make_async_copy(wout_hbm, wout_ref, loc.at[2]),
             pltpu.make_async_copy(wqkv_hbm, wqkv_ref, loc.at[3])]
    for cp in loads:
        cp.start()
    pos = head_places(kind_ref)
    gamma = gamma_ref[...].reshape(1, D).astype(F32)
    bout = bout_ref[...].reshape(1, D).astype(F32)
    barrier_wait()
    sends = exchange(pc, lambda t: so_hbm.at[t], lambda t: ro_ref.at[t], o_send, o_recv)
    half = rcopy(dwp_ref.at[1 - pc.core], dwx_ref, x_send.at[0], x_recv.at[0], pc.sib)
    half.start()
    sends += exchange(pc, lambda t: sd_hbm.at[t], lambda t: rd_ref.at[t], d_send, d_recv)
    half.wait_recv()
    dws_ref[...] = dwp_ref[pc.core] + dwx_ref[...]

    def w_rows(p):
        return pl.ds(W_ROWS[p], W_ROWS[p + 1] - W_ROWS[p])

    def o_rows(p):
        return pl.ds(O_ROWS[p], O_ROWS[p + 1] - O_ROWS[p])

    def w_slot(c, p, core=pc.core):
        return dwg_ref.at[c, core, w_rows(p)]

    def g_slot(c, p, core=pc.core):
        return dwo_ref.at[core, c, o_rows(p)]

    def to_sib(n, src, dst, send, recv):
        cp = rcopy(src, dst, send.at[n], recv.at[n], pc.sib)
        cp.start()
        sends.append(cp)

    wtree = Tree(pc, lambda p: dws_ref.at[w_rows(p)], w_slot, w_send, w_recv)
    wtree.start_own()
    keep_w = pltpu.make_async_copy(dws_ref, dwg_ref.at[pc.chip, pc.core], loc.at[4])
    keep_w.start()
    for p in R3:
        to_sib(p, dws_ref.at[w_rows(p)], w_slot(pc.chip, p), ws_send, ws_recv)

    def w_arrive(s):
        for e in wtree.level(s):
            c, p = wtree.arrive(e)
            to_sib(3 + wtree.entries.index(e), w_slot(c, p), w_slot(c, p), ws_send, ws_recv)

    loads[0].wait()
    loads[2].wait()
    exchange_wait(pc, lambda t: ro_ref.at[t], o_send, o_recv)
    for b in R4:
        for m in R8:
            o_ref[b * L:(b + 1) * L, m * L:(m + 1) * L] = gather_heads(lambda q, j: ro_ref[q, j], pos, b, m)
    dy_all = dy_ref[...].reshape(T, D)
    for c in R4:
        part_ref[c // 2, c % 2 * QB:(c % 2 + 1) * QB] = dot_tn(o_ref[:, c * QB:(c + 1) * QB], dy_all)
    dbo = jnp.zeros((1, D), F32)
    for b in R4:
        rows = slice(b * L, (b + 1) * L)
        xf = x_ref[b].astype(F32)
        y_ref[b] = (xf + dot_nn(o_ref[rows], wout_ref[...]) + bout).astype(BF)
        dbo += jnp.sum(dy_ref[b].astype(F32), axis=0, keepdims=True)
    xp = rcopy(part_ref.at[1 - pc.core], px_ref, x_send.at[1], x_recv.at[1], pc.sib)
    xp.start()
    xp.wait_recv()
    acc_ref[...] = (part_ref[pc.core] + px_ref[...]).reshape(8, 64, D)

    bufs = (rs0_ref, rs1_ref, rs2_ref)

    def reduce_step(s, wait):
        for p in R3:
            order = [(p + j) % 3 for j in R3]
            for i, sub in enumerate(subsets(order[s + 1:])):
                n = p * 7 + (0, 4, 6)[s] + i
                dst = bufs[s].at[i, o_rows(p)]
                if not wait:
                    cp = rcopy(acc_ref.at[pc.chip_at((order[s],) + sub), o_rows(p)], dst,
                               r_send.at[n], r_recv.at[n], pc.next_dev(order[s]))
                    cp.start()
                    sends.append(cp)
                else:
                    rcopy(dst, dst, r_send.at[n], r_recv.at[n], pc.sib).wait_recv()
                    acc_ref[pc.chip_at(sub), o_rows(p)] += bufs[s][i, o_rows(p)]

    reduce_step(0, False)
    loads[1].wait()
    loads[3].wait()
    exchange_wait(pc, lambda t: rd_ref.at[t], d_send, d_recv)
    w_arrive(0)
    for b in R4:
        for m in R8:
            for t in R3:
                dqkv_ref[b * L:(b + 1) * L, t * D + m * L:t * D + (m + 1) * L] = gather_heads(
                    lambda q, j: rd_ref[q, j, t], pos, b, m)
    reduce_step(0, True)
    reduce_step(1, False)
    dg = jnp.zeros((1, D), F32)
    db = jnp.zeros((1, D), F32)
    for b in R4:
        rows = slice(b * L, (b + 1) * L)
        xf = x_ref[b].astype(F32)
        cen = xf - jnp.mean(xf, axis=-1, keepdims=True)
        rstd = lax.rsqrt(jnp.mean(cen * cen, axis=-1, keepdims=True) + LN_EPS)
        xhat = cen * rstd
        dh = dot_nt(dqkv_ref[rows], wqkv_ref[...]).astype(BF).astype(F32)
        dg += jnp.sum(dh * xhat, axis=0, keepdims=True)
        db += jnp.sum(dh, axis=0, keepdims=True)
        dxh = dh * gamma
        m1 = jnp.mean(dxh, axis=-1, keepdims=True)
        m2 = jnp.mean(dxh * xhat, axis=-1, keepdims=True)
        dx_ref[b] = (dy_ref[b].astype(F32) + rstd * (dxh - m1 - xhat * m2)).astype(BF)
    row = lax.broadcasted_iota(jnp.int32, (8, D), 0)
    sm_ref[pc.me] = jnp.where(row == 0, dg, jnp.where(row == 1, db, jnp.where(row == 2, dbo, 0.0)))
    w_arrive(1)
    reduce_step(1, True)
    reduce_step(2, False)
    sends += exchange(pc, lambda t: sm_ref.at[pc.me], lambda t: sm_ref.at[t], s_send, s_recv)
    reduce_step(2, True)
    gtree = Tree(pc, lambda p: acc_ref.at[pc.chip, o_rows(p)], g_slot, g_send, g_recv)
    gtree.start_own()
    keep_g = pltpu.make_async_copy(acc_ref.at[pc.chip], dwo_ref.at[pc.core, pc.chip], loc.at[5])
    keep_g.start()
    for p in R3:
        to_sib(p, acc_ref.at[pc.chip, o_rows(p)], g_slot(pc.chip, p), gs_send, gs_recv)

    def g_arrive(s):
        for e in gtree.level(s):
            c, p = gtree.arrive(e)
            to_sib(3 + gtree.entries.index(e), g_slot(c, p), g_slot(c, p), gs_send, gs_recv)

    w_arrive(2)
    g_arrive(0)
    exchange_wait(pc, lambda t: sm_ref.at[t], s_send, s_recv)
    tot = sm_ref[0]
    for n in range(1, N):
        tot = tot + sm_ref[n]
    small_ref[...] = tot
    g_arrive(1)
    g_arrive(2)
    for tree, slot, send, recv in ((wtree, w_slot, ws_send, ws_recv), (gtree, g_slot, gs_send, gs_recv)):
        for p in R3:
            at = slot(pc.chip, p, 1 - pc.core)
            rcopy(at, at, send.at[p], recv.at[p], pc.sib).wait_recv()
        for i, (p, axis, sub) in enumerate(tree.entries):
            at = slot(pc.chip_at(sub + (axis,)), p, 1 - pc.core)
            rcopy(at, at, send.at[3 + i], recv.at[3 + i], pc.sib).wait_recv()
        tree.finish()
    for cp in sends + [half, xp]:
        cp.wait_send()
    keep_w.wait()
    keep_g.wait()


def post_call(kind, so, sd, dwp, x, dy, gamma, bout, wqkv, wout):
    vm, sm, hb = (pl.BlockSpec(memory_space=m) for m in (pltpu.VMEM, pltpu.SMEM, pl.ANY))
    sem = pltpu.SemaphoreType.DMA
    tok = jax.ShapeDtypeStruct((4, L, D), BF)
    pair = lambda n: [sem((n,)), sem((n,))]
    return pl.pallas_call(
        post_kernel,
        out_shape=(tok, tok, jax.ShapeDtypeStruct((8, D), F32), jax.ShapeDtypeStruct((8, 2, HR, W3), F32),
                   jax.ShapeDtypeStruct((2, 8, 64, D), F32)),
        in_specs=[sm, hb, hb] + [vm] * 5 + [hb, hb],
        out_specs=(vm, vm, vm, hb, hb),
        scratch_shapes=[
            pltpu.VMEM((N, 2, L, L), BF), pltpu.VMEM((N, 2, 3, L, L), BF),
            pltpu.VMEM((T, D), BF), pltpu.VMEM((T, D3), BF), pltpu.VMEM((D, D3), BF), pltpu.VMEM((D, D), BF),
            pltpu.VMEM((HR, W3), F32), pltpu.VMEM((HR, W3), F32),
            pltpu.VMEM((2, T, D), F32), pltpu.VMEM((T, D), F32), pltpu.VMEM((8, 64, D), F32),
            pltpu.VMEM((4, 64, D), F32), pltpu.VMEM((2, 64, D), F32), pltpu.VMEM((1, 64, D), F32),
            pltpu.VMEM((N, 8, D), F32), sem((6,))]
        + pair(N) + pair(N) + pair(N) + pair(2) + pair(21) + pair(21) + pair(24) + pair(24) + pair(21),
        compiler_params=pltpu.CompilerParams(vmem_limit_bytes=VMEM_CAP, collective_id=1, has_side_effects=True),
        name="post",
    )(kind, so, sd, dwp, x, dy, gamma, bout, wqkv, wout)


def unpack_kernel(kind_ref, dw_ref, bias_in_ref, dwo_ref, small_ref, out_ref, bias_ref, wo_ref, dg_ref, db_ref, dbo_ref):
    pos = head_places(kind_ref)
    wo_ref[...] = dwo_ref[...]

    def pick(ref, t, m):
        cols = slice(t * L, (t + 1) * L)
        pa, pb = pos[2 * m], pos[2 * m + 1]
        return pair_halves(ref[pa % 8, :, cols], pa // 8, ref[pb % 8, :, cols], pb // 8)

    for t in R3:
        for m in R8:
            out_ref[:, t * D + m * L:t * D + (m + 1) * L] = pick(dw_ref, t, m)

    @pl.when(pl.program_id(0) == 0)
    def _():
        for t in R3:
            for m in R8:
                bias_ref[t * D + m * L:t * D + (m + 1) * L] = pick(bias_in_ref, t, m)[0]
        dg_ref[...] = small_ref[0]
        db_ref[...] = small_ref[1]
        dbo_ref[...] = small_ref[2]


def unpack_call(kind, dwg, dwo, small):
    vec = jax.ShapeDtypeStruct((D,), F32)
    one = lambda r, s: (0,)
    return pl.pallas_call(
        unpack_kernel,
        grid_spec=pltpu.PrefetchScalarGridSpec(
            num_scalar_prefetch=1,
            grid=(8,),
            in_specs=[pl.BlockSpec((8, L, W3), lambda r, s: (0, r, 0)), pl.BlockSpec((8, 8, W3), lambda r, s: (0, L, 0)),
                      pl.BlockSpec((L, D), lambda r, s: (r, 0)), pl.BlockSpec((8, D), lambda r, s: (0, 0))],
            out_specs=[pl.BlockSpec((L, D3), lambda r, s: (r, 0)), pl.BlockSpec((D3,), one),
                       pl.BlockSpec((L, D), lambda r, s: (r, 0))] + [pl.BlockSpec((D,), one)] * 3,
        ),
        out_shape=[jax.ShapeDtypeStruct((D, D3), F32), jax.ShapeDtypeStruct((D3,), F32),
                   jax.ShapeDtypeStruct((D, D), F32), vec, vec, vec],
        compiler_params=pltpu.CompilerParams(vmem_limit_bytes=VMEM_CAP),
        name="unpack",
    )(kind, dwg, dwg, dwo, small)


def solution(mesh):
    tok_spec = P(None, "sp", None)

    def local_block(x, d_y, ln_gamma, ln_beta, w_qkv, b_qkv, w_out, b_out, head_kind):
        hg, dog, sel = pre_call(head_kind, x, d_y, ln_gamma, ln_beta, w_out.reshape(N, 64, D))
        b3 = jnp.broadcast_to(b_qkv.reshape(24, 1, L), (24, 8, L))
        so, sd, dwp = attn_call(sel, hg.reshape(8, 2, QB, D), dog, w_qkv, b3)
        y, dx, small, dwg, dwo = post_call(
            head_kind, so, sd, dwp.reshape(2, HR, W3), x, d_y, ln_gamma, b_out, w_qkv, w_out)
        dw, dbias, dwout, dg, db, dbo = unpack_call(head_kind, dwg.reshape(8, DR, W3), dwo.reshape(D, D), small)
        return y, dx, dg, db, dw, dbias, dwout, dbo

    return jax.shard_map(
        local_block, mesh=mesh,
        in_specs=(tok_spec, tok_spec, P(), P(), P(), P(), P(), P(), P()),
        out_specs=(tok_spec, tok_spec, P(), P(), P(), P(), P(), P()), check_vma=False)
```

```python
import functools
import math

import jax
import jax.numpy as jnp
from jax import lax
from jax.experimental import pallas as pl
from jax.experimental.pallas import tpu as pltpu
from jax.sharding import PartitionSpec as P

LN_EPS = 1e-5
NEG_BIG = -1e30
BF = jnp.bfloat16
F32 = jnp.float32
QB = 256
L = 128
W3 = 384
T = 512
D = 1024
DR = 1040
HR = 520
N = 16
R3, R4, R8 = range(3), range(4), range(8)
MESH = pl.DeviceIdType.MESH
H_ROWS = (0, 96, 176, 256)
W_ROWS = (0, 176, 352, 520)
O_ROWS = (0, 24, 48, 64)
S = 2048
D3 = 3072
VMEM_CAP = 63 * D * D


def dot_nn(a, b):
    return lax.dot_general(a, b, (((1,), (0,)), ((), ())), preferred_element_type=F32)


def dot_nt(a, b):
    return lax.dot_general(a, b, (((1,), (1,)), ((), ())), preferred_element_type=F32)


def dot_tn(a, b):
    return lax.dot_general(a, b, (((0,), (0,)), ((), ())), preferred_element_type=F32)


def swap_halves(a):
    return jnp.concatenate([a[:, 64:], a[:, :64]], axis=1)


def pair_halves(a, a_half, b, b_half):
    lane = lax.broadcasted_iota(jnp.int32, a.shape, 1)
    a = jnp.where(a_half == 1, swap_halves(a), a)
    b = jnp.where(b_half == 0, swap_halves(b), b)
    return jnp.where(lane < 64, a, b)


class Place:
    def __init__(self):
        self.me = lax.axis_index("sp")
        self.core, self.chip = self.me % 2, self.me // 2
        self.sib = self.me + 1 - 2 * self.core
        bits = (self.chip % 2, self.chip // 2 % 2, self.chip // 4)
        self.step = [(1 - 2 * v) * w for v, w in zip(bits, (1, 2, 4))]

    def chip_at(self, axes):
        out = self.chip
        for a in axes:
            out = out + self.step[a]
        return out

    def next_dev(self, axis):
        return self.me + 2 * self.step[axis]


def rcopy(src, dst, send, recv, dev):
    return pltpu.make_async_remote_copy(
        src_ref=src, dst_ref=dst, send_sem=send, recv_sem=recv, device_id=(dev,), device_id_type=MESH)


def subsets(axes):
    out = [()]
    for a in axes:
        out += [v + (a,) for v in out]
    return out


class Tree:
    def __init__(self, place, own, slot, send, recv):
        self.place, self.own, self.slot, self.send, self.recv = place, own, slot, send, recv
        self.entries = []
        for s in R3:
            for p in R3:
                order = [(p + j) % 3 for j in R3]
                for sub in subsets(order[:s]):
                    self.entries.append((p, order[s], sub))

    def copy(self, e):
        p, axis, sub = e
        i = self.entries.index(e)
        at = self.slot(self.place.chip_at(sub), p)
        return rcopy(at if sub else self.own(p), at, self.send.at[i], self.recv.at[i], self.place.next_dev(axis))

    def start_own(self):
        for e in self.entries:
            if not e[2]:
                self.copy(e).start()

    def arrive(self, e):
        p, axis, sub = e
        got = sub + (axis,)
        chip = self.place.chip_at(got)
        at = self.slot(chip, p)
        i = self.entries.index(e)
        rcopy(at, at, self.send.at[i], self.recv.at[i], self.place.next_dev(axis)).wait_recv()
        for n in self.entries:
            if n[0] == p and n[2] == got:
                self.copy(n).start()
        return chip, p

    def level(self, s):
        return [e for e in self.entries if len(e[2]) <= s and (e[1] - e[0]) % 3 == s]

    def finish(self):
        for e in self.entries:
            self.copy(e).wait_send()


def barrier_signal(place):
    sem = pltpu.get_barrier_semaphore()
    for r in range(1, N):
        pl.semaphore_signal(sem, inc=1, device_id=((place.me + r) % N,), device_id_type=MESH)


def barrier_wait():
    pl.semaphore_wait(pltpu.get_barrier_semaphore(), N - 1)


def head_places(kind_ref):
    pos, zeros, ones = [], 0, 8
    for n in range(N):
        k = kind_ref[n]
        pos.append(jnp.where(k == 0, zeros, ones))
        zeros, ones = zeros + 1 - k, ones + k
    return pos


class Exchange:
    def __init__(self, place, src, dst, send, recv):
        self.place, self.src, self.dst, self.send, self.recv = place, src, dst, send, recv

    def copies(self):
        me = self.place.me
        for r in range(1, N):
            to = (me + r) % N
            yield rcopy(self.src(to), self.dst(me), self.send(r), self.recv(r), to)

    def start(self):
        for cp in self.copies():
            cp.start()

    def wait(self):
        for r in range(1, N):
            at = self.dst((self.place.me + N - r) % N)
            rcopy(at, at, self.send(r), self.recv(r), self.place.me).wait_recv()

    def finish(self):
        for cp in self.copies():
            cp.wait_send()


def gather_heads(recv_at, pos, b, m):
    pa, pb = pos[2 * m], pos[2 * m + 1]
    k, j = b // 2, b % 2
    a = recv_at(j, 2 * (pa % 8) + k)
    c = recv_at(j, 2 * (pb % 8) + k)
    return pair_halves(a, pa // 8, c, pb // 8)


def span(tab):
    return lambda p: pl.ds(tab[p], tab[p + 1] - tab[p])


def centre(xb):
    xf = xb.astype(F32)
    cen = xf - jnp.mean(xf, axis=-1, keepdims=True)
    rstd = lax.rsqrt(jnp.mean(cen * cen, axis=-1, keepdims=True) + LN_EPS)
    return xf, cen * rstd, rstd


def layer_kernel(kind_ref, x_ref, dy_ref, gamma_ref, beta_ref, bout_ref, b3_ref, wqkv_hbm, wout_hbm,
                 y_ref, dx_ref, small_ref, dwg_ref, dwo_ref,
                 hg_ref, out_ref, wout_ref, wp_ref, do_ref, dog_ref, w_ref, bias_ref, qkv_ref, dqkv_ref, qt_ref, dot_ref,
                 dkt_ref, dvt_ref, s_f, p_f, ds_f, s_g, p_g, ds_g, so_ref, sd_ref, ro_ref, rd_ref, o_nat, dqkv_nat,
                 dwp_ref, dws_ref, part_ref, px_ref, acc_ref, rs0_ref, rs1_ref, rs2_ref, sm_ref,
                 loc, sib_send, sib_recv, h_send, h_recv, do_send, do_recv, o_send, o_recv, d_send, d_recv,
                 s_send, s_recv, w_send, w_recv, g_send, g_recv, ws_send, ws_recv, gs_send, gs_recv, r_send, r_recv):
    pc = Place()
    barrier_signal(pc)

    def w_load(r):
        return pltpu.make_async_copy(wqkv_hbm.at[r * T:(r + 1) * T], dqkv_nat, loc.at[r])

    wo_load = pltpu.make_async_copy(wout_hbm, wout_ref, loc.at[2])
    w_load(0).start()
    wo_load.start()
    gamma = gamma_ref[...].reshape(1, D).astype(F32)
    beta = beta_ref[...].reshape(1, D).astype(F32)
    bout = bout_ref[...].reshape(1, D).astype(F32)

    def rows_of(core):
        return pl.ds(pl.multiple_of(core * L, L), L)

    def norm(xb):
        return (centre(xb)[1] * gamma + beta).astype(BF)

    def sib_copy(j):
        return rcopy(out_ref.at[j], hg_ref.at[pc.chip, j, rows_of(pc.core)], sib_send.at[j], sib_recv.at[j], pc.sib)

    for j in range(2):
        out_ref[j] = norm(x_ref[2 * (1 - pc.core) + j])
    for j in range(2):
        hg_ref[pc.chip, j, rows_of(pc.core)] = norm(x_ref[2 * pc.core + j])
    barrier_wait()
    for j in range(2):
        sib_copy(j).start()

    h_rows, w_rows, o_rows = span(H_ROWS), span(W_ROWS), span(O_ROWS)

    def h_tree(j):
        slot = lambda c, p: hg_ref.at[c, j, h_rows(p)]
        return Tree(pc, lambda p: slot(pc.chip, p), slot, h_send.at[j], h_recv.at[j])

    def sib_arrive(j):
        at = hg_ref.at[pc.chip, j, rows_of(1 - pc.core)]
        rcopy(at, at, sib_send.at[j], sib_recv.at[j], pc.sib).wait_recv()

    do_out = do_ref.reshape(N, 2, L, L)

    def swap(src, dst, send, recv, j):
        return Exchange(pc, lambda t: src(t, j), lambda t: dst.at[j, t], lambda r: send.at[j, r], lambda r: recv.at[j, r])

    def do_swap(j):
        return swap(lambda t, j: do_out.at[t, j], dog_ref, do_send, do_recv, j)

    def o_swap(j):
        return swap(lambda t, j: so_ref.at[j, t], ro_ref, o_send, o_recv, j)

    def d_swap(j):
        return swap(lambda t, j: sd_ref.at[j, t], rd_ref, d_send, d_recv, j)

    trees = [h_tree(0), h_tree(1)]
    sib_arrive(0)
    trees[0].start_own()
    pos = head_places(kind_ref)
    perm = []
    for j in range(N):
        v = 0
        for n in range(1, N):
            v = v + jnp.where(pos[n] == j, n, 0)
        perm.append(v)
    f = g = 0
    for c in R8:
        f = f + jnp.where(pc.chip == c, perm[c], 0)
        g = g + jnp.where(pc.chip == c, perm[8 + c], 0)
    wo_load.wait()
    dy_all = dy_ref[...].reshape(T, D)
    for c in R4:
        for u in range(2):
            wp_ref[u * L:u * L + 64] = wout_ref[perm[2 * c + u]]
            wp_ref[u * L + 64:u * L + L] = wout_ref[perm[8 + 2 * c + u]]
        d = dot_nt(dy_all, wp_ref[...]).astype(BF)
        for u in range(2):
            do_ref[2 * c + u] = d[:, u * L:(u + 1) * L].reshape(4, L, L)
    for e in trees[0].level(0):
        trees[0].arrive(e)
    do_swap(0).start()
    for j in range(2):
        dog_ref[j, pc.me] = do_out[pc.me, j]

    def w_cols(t, k, head):
        out = None
        for m in R8:
            cur = dqkv_nat[k * L:(k + 1) * L, t * D + m * L:t * D + (m + 1) * L]
            out = cur if out is None else jnp.where(head // 2 == m, cur, out)
        return out

    for r in range(2):
        w_load(r).wait()
        for t in R3:
            for k in R4:
                w_ref[r * T + k * L:r * T + (k + 1) * L, t * L:(t + 1) * L] = pair_halves(
                    w_cols(t, k, f), f % 2, w_cols(t, k, g), g % 2)
        if r == 0:
            w_load(1).start()
    for t in R3:
        bias_ref[:, t * L:(t + 1) * L] = pair_halves(
            b3_ref[t * 8 + f // 2].astype(F32), f % 2, b3_ref[t * 8 + g // 2].astype(F32), g % 2)
    dwp_ref[...] = jnp.zeros_like(dwp_ref)
    for e in trees[0].level(1):
        trees[0].arrive(e)
    sib_arrive(1)
    trees[1].start_own()
    for e in trees[0].level(2):
        trees[0].arrive(e)
    do_swap(0).wait()

    lane = lax.broadcasted_iota(jnp.int32, (QB, L), 1)
    row_i = lax.broadcasted_iota(jnp.int32, (QB, QB), 0)
    col_i = lax.broadcasted_iota(jnp.int32, (QB, QB), 1)

    def head_block(j, i, hd):
        s_ref, p_ref, ds_ref = ((s_f, p_f, ds_f), (s_g, p_g, ds_g))[hd]
        first = 0 if hd == 0 else max(0, i - 2)
        blocks = range(first, i + 1)
        mine = (lane < 64) if hd == 0 else (lane >= 64)
        qi = qkv_ref[i * QB:(i + 1) * QB, 0:L] * BF(0.125)
        doi = dog_ref[j, 2 * i:2 * i + 2].reshape(QB, L)
        qm = jnp.where(mine, qi, BF(0))
        dom = jnp.where(mine, doi, BF(0))
        k_at = lambda kb: qkv_ref[kb * QB:(kb + 1) * QB, L:2 * L]
        v_at = lambda kb: qkv_ref[kb * QB:(kb + 1) * QB, 2 * L:3 * L]
        at = lambda kb: slice((kb - first) * QB, (kb - first + 1) * QB)
        mx = None
        for kb in blocks:
            s = dot_nt(qm, k_at(kb))
            if kb == i:
                s = jnp.where(col_i <= row_i, s, NEG_BIG)
            if hd == 1 and kb == i - 2:
                s = jnp.where(col_i > row_i, s, NEG_BIG)
            s_ref[:, at(kb)] = s
            cur = jnp.maximum(s[:, :L], s[:, L:])
            mx = cur if mx is None else jnp.maximum(mx, cur)
        m = jnp.max(mx, axis=1, keepdims=True)
        ls = None
        for kb in blocks:
            e = jnp.exp(s_ref[:, at(kb)] - m)
            s_ref[:, at(kb)] = e
            cur = e[:, :L] + e[:, L:]
            ls = cur if ls is None else ls + cur
        rl = 1.0 / jnp.sum(ls, axis=1, keepdims=True)
        acc = None
        for kb in blocks:
            p_ = s_ref[:, at(kb)] * rl
            s_ref[:, at(kb)] = p_
            pb = p_.astype(BF)
            p_ref[:, at(kb)] = pb
            cur = dot_nn(pb, v_at(kb))
            acc = cur if acc is None else acc + cur
        dsum = jnp.sum(dom.astype(F32) * acc, axis=1, keepdims=True)
        dq = None
        for kb in blocks:
            dp = dot_nt(dom, v_at(kb)).astype(BF).astype(F32)
            ds = (s_ref[:, at(kb)] * (dp - dsum)).astype(BF)
            ds_ref[:, at(kb)] = ds
            cur = dot_nn(ds, k_at(kb))
            dq = cur if dq is None else dq + cur
        hr = slice(hd * 64, hd * 64 + 64)
        n = len(blocks) * QB
        keys = slice(first * QB, first * QB + n)
        dvt_ref[hr, keys] += dot_nn(dot_ref[hr, i * QB:(i + 1) * QB], p_ref[:, :n])
        dkt_ref[hr, keys] += dot_nn(qt_ref[hr, i * QB:(i + 1) * QB], ds_ref[:, :n])
        return acc, dq * 0.125

    def batch_step(j, carry):
        def qkv_step(r, c):
            rows = hg_ref[pl.ds(2 * r, 2), j].reshape(T, D)
            out = dot_nn(rows, w_ref[...]) + bias_ref[0:1, :]
            qkv_ref[pl.ds(pl.multiple_of(r * T, T), T), :] = out.astype(BF)
            return c

        lax.fori_loop(0, 4, qkv_step, 0)

        @pl.when(j == 0)
        def _():
            for e in trees[1].level(0):
                trees[1].arrive(e)
            do_swap(1).start()

        for i in R8:
            qs = qkv_ref[i * QB:(i + 1) * QB, 0:L] * BF(0.125)
            qt_ref[:, i * QB:(i + 1) * QB] = qs.T
            dot_ref[:, i * QB:(i + 1) * QB] = dog_ref[j, 2 * i:2 * i + 2].reshape(QB, L).T
        dkt_ref[...] = jnp.zeros_like(dkt_ref)
        dvt_ref[...] = jnp.zeros_like(dvt_ref)
        for i in R8:
            of, dqf = head_block(j, i, 0)
            og, dqg = head_block(j, i, 1)
            o = jnp.where(lane < 64, of, og).astype(BF)
            dq = jnp.where(lane < 64, dqf, dqg).astype(BF)
            for u in range(2):
                so_ref[j, 2 * i + u] = o[u * L:(u + 1) * L]
                sd_ref[j, 2 * i + u, 0] = dq[u * L:(u + 1) * L]
            dqkv_ref[i * QB:(i + 1) * QB, 0:L] = dq
            if i == 4:
                @pl.when(j == 0)
                def _():
                    for e in trees[1].level(1):
                        trees[1].arrive(e)
        for t, src in ((1, dkt_ref), (2, dvt_ref)):
            for n in range(N):
                d = src[:, n * L:(n + 1) * L].T.astype(BF)
                sd_ref[j, n, t] = d
                dqkv_ref[n * L:(n + 1) * L, t * L:(t + 1) * L] = d
        o_swap(j).start()
        d_swap(j).start()
        ro_ref[j, pc.me] = so_ref[j, pc.me]
        rd_ref[j, pc.me] = sd_ref[j, pc.me]

        def dw_step(r, c):
            cols = pl.ds(pl.multiple_of(r * QB, QB), QB)
            dwp_ref[cols, :] += dot_tn(hg_ref[:, j, :, cols].reshape(S, QB), dqkv_ref[...])
            return c

        lax.fori_loop(0, 4, dw_step, 0)
        dwp_ref[D:D + 1, :] += jnp.sum(dqkv_ref[...].astype(F32), axis=0, keepdims=True)

        @pl.when(j == 0)
        def _():
            for e in trees[1].level(2):
                trees[1].arrive(e)
            do_swap(1).wait()

        return carry

    lax.fori_loop(0, 2, batch_step, 0)

    def half_of(core):
        return dwp_ref.at[pl.ds(pl.multiple_of(core * HR, 8), HR)]

    sends = []

    def to_sib(n, src, dst, send, recv):
        cp = rcopy(src, dst, send.at[n], recv.at[n], pc.sib)
        cp.start()
        sends.append(cp)
        return cp

    half = to_sib(2, half_of(1 - pc.core), dws_ref, sib_send, sib_recv)
    for j in range(2):
        trees[j].finish()
        do_swap(j).finish()
    w_flat = hg_ref.reshape(2 * S, D)
    w_loads = [pltpu.make_async_copy(wqkv_hbm.at[:, t * D:(t + 1) * D], w_flat.at[t * D:(t + 1) * D], loc.at[3 + t]) for t in R3]
    for cp in w_loads:
        cp.start()
    for j in range(2):
        o_swap(j).wait()
    for b in R4:
        for m in R8:
            o_nat[b * L:(b + 1) * L, m * L:(m + 1) * L] = gather_heads(lambda j, q: ro_ref[j, q], pos, b, m)

    def wout_part(core, c):
        cols = pl.ds(pl.multiple_of(core * T + c * QB, QB), QB)
        return dot_tn(o_nat[:, cols], dy_all)

    for c in range(2):
        part_ref[c * QB:(c + 1) * QB] = wout_part(1 - pc.core, c)
    xp = to_sib(3, part_ref, px_ref, sib_send, sib_recv)
    for c in range(2):
        acc_ref[4 * c:4 * c + 4] = wout_part(pc.core, c).reshape(4, 64, D)
    xp.wait_recv()
    acc_ref[...] += px_ref[...].reshape(8, 64, D)

    bufs = (rs0_ref, rs1_ref, rs2_ref)

    def reduce_step(s, wait):
        for p in R3:
            order = [(p + j) % 3 for j in R3]
            for i, sub in enumerate(subsets(order[s + 1:])):
                n = p * 7 + (0, 4, 6)[s] + i
                dst = bufs[s].at[i, o_rows(p)]
                if not wait:
                    cp = rcopy(acc_ref.at[pc.chip_at((order[s],) + sub), o_rows(p)], dst,
                               r_send.at[n], r_recv.at[n], pc.next_dev(order[s]))
                    cp.start()
                    sends.append(cp)
                else:
                    rcopy(dst, dst, r_send.at[n], r_recv.at[n], pc.sib).wait_recv()
                    acc_ref[pc.chip_at(sub), o_rows(p)] += bufs[s][i, o_rows(p)]

    reduce_step(0, False)
    half.wait_recv()
    dws_ref[...] += half_of(pc.core)[...]

    def w_slot(c, p, core=pc.core):
        return dwg_ref.at[c, core, w_rows(p)]

    def g_slot(c, p, core=pc.core):
        return dwo_ref.at[core, c, o_rows(p)]

    wtree = Tree(pc, lambda p: dws_ref.at[w_rows(p)], w_slot, w_send, w_recv)
    wtree.start_own()
    keep_w = pltpu.make_async_copy(dws_ref, dwg_ref.at[pc.chip, pc.core], loc.at[0])
    keep_w.start()
    for p in R3:
        to_sib(p, dws_ref.at[w_rows(p)], w_slot(pc.chip, p), ws_send, ws_recv)

    def pass_on(tree, slot, s, send, recv):
        for e in tree.level(s):
            c, p = tree.arrive(e)
            to_sib(3 + tree.entries.index(e), slot(c, p), slot(c, p), send, recv)

    dbo = jnp.zeros((1, D), F32)
    for b in R4:
        rows = slice(b * L, (b + 1) * L)
        y_ref[b] = (x_ref[b].astype(F32) + dot_nn(o_nat[rows], wout_ref.reshape(D, D)[...]) + bout).astype(BF)
        dbo += jnp.sum(dy_ref[b].astype(F32), axis=0, keepdims=True)
    for j in range(2):
        d_swap(j).wait()
    reduce_step(0, True)
    reduce_step(1, False)
    pass_on(wtree, w_slot, 0, ws_send, ws_recv)
    for b in R4:
        for m in R8:
            for t in R3:
                dqkv_nat[b * L:(b + 1) * L, t * D + m * L:t * D + (m + 1) * L] = gather_heads(
                    lambda j, q: rd_ref[j, q, t], pos, b, m)
    for cp in w_loads:
        cp.wait()
    reduce_step(1, True)
    reduce_step(2, False)
    dg = jnp.zeros((1, D), F32)
    db = jnp.zeros((1, D), F32)
    for b in R4:
        rows = slice(b * L, (b + 1) * L)
        _, xhat, rstd = centre(x_ref[b])
        dh = None
        for t in R3:
            cur = dot_nt(dqkv_nat[rows, t * D:(t + 1) * D], w_flat[t * D:(t + 1) * D])
            dh = cur if dh is None else dh + cur
        dh = dh.astype(BF).astype(F32)
        dg += jnp.sum(dh * xhat, axis=0, keepdims=True)
        db += jnp.sum(dh, axis=0, keepdims=True)
        dxh = dh * gamma
        m1 = jnp.mean(dxh, axis=-1, keepdims=True)
        m2 = jnp.mean(dxh * xhat, axis=-1, keepdims=True)
        dx_ref[b] = (dy_ref[b].astype(F32) + rstd * (dxh - m1 - xhat * m2)).astype(BF)
    row = lax.broadcasted_iota(jnp.int32, (8, D), 0)
    sm_ref[pc.me] = jnp.where(row == 0, dg, jnp.where(row == 1, db, jnp.where(row == 2, dbo, 0.0)))
    s_swap = Exchange(pc, lambda t: sm_ref.at[pc.me], lambda t: sm_ref.at[t], lambda r: s_send.at[r], lambda r: s_recv.at[r])
    s_swap.start()
    reduce_step(2, True)
    gtree = Tree(pc, lambda p: acc_ref.at[pc.chip, o_rows(p)], g_slot, g_send, g_recv)
    gtree.start_own()
    keep_g = pltpu.make_async_copy(acc_ref.at[pc.chip], dwo_ref.at[pc.core, pc.chip], loc.at[1])
    keep_g.start()
    for p in R3:
        to_sib(p, acc_ref.at[pc.chip, o_rows(p)], g_slot(pc.chip, p), gs_send, gs_recv)
    pass_on(wtree, w_slot, 1, ws_send, ws_recv)
    pass_on(gtree, g_slot, 0, gs_send, gs_recv)
    pass_on(gtree, g_slot, 1, gs_send, gs_recv)
    s_swap.wait()
    tot = sm_ref[0]
    for n in range(1, N):
        tot = tot + sm_ref[n]
    small_ref[...] = tot
    pass_on(wtree, w_slot, 2, ws_send, ws_recv)
    pass_on(gtree, g_slot, 2, gs_send, gs_recv)
    for tree, slot, send, recv in ((wtree, w_slot, ws_send, ws_recv), (gtree, g_slot, gs_send, gs_recv)):
        for p in R3:
            at = slot(pc.chip, p, 1 - pc.core)
            rcopy(at, at, send.at[p], recv.at[p], pc.sib).wait_recv()
        for i, (p, axis, sub) in enumerate(tree.entries):
            at = slot(pc.chip_at(sub + (axis,)), p, 1 - pc.core)
            rcopy(at, at, send.at[3 + i], recv.at[3 + i], pc.sib).wait_recv()
        tree.finish()
    for j in range(2):
        sib_copy(j).wait_send()
        o_swap(j).finish()
        d_swap(j).finish()
    s_swap.finish()
    for cp in sends:
        cp.wait_send()
    keep_w.wait()
    keep_g.wait()


def layer_call(kind, x, dy, gamma, beta, bout, b3, wqkv, wout):
    vm, sm, hb = (pl.BlockSpec(memory_space=m) for m in (pltpu.VMEM, pltpu.SMEM, pl.ANY))
    sem = pltpu.SemaphoreType.DMA
    tok = jax.ShapeDtypeStruct((4, L, D), BF)

    def pair(*n):
        return [sem(n), sem(n)]

    def bf(*n):
        return pltpu.VMEM(n, BF)

    def ff(*n):
        return pltpu.VMEM(n, F32)

    band = 3 * QB
    return pl.pallas_call(
        layer_kernel,
        out_shape=(tok, tok, jax.ShapeDtypeStruct((8, D), F32), jax.ShapeDtypeStruct((8, 2, HR, W3), F32),
                   jax.ShapeDtypeStruct((2, 8, 64, D), F32)),
        in_specs=[sm] + [vm] * 6 + [hb, hb],
        out_specs=(vm, vm, vm, hb, hb),
        scratch_shapes=[
            bf(8, 2, QB, D), bf(2, L, D), bf(N, 64, D), bf(QB, D), bf(8, 4, L, L), bf(2, N, L, L), bf(D, W3), ff(8, W3),
            bf(S, W3), bf(S, W3), bf(L, S), bf(L, S), ff(L, S), ff(L, S),
            ff(QB, S), bf(QB, S), bf(QB, S), ff(QB, band), bf(QB, band), bf(QB, band),
            bf(2, N, L, L), bf(2, N, 3, L, L), bf(2, N, L, L), bf(2, N, 3, L, L), bf(T, D), bf(T, D3),
            ff(DR, W3), ff(HR, W3), ff(T, D), ff(T, D), ff(8, 64, D),
            ff(4, 64, D), ff(2, 64, D), ff(1, 64, D), ff(N, 8, D), sem((6,))]
        + pair(4) + pair(2, 21) + pair(2, N) + pair(2, N) + pair(2, N) + pair(N)
        + pair(21) + pair(21) + pair(24) + pair(24) + pair(21),
        compiler_params=pltpu.CompilerParams(vmem_limit_bytes=VMEM_CAP, collective_id=0, has_side_effects=True),
        name="layer",
    )(kind, x, dy, gamma, beta, bout, b3, wqkv, wout)


def unpack_kernel(kind_ref, dw_ref, bias_in_ref, dwo_ref, small_ref, out_ref, bias_ref, wo_ref, dg_ref, db_ref, dbo_ref):
    pos = head_places(kind_ref)
    wo_ref[...] = dwo_ref[...]

    def pick(ref, t, m):
        cols = slice(t * L, (t + 1) * L)
        pa, pb = pos[2 * m], pos[2 * m + 1]
        return pair_halves(ref[pa % 8, :, cols], pa // 8, ref[pb % 8, :, cols], pb // 8)

    for t in R3:
        for m in R8:
            out_ref[:, t * D + m * L:t * D + (m + 1) * L] = pick(dw_ref, t, m)

    @pl.when(pl.program_id(0) == 0)
    def _():
        for t in R3:
            for m in R8:
                bias_ref[t * D + m * L:t * D + (m + 1) * L] = pick(bias_in_ref, t, m)[0]
        dg_ref[...] = small_ref[0]
        db_ref[...] = small_ref[1]
        dbo_ref[...] = small_ref[2]


def unpack_call(kind, dwg, dwo, small):
    vec = jax.ShapeDtypeStruct((D,), F32)
    one = lambda r, s: (0,)
    return pl.pallas_call(
        unpack_kernel,
        grid_spec=pltpu.PrefetchScalarGridSpec(
            num_scalar_prefetch=1,
            grid=(8,),
            in_specs=[pl.BlockSpec((8, L, W3), lambda r, s: (0, r, 0)), pl.BlockSpec((8, 8, W3), lambda r, s: (0, L, 0)),
                      pl.BlockSpec((L, D), lambda r, s: (r, 0)), pl.BlockSpec((8, D), lambda r, s: (0, 0))],
            out_specs=[pl.BlockSpec((L, D3), lambda r, s: (r, 0)), pl.BlockSpec((D3,), one),
                       pl.BlockSpec((L, D), lambda r, s: (r, 0))] + [pl.BlockSpec((D,), one)] * 3,
        ),
        out_shape=[jax.ShapeDtypeStruct((D, D3), F32), jax.ShapeDtypeStruct((D3,), F32),
                   jax.ShapeDtypeStruct((D, D), F32), vec, vec, vec],
        compiler_params=pltpu.CompilerParams(vmem_limit_bytes=VMEM_CAP),
        name="unpack",
    )(kind, dwg, dwg, dwo, small)


def solution(mesh):
    tok_spec = P(None, "sp", None)

    def local_block(x, d_y, ln_gamma, ln_beta, w_qkv, b_qkv, w_out, b_out, head_kind):
        b3 = jnp.broadcast_to(b_qkv.reshape(24, 1, L), (24, 8, L))
        y, dx, small, dwg, dwo = layer_call(head_kind, x, d_y, ln_gamma, ln_beta, b_out, b3, w_qkv, w_out.reshape(N, 64, D))
        dw, dbias, dwout, dg, db, dbo = unpack_call(head_kind, dwg.reshape(8, DR, W3), dwo.reshape(D, D), small)
        return y, dx, dg, db, dw, dbias, dwout, dbo

    return jax.shard_map(
        local_block, mesh=mesh,
        in_specs=(tok_spec, tok_spec, P(), P(), P(), P(), P(), P(), P()),
        out_specs=(tok_spec, tok_spec, P(), P(), P(), P(), P(), P()), check_vma=False)
```

```python
import functools
import math

import jax
import jax.numpy as jnp
from jax import lax
from jax.experimental import pallas as pl
from jax.experimental.pallas import tpu as pltpu
from jax.sharding import PartitionSpec as P

LN_EPS = 1e-5
NEG_BIG = -1e30
BF = jnp.bfloat16
F32 = jnp.float32
QB = 256
L = 128
W3 = 384
T = 512
D = 1024
DR = 1040
HR = 520
N = 16
R3, R4, R8 = range(3), range(4), range(8)
MESH = pl.DeviceIdType.MESH
H_ROWS = (0, 96, 176, 256)
W_ROWS = (0, 176, 352, 520)
O_ROWS = (0, 24, 48, 64)
S = 2048
D3 = 3072
VMEM_CAP = 63 * D * D


def dot_nn(a, b):
    return lax.dot_general(a, b, (((1,), (0,)), ((), ())), preferred_element_type=F32)


def dot_nt(a, b):
    return lax.dot_general(a, b, (((1,), (1,)), ((), ())), preferred_element_type=F32)


def dot_tn(a, b):
    return lax.dot_general(a, b, (((0,), (0,)), ((), ())), preferred_element_type=F32)


def swap_halves(a):
    return jnp.concatenate([a[:, 64:], a[:, :64]], axis=1)


def pair_halves(a, a_half, b, b_half):
    lane = lax.broadcasted_iota(jnp.int32, a.shape, 1)
    a = jnp.where(a_half == 1, swap_halves(a), a)
    b = jnp.where(b_half == 0, swap_halves(b), b)
    return jnp.where(lane < 64, a, b)


class Place:
    def __init__(self):
        self.me = lax.axis_index("sp")
        self.core, self.chip = self.me % 2, self.me // 2
        self.sib = self.me + 1 - 2 * self.core
        bits = (self.chip % 2, self.chip // 2 % 2, self.chip // 4)
        self.step = [(1 - 2 * v) * w for v, w in zip(bits, (1, 2, 4))]

    def chip_at(self, axes):
        out = self.chip
        for a in axes:
            out = out + self.step[a]
        return out

    def next_dev(self, axis):
        return self.me + 2 * self.step[axis]


def rcopy(src, dst, send, recv, dev):
    return pltpu.make_async_remote_copy(
        src_ref=src, dst_ref=dst, send_sem=send, recv_sem=recv, device_id=(dev,), device_id_type=MESH)


def subsets(axes):
    out = [()]
    for a in axes:
        out += [v + (a,) for v in out]
    return out


class Tree:
    def __init__(self, place, own, slot, send, recv):
        self.place, self.own, self.slot, self.send, self.recv = place, own, slot, send, recv
        self.entries = []
        for s in R3:
            for p in R3:
                order = [(p + j) % 3 for j in R3]
                for sub in subsets(order[:s]):
                    self.entries.append((p, order[s], sub))

    def copy(self, e):
        p, axis, sub = e
        i = self.entries.index(e)
        at = self.slot(self.place.chip_at(sub), p)
        return rcopy(at if sub else self.own(p), at, self.send.at[i], self.recv.at[i], self.place.next_dev(axis))

    def start_own(self):
        for e in self.entries:
            if not e[2]:
                self.copy(e).start()

    def arrive(self, e):
        p, axis, sub = e
        got = sub + (axis,)
        chip = self.place.chip_at(got)
        at = self.slot(chip, p)
        i = self.entries.index(e)
        rcopy(at, at, self.send.at[i], self.recv.at[i], self.place.next_dev(axis)).wait_recv()
        for n in self.entries:
            if n[0] == p and n[2] == got:
                self.copy(n).start()
        return chip, p

    def hops(self, n):
        return [e for e in self.entries if len(e[2]) == n]

    def finish(self):
        for e in self.entries:
            self.copy(e).wait_send()


def barrier_signal(place):
    sem = pltpu.get_barrier_semaphore()
    for r in range(1, N):
        pl.semaphore_signal(sem, inc=1, device_id=((place.me + r) % N,), device_id_type=MESH)


def barrier_wait():
    pl.semaphore_wait(pltpu.get_barrier_semaphore(), N - 1)


def head_places(kind_ref):
    pos, zeros, ones = [], 0, 8
    for n in range(N):
        k = kind_ref[n]
        pos.append(jnp.where(k == 0, zeros, ones))
        zeros, ones = zeros + 1 - k, ones + k
    return pos


class Exchange:
    def __init__(self, place, src, dst, send, recv):
        self.place, self.src, self.dst, self.send, self.recv = place, src, dst, send, recv

    def copies(self):
        me = self.place.me
        for r in range(1, N):
            to = (me + r) % N
            yield rcopy(self.src(to), self.dst(me), self.send(r), self.recv(r), to)

    def start(self):
        for cp in self.copies():
            cp.start()

    def wait(self):
        for r in range(1, N):
            at = self.dst((self.place.me + N - r) % N)
            rcopy(at, at, self.send(r), self.recv(r), self.place.me).wait_recv()

    def finish(self):
        for cp in self.copies():
            cp.wait_send()


def gather_heads(recv_at, pos, b, m):
    pa, pb = pos[2 * m], pos[2 * m + 1]
    k, j = b // 2, b % 2
    a = recv_at(j, 2 * (pa % 8) + k)
    c = recv_at(j, 2 * (pb % 8) + k)
    return pair_halves(a, pa // 8, c, pb // 8)


def span(tab):
    return lambda p: pl.ds(tab[p], tab[p + 1] - tab[p])


def centre(xb):
    xf = xb.astype(F32)
    cen = xf - jnp.mean(xf, axis=-1, keepdims=True)
    rstd = lax.rsqrt(jnp.mean(cen * cen, axis=-1, keepdims=True) + LN_EPS)
    return xf, cen * rstd, rstd


class Marks:
    def __init__(self):
        self.cur = None

    def __call__(self, name):
        if self.cur is not None:
            self.cur.__exit__(None, None, None)
        self.cur = None
        if name is not None:
            self.cur = jax.named_scope(name)
            self.cur.__enter__()


def layer_kernel(kind_ref, x_ref, dy_ref, gamma_ref, beta_ref, bout_ref, bqkv_ref, wqkv_hbm, wout_hbm,
                 y_ref, dx_ref, small_ref, dwg_ref, dwo_ref,
                 hg_ref, out_ref, wout_ref, wp_ref, do_ref, dog_ref, w_ref, bias_ref, qkv_ref, dqkv_ref, qt_ref, dot_ref,
                 dkt_ref, dvt_ref, s_f, p_f, ds_f, s_g, p_g, ds_g, so_ref, sd_ref, ro_ref, rd_ref, o_nat, dqkv_nat,
                 dwp_ref, dws_ref, part_ref, px_ref, acc_ref, rs0_ref, rs1_ref, rs2_ref, sm_ref,
                 loc, sib_send, sib_recv, h_send, h_recv, do_send, do_recv, o_send, o_recv, d_send, d_recv,
                 s_send, s_recv, w_send, w_recv, g_send, g_recv, ws_send, ws_recv, gs_send, gs_recv, r_send, r_recv):
    pc = Place()
    mk, mj = Marks(), Marks()
    barrier_signal(pc)

    def w_load(r):
        return pltpu.make_async_copy(wqkv_hbm.at[r * T:(r + 1) * T], dqkv_nat, loc.at[r])

    wo_load = pltpu.make_async_copy(wout_hbm, wout_ref, loc.at[2])
    w_load(0).start()
    wo_load.start()
    gamma = gamma_ref[...].reshape(1, D).astype(F32)
    beta = beta_ref[...].reshape(1, D).astype(F32)
    bout = bout_ref[...].reshape(1, D).astype(F32)
    bqkv = bqkv_ref[...].reshape(1, D3).astype(F32)

    def rows_of(core):
        return pl.ds(pl.multiple_of(core * L, L), L)

    def norm(xb):
        return (centre(xb)[1] * gamma + beta).astype(BF)

    def sib_copy(j):
        return rcopy(out_ref.at[j], hg_ref.at[pc.chip, j, rows_of(pc.core)], sib_send.at[j], sib_recv.at[j], pc.sib)

    for j in range(2):
        out_ref[j] = norm(x_ref[2 * (1 - pc.core) + j])
    for j in range(2):
        hg_ref[pc.chip, j, rows_of(pc.core)] = norm(x_ref[2 * pc.core + j])
    mk('barrier')
    barrier_wait()
    for j in range(2):
        sib_copy(j).start()

    h_rows, w_rows, o_rows = span(H_ROWS), span(W_ROWS), span(O_ROWS)

    def h_tree(j):
        slot = lambda c, p: hg_ref.at[c, j, h_rows(p)]
        return Tree(pc, lambda p: slot(pc.chip, p), slot, h_send.at[j], h_recv.at[j])

    def sib_arrive(j):
        at = hg_ref.at[pc.chip, j, rows_of(1 - pc.core)]
        rcopy(at, at, sib_send.at[j], sib_recv.at[j], pc.sib).wait_recv()

    do_out = do_ref.reshape(N, 2, L, L)

    def swap(src, dst, send, recv, j):
        return Exchange(pc, lambda t: src(t, j), lambda t: dst.at[j, t], lambda r: send.at[j, r], lambda r: recv.at[j, r])

    def do_swap(j):
        return swap(lambda t, j: do_out.at[t, j], dog_ref, do_send, do_recv, j)

    def o_swap(j):
        return swap(lambda t, j: so_ref.at[j, t], ro_ref, o_send, o_recv, j)

    def d_swap(j):
        return swap(lambda t, j: sd_ref.at[j, t], rd_ref, d_send, d_recv, j)

    mk('sibwait')
    trees = [h_tree(0), h_tree(1)]
    sib_arrive(0)
    trees[0].start_own()
    pos = head_places(kind_ref)
    perm = []
    for j in range(N):
        v = 0
        for n in range(1, N):
            v = v + jnp.where(pos[n] == j, n, 0)
        perm.append(v)
    f = g = 0
    for c in R8:
        f = f + jnp.where(pc.chip == c, perm[c], 0)
        g = g + jnp.where(pc.chip == c, perm[8 + c], 0)
    mk('dO_mm')
    wo_load.wait()
    dy_all = dy_ref[...].reshape(T, D)
    for c in R4:
        for u in range(2):
            wp_ref[u * L:u * L + 64] = wout_ref[perm[2 * c + u]]
            wp_ref[u * L + 64:u * L + L] = wout_ref[perm[8 + 2 * c + u]]
        d = dot_nt(dy_all, wp_ref[...]).astype(BF)
        for u in range(2):
            do_ref[2 * c + u] = d[:, u * L:(u + 1) * L].reshape(4, L, L)
    mk('t0_h0')
    for e in trees[0].hops(0):
        trees[0].arrive(e)
    mk('wsel')
    do_swap(0).start()
    for j in range(2):
        dog_ref[j, pc.me] = do_out[pc.me, j]

    def w_cols(t, k, head):
        out = None
        for m in R8:
            cur = dqkv_nat[k * L:(k + 1) * L, t * D + m * L:t * D + (m + 1) * L]
            out = cur if out is None else jnp.where(head // 2 == m, cur, out)
        return out

    for r in range(2):
        w_load(r).wait()
        for t in R3:
            for k in R4:
                w_ref[r * T + k * L:r * T + (k + 1) * L, t * L:(t + 1) * L] = pair_halves(
                    w_cols(t, k, f), f % 2, w_cols(t, k, g), g % 2)
        if r == 0:
            w_load(1).start()
    for t in R3:
        halves = []
        for head in (f, g):
            out = None
            for m in R8:
                cur = bqkv[:, t * D + m * L:t * D + (m + 1) * L]
                out = cur if out is None else jnp.where(head // 2 == m, cur, out)
            halves += [out, head % 2]
        bias_ref[:, t * L:(t + 1) * L] = jnp.broadcast_to(pair_halves(*halves), (8, L))
    dwp_ref[...] = jnp.zeros_like(dwp_ref)
    mk('t0_h1')
    for e in trees[0].hops(1):
        trees[0].arrive(e)
    sib_arrive(1)
    trees[1].start_own()

    lane = lax.broadcasted_iota(jnp.int32, (QB, L), 1)
    row_i = lax.broadcasted_iota(jnp.int32, (QB, QB), 0)
    col_i = lax.broadcasted_iota(jnp.int32, (QB, QB), 1)

    def head_block(j, i, hd):
        s_ref, p_ref, ds_ref = ((s_f, p_f, ds_f), (s_g, p_g, ds_g))[hd]
        first = 0 if hd == 0 else max(0, i - 2)
        blocks = range(first, i + 1)
        mine = (lane < 64) if hd == 0 else (lane >= 64)
        qi = qkv_ref[i * QB:(i + 1) * QB, 0:L] * BF(0.125)
        doi = dog_ref[j, 2 * i:2 * i + 2].reshape(QB, L)
        qm = jnp.where(mine, qi, BF(0))
        dom = jnp.where(mine, doi, BF(0))
        k_at = lambda kb: qkv_ref[kb * QB:(kb + 1) * QB, L:2 * L]
        v_at = lambda kb: qkv_ref[kb * QB:(kb + 1) * QB, 2 * L:3 * L]
        at = lambda kb: slice((kb - first) * QB, (kb - first + 1) * QB)
        mx = None
        for kb in blocks:
            s = dot_nt(qm, k_at(kb))
            if kb == i:
                s = jnp.where(col_i <= row_i, s, NEG_BIG)
            if hd == 1 and kb == i - 2:
                s = jnp.where(col_i > row_i, s, NEG_BIG)
            s_ref[:, at(kb)] = s
            cur = jnp.maximum(s[:, :L], s[:, L:])
            mx = cur if mx is None else jnp.maximum(mx, cur)
        m = jnp.max(mx, axis=1, keepdims=True)
        ls = None
        for kb in blocks:
            e = jnp.exp(s_ref[:, at(kb)] - m)
            s_ref[:, at(kb)] = e
            cur = e[:, :L] + e[:, L:]
            ls = cur if ls is None else ls + cur
        rl = 1.0 / jnp.sum(ls, axis=1, keepdims=True)
        acc = None
        for kb in blocks:
            p_ = s_ref[:, at(kb)] * rl
            s_ref[:, at(kb)] = p_
            pb = p_.astype(BF)
            p_ref[:, at(kb)] = pb
            cur = dot_nn(pb, v_at(kb))
            acc = cur if acc is None else acc + cur
        dsum = jnp.sum(dom.astype(F32) * acc, axis=1, keepdims=True)
        dq = None
        for kb in blocks:
            dp = dot_nt(dom, v_at(kb)).astype(BF).astype(F32)
            ds = (s_ref[:, at(kb)] * (dp - dsum)).astype(BF)
            ds_ref[:, at(kb)] = ds
            cur = dot_nn(ds, k_at(kb))
            dq = cur if dq is None else dq + cur
        hr = slice(hd * 64, hd * 64 + 64)
        n = len(blocks) * QB
        keys = slice(first * QB, first * QB + n)
        dvt_ref[hr, keys] += dot_nn(dot_ref[hr, i * QB:(i + 1) * QB], p_ref[:, :n])
        dkt_ref[hr, keys] += dot_nn(qt_ref[hr, i * QB:(i + 1) * QB], ds_ref[:, :n])
        return acc, dq * 0.125

    def batch_step(j, carry):
        mj('t_h2')
        last = h_tree(j)
        for e in last.hops(2):
            last.arrive(e)
        do_swap(j).wait()

        def qkv_step(r, c):
            rows = hg_ref[pl.ds(2 * r, 2), j].reshape(T, D)
            out = dot_nn(rows, w_ref[...]) + bias_ref[0:1, :]
            qkv_ref[pl.ds(pl.multiple_of(r * T, T), T), :] = out.astype(BF)
            return c

        mj('qkv')
        lax.fori_loop(0, 4, qkv_step, 0)

        mj('when')
        @pl.when(j == 0)
        def _():
            for e in trees[1].hops(0):
                trees[1].arrive(e)
            do_swap(1).start()

        mj('transp')
        for i in R8:
            qs = qkv_ref[i * QB:(i + 1) * QB, 0:L] * BF(0.125)
            qt_ref[:, i * QB:(i + 1) * QB] = qs.T
            dot_ref[:, i * QB:(i + 1) * QB] = dog_ref[j, 2 * i:2 * i + 2].reshape(QB, L).T
        dkt_ref[...] = jnp.zeros_like(dkt_ref)
        dvt_ref[...] = jnp.zeros_like(dvt_ref)
        for i in R8:
            mj('att')
            of, dqf = head_block(j, i, 0)
            og, dqg = head_block(j, i, 1)
            o = jnp.where(lane < 64, of, og).astype(BF)
            dq = jnp.where(lane < 64, dqf, dqg).astype(BF)
            for u in range(2):
                so_ref[j, 2 * i + u] = o[u * L:(u + 1) * L]
                sd_ref[j, 2 * i + u, 0] = dq[u * L:(u + 1) * L]
            dqkv_ref[i * QB:(i + 1) * QB, 0:L] = dq

        mj('when')
        @pl.when(j == 0)
        def _():
            for e in trees[1].hops(1):
                trees[1].arrive(e)

        mj('dkdv')
        for t, src in ((1, dkt_ref), (2, dvt_ref)):
            for n in range(N):
                d = src[:, n * L:(n + 1) * L].T.astype(BF)
                sd_ref[j, n, t] = d
                dqkv_ref[n * L:(n + 1) * L, t * L:(t + 1) * L] = d
        o_swap(j).start()
        ro_ref[j, pc.me] = so_ref[j, pc.me]
        rd_ref[j, pc.me] = sd_ref[j, pc.me]

        def dw_step(r, c):
            cols = pl.ds(pl.multiple_of(r * QB, QB), QB)
            dwp_ref[cols, :] += dot_tn(hg_ref[:, j, :, cols].reshape(S, QB), dqkv_ref[...])
            return c

        mj('dw')
        lax.fori_loop(0, 4, dw_step, 0)
        d_swap(j).start()
        dwp_ref[D:D + 1, :] += jnp.sum(dqkv_ref[...].astype(F32), axis=0, keepdims=True)
        mj(None)
        return carry

    mk(None)
    lax.fori_loop(0, 2, batch_step, 0)

    def half_of(core):
        return dwp_ref.at[pl.ds(pl.multiple_of(core * HR, 8), HR)]

    sends = []

    def to_sib(n, src, dst, send, recv):
        cp = rcopy(src, dst, send.at[n], recv.at[n], pc.sib)
        cp.start()
        sends.append(cp)
        return cp

    mk('half_start')
    half = to_sib(2, half_of(1 - pc.core), dws_ref, sib_send, sib_recv)
    mk('tree_fin')
    for j in range(2):
        trees[j].finish()
        do_swap(j).finish()
    w_flat = hg_ref.reshape(2 * S, D)
    w_loads = [pltpu.make_async_copy(wqkv_hbm.at[:, t * D:(t + 1) * D], w_flat.at[t * D:(t + 1) * D], loc.at[3 + t]) for t in R3]
    for cp in w_loads:
        cp.start()
    mk('o_wait')
    for j in range(2):
        o_swap(j).wait()
    for b in R4:
        for m in R8:
            o_nat[b * L:(b + 1) * L, m * L:(m + 1) * L] = gather_heads(lambda j, q: ro_ref[j, q], pos, b, m)

    def wout_part(core, c):
        cols = pl.ds(pl.multiple_of(core * T + c * QB, QB), QB)
        return dot_tn(o_nat[:, cols], dy_all)

    mk('part')
    for c in range(2):
        part_ref[c * QB:(c + 1) * QB] = wout_part(1 - pc.core, c)
    xp = to_sib(3, part_ref, px_ref, sib_send, sib_recv)
    for c in range(2):
        acc_ref[4 * c:4 * c + 4] = wout_part(pc.core, c).reshape(4, 64, D)
    mk('xp_wait')
    xp.wait_recv()
    acc_ref[...] += px_ref[...].reshape(8, 64, D)

    bufs = (rs0_ref, rs1_ref, rs2_ref)

    def reduce_step(s, wait):
        for p in R3:
            order = [(p + j) % 3 for j in R3]
            for i, sub in enumerate(subsets(order[s + 1:])):
                n = p * 7 + (0, 4, 6)[s] + i
                dst = bufs[s].at[i, o_rows(p)]
                if not wait:
                    cp = rcopy(acc_ref.at[pc.chip_at((order[s],) + sub), o_rows(p)], dst,
                               r_send.at[n], r_recv.at[n], pc.next_dev(order[s]))
                    cp.start()
                    sends.append(cp)
                else:
                    rcopy(dst, dst, r_send.at[n], r_recv.at[n], pc.sib).wait_recv()
                    acc_ref[pc.chip_at(sub), o_rows(p)] += bufs[s][i, o_rows(p)]

    mk('rs0_send')
    reduce_step(0, False)
    mk('half_wait')
    half.wait_recv()
    dws_ref[...] += half_of(pc.core)[...]

    def w_slot(c, p, core=pc.core):
        return dwg_ref.at[c, core, w_rows(p)]

    def g_slot(c, p, core=pc.core):
        return dwo_ref.at[core, c, o_rows(p)]

    wtree = Tree(pc, lambda p: dws_ref.at[w_rows(p)], w_slot, w_send, w_recv)
    wtree.start_own()
    keep_w = pltpu.make_async_copy(dws_ref, dwg_ref.at[pc.chip, pc.core], loc.at[0])
    keep_w.start()
    for p in R3:
        to_sib(p, dws_ref.at[w_rows(p)], w_slot(pc.chip, p), ws_send, ws_recv)

    def pass_on(tree, slot, n, send, recv):
        for e in tree.hops(n):
            c, p = tree.arrive(e)
            to_sib(3 + tree.entries.index(e), slot(c, p), slot(c, p), send, recv)

    mk('y')
    dbo = jnp.zeros((1, D), F32)
    for b in R4:
        rows = slice(b * L, (b + 1) * L)
        y_ref[b] = (x_ref[b].astype(F32) + dot_nn(o_nat[rows], wout_ref.reshape(D, D)[...]) + bout).astype(BF)
        dbo += jnp.sum(dy_ref[b].astype(F32), axis=0, keepdims=True)
    mk('rs0_wait')
    reduce_step(0, True)
    reduce_step(1, False)
    mk('d_wait')
    for j in range(2):
        d_swap(j).wait()

    def spread(b, c):
        rows = pl.ds(pl.multiple_of(b * L, L), L)
        for m in R8:
            for t in R3:
                dqkv_nat[rows, t * D + m * L:t * D + (m + 1) * L] = gather_heads(lambda j, q: rd_ref[j, q, t], pos, b, m)
        return c

    mk('spread')
    lax.fori_loop(0, 4, spread, 0)
    mk('rs1_wait')
    reduce_step(1, True)
    reduce_step(2, False)
    mk('wload_wait')
    for cp in w_loads:
        cp.wait()
    mk('rs2_wait')
    reduce_step(2, True)
    gtree = Tree(pc, lambda p: acc_ref.at[pc.chip, o_rows(p)], g_slot, g_send, g_recv)
    gtree.start_own()
    keep_g = pltpu.make_async_copy(acc_ref.at[pc.chip], dwo_ref.at[pc.core, pc.chip], loc.at[1])
    keep_g.start()
    for p in R3:
        to_sib(p, acc_ref.at[pc.chip, o_rows(p)], g_slot(pc.chip, p), gs_send, gs_recv)
    mk('w_h0')
    pass_on(wtree, w_slot, 0, ws_send, ws_recv)

    def back(b, c):
        dg, db = c
        rows = pl.ds(pl.multiple_of(b * L, L), L)
        _, xhat, rstd = centre(x_ref[b])
        dh = None
        for t in R3:
            cur = dot_nt(dqkv_nat[rows, t * D:(t + 1) * D], w_flat[t * D:(t + 1) * D])
            dh = cur if dh is None else dh + cur
        dh = dh.astype(BF).astype(F32)
        dxh = dh * gamma
        m1 = jnp.mean(dxh, axis=-1, keepdims=True)
        m2 = jnp.mean(dxh * xhat, axis=-1, keepdims=True)
        dx_ref[b] = (dy_ref[b].astype(F32) + rstd * (dxh - m1 - xhat * m2)).astype(BF)
        return dg + jnp.sum(dh * xhat, axis=0, keepdims=True), db + jnp.sum(dh, axis=0, keepdims=True)

    mk('dh')
    zero = jnp.zeros((1, D), F32)
    dg, db = lax.fori_loop(0, 4, back, (zero, zero))
    row = lax.broadcasted_iota(jnp.int32, (8, D), 0)
    sm_ref[pc.me] = jnp.where(row == 0, dg, jnp.where(row == 1, db, jnp.where(row == 2, dbo, 0.0)))
    s_swap = Exchange(pc, lambda t: sm_ref.at[pc.me], lambda t: sm_ref.at[t], lambda r: s_send.at[r], lambda r: s_recv.at[r])
    s_swap.start()
    mk('g_h0')
    pass_on(gtree, g_slot, 0, gs_send, gs_recv)
    mk('g_h1')
    pass_on(gtree, g_slot, 1, gs_send, gs_recv)
    mk('w_h1')
    pass_on(wtree, w_slot, 1, ws_send, ws_recv)
    mk('s_wait')
    s_swap.wait()
    tot = sm_ref[0]
    for n in range(1, N):
        tot = tot + sm_ref[n]
    small_ref[...] = tot
    mk('g_h2')
    pass_on(gtree, g_slot, 2, gs_send, gs_recv)
    mk('w_h2')
    pass_on(wtree, w_slot, 2, ws_send, ws_recv)
    mk('sib_waits')
    for tree, slot, send, recv in ((wtree, w_slot, ws_send, ws_recv), (gtree, g_slot, gs_send, gs_recv)):
        for p in R3:
            at = slot(pc.chip, p, 1 - pc.core)
            rcopy(at, at, send.at[p], recv.at[p], pc.sib).wait_recv()
        for i, (p, axis, sub) in enumerate(tree.entries):
            at = slot(pc.chip_at(sub + (axis,)), p, 1 - pc.core)
            rcopy(at, at, send.at[3 + i], recv.at[3 + i], pc.sib).wait_recv()
        tree.finish()
    mk('final')
    for j in range(2):
        sib_copy(j).wait_send()
        o_swap(j).finish()
        d_swap(j).finish()
    s_swap.finish()
    for cp in sends:
        cp.wait_send()
    keep_w.wait()
    keep_g.wait()
    mk(None)


def layer_call(kind, x, dy, gamma, beta, bout, bqkv, wqkv, wout):
    vm, sm, hb = (pl.BlockSpec(memory_space=m) for m in (pltpu.VMEM, pltpu.SMEM, pl.ANY))
    sem = pltpu.SemaphoreType.DMA
    tok = jax.ShapeDtypeStruct((4, L, D), BF)

    def pair(*n):
        return [sem(n), sem(n)]

    def bf(*n):
        return pltpu.VMEM(n, BF)

    def ff(*n):
        return pltpu.VMEM(n, F32)

    band = 3 * QB
    return pl.pallas_call(
        layer_kernel,
        out_shape=(tok, tok, jax.ShapeDtypeStruct((8, D), F32), jax.ShapeDtypeStruct((8, 2, HR, W3), F32),
                   jax.ShapeDtypeStruct((2, 8, 64, D), F32)),
        in_specs=[sm] + [vm] * 6 + [hb, hb],
        out_specs=(vm, vm, vm, hb, hb),
        scratch_shapes=[
            bf(8, 2, QB, D), bf(2, L, D), bf(N, 64, D), bf(QB, D), bf(8, 4, L, L), bf(2, N, L, L), bf(D, W3), ff(8, W3),
            bf(S, W3), bf(S, W3), bf(L, S), bf(L, S), ff(L, S), ff(L, S),
            ff(QB, S), bf(QB, S), bf(QB, S), ff(QB, band), bf(QB, band), bf(QB, band),
            bf(2, N, L, L), bf(2, N, 3, L, L), bf(2, N, L, L), bf(2, N, 3, L, L), bf(T, D), bf(T, D3),
            ff(DR, W3), ff(HR, W3), ff(T, D), ff(T, D), ff(8, 64, D),
            ff(4, 64, D), ff(2, 64, D), ff(1, 64, D), ff(N, 8, D), sem((6,))]
        + pair(4) + pair(2, 21) + pair(2, N) + pair(2, N) + pair(2, N) + pair(N)
        + pair(21) + pair(21) + pair(24) + pair(24) + pair(21),
        compiler_params=pltpu.CompilerParams(vmem_limit_bytes=VMEM_CAP, collective_id=0, has_side_effects=True),
        name="layer",
    )(kind, x, dy, gamma, beta, bout, bqkv, wqkv, wout)


def unpack_kernel(kind_ref, dw_ref, bias_in_ref, dwo_ref, small_ref, y_in, dx_in,
                  out_ref, bias_ref, wo_ref, dg_ref, db_ref, dbo_ref, y_ref, dx_ref):
    pos = head_places(kind_ref)
    wo_ref[...] = dwo_ref[...]
    y_ref[...] = y_in[...]
    dx_ref[...] = dx_in[...]

    def pick(ref, t, m):
        cols = slice(t * L, (t + 1) * L)
        pa, pb = pos[2 * m], pos[2 * m + 1]
        a, b = ref[pa % 8, :, cols], ref[pb % 8, :, cols]
        lane = lax.broadcasted_iota(jnp.int32, a.shape, 1)
        a = jnp.where(pa // 8 == 1, pltpu.roll(a, 64, 1), a)
        b = jnp.where(pb // 8 == 0, pltpu.roll(b, 64, 1), b)
        return jnp.where(lane < 64, a, b)

    for t in R3:
        for m in R8:
            out_ref[:, t * D + m * L:t * D + (m + 1) * L] = pick(dw_ref, t, m)

    @pl.when(pl.program_id(0) == 0)
    def _():
        for t in R3:
            for m in R8:
                bias_ref[t * D + m * L:t * D + (m + 1) * L] = pick(bias_in_ref, t, m)[0]
        dg_ref[...] = small_ref[0]
        db_ref[...] = small_ref[1]
        dbo_ref[...] = small_ref[2]


def unpack_call(kind, dwg, dwo, small, y, dx):
    vec = jax.ShapeDtypeStruct((D,), F32)
    tok = pl.BlockSpec((1, 64, D), lambda r, s: (r // 2, r % 2, 0))
    tok_out = jax.ShapeDtypeStruct((4, L, D), BF)
    one = lambda r, s: (0,)
    return pl.pallas_call(
        unpack_kernel,
        grid_spec=pltpu.PrefetchScalarGridSpec(
            num_scalar_prefetch=1,
            grid=(8,),
            in_specs=[pl.BlockSpec((8, L, W3), lambda r, s: (0, r, 0)), pl.BlockSpec((8, 8, W3), lambda r, s: (0, L, 0)),
                      pl.BlockSpec((L, D), lambda r, s: (r, 0)), pl.BlockSpec((8, D), lambda r, s: (0, 0)), tok, tok],
            out_specs=[pl.BlockSpec((L, D3), lambda r, s: (r, 0)), pl.BlockSpec((D3,), one),
                       pl.BlockSpec((L, D), lambda r, s: (r, 0))] + [pl.BlockSpec((D,), one)] * 3 + [tok, tok],
        ),
        out_shape=[jax.ShapeDtypeStruct((D, D3), F32), jax.ShapeDtypeStruct((D3,), F32),
                   jax.ShapeDtypeStruct((D, D), F32), vec, vec, vec, tok_out, tok_out],
        compiler_params=pltpu.CompilerParams(vmem_limit_bytes=VMEM_CAP),
        name="unpack",
    )(kind, dwg, dwg, dwo, small, y, dx)


def solution(mesh):
    tok_spec = P(None, "sp", None)

    def local_block(x, d_y, ln_gamma, ln_beta, w_qkv, b_qkv, w_out, b_out, head_kind):
        y, dx, small, dwg, dwo = layer_call(head_kind, x, d_y, ln_gamma, ln_beta, b_out, b_qkv, w_qkv, w_out.reshape(N, 64, D))
        dw, dbias, dwout, dg, db, dbo, y, dx = unpack_call(
            head_kind, dwg.reshape(8, DR, W3), dwo.reshape(D, D), small, y, dx)
        return y, dx, dg, db, dw, dbias, dwout, dbo

    return jax.shard_map(
        local_block, mesh=mesh,
        in_specs=(tok_spec, tok_spec, P(), P(), P(), P(), P(), P(), P()),
        out_specs=(tok_spec, tok_spec, P(), P(), P(), P(), P(), P()), check_vma=False)
```

```python
import functools
import math

import jax
import jax.numpy as jnp
from jax import lax
from jax.experimental import pallas as pl
from jax.experimental.pallas import tpu as pltpu
from jax.sharding import PartitionSpec as P

LN_EPS = 1e-5
NEG_BIG = -1e30
BF = jnp.bfloat16
F32 = jnp.float32
QB = 256
L = 128
W3 = 384
T = 512
D = 1024
DR = 1040
HR = 520
N = 16
R3, R4, R8 = range(3), range(4), range(8)
MESH = pl.DeviceIdType.MESH
H_ROWS = (0, 96, 176, 256)
W_ROWS = (0, 176, 352, 520)
O_ROWS = (0, 24, 48, 64)
S = 2048
D3 = 3072
VMEM_CAP = 63 * D * D


def dot_nn(a, b):
    return lax.dot_general(a, b, (((1,), (0,)), ((), ())), preferred_element_type=F32)


def dot_nt(a, b):
    return lax.dot_general(a, b, (((1,), (1,)), ((), ())), preferred_element_type=F32)


def dot_tn(a, b):
    return lax.dot_general(a, b, (((0,), (0,)), ((), ())), preferred_element_type=F32)


def swap_halves(a):
    return jnp.concatenate([a[:, 64:], a[:, :64]], axis=1)


def pair_halves(a, a_half, b, b_half):
    lane = lax.broadcasted_iota(jnp.int32, a.shape, 1)
    a = jnp.where(a_half == 1, swap_halves(a), a)
    b = jnp.where(b_half == 0, swap_halves(b), b)
    return jnp.where(lane < 64, a, b)


class Place:
    def __init__(self):
        self.me = lax.axis_index("sp")
        self.core, self.chip = self.me % 2, self.me // 2
        self.sib = self.me + 1 - 2 * self.core
        bits = (self.chip % 2, self.chip // 2 % 2, self.chip // 4)
        self.step = [(1 - 2 * v) * w for v, w in zip(bits, (1, 2, 4))]

    def chip_at(self, axes):
        out = self.chip
        for a in axes:
            out = out + self.step[a]
        return out

    def next_dev(self, axis):
        return self.me + 2 * self.step[axis]


def rcopy(src, dst, send, recv, dev):
    return pltpu.make_async_remote_copy(
        src_ref=src, dst_ref=dst, send_sem=send, recv_sem=recv, device_id=(dev,), device_id_type=MESH)


def subsets(axes):
    out = [()]
    for a in axes:
        out += [v + (a,) for v in out]
    return out


class Tree:
    def __init__(self, place, own, slot, send, recv):
        self.place, self.own, self.slot, self.send, self.recv = place, own, slot, send, recv
        self.entries = []
        for s in R3:
            for p in R3:
                order = [(p + j) % 3 for j in R3]
                for sub in subsets(order[:s]):
                    self.entries.append((p, order[s], sub))

    def copy(self, e):
        p, axis, sub = e
        i = self.entries.index(e)
        at = self.slot(self.place.chip_at(sub), p)
        return rcopy(at if sub else self.own(p), at, self.send.at[i], self.recv.at[i], self.place.next_dev(axis))

    def start_own(self):
        for e in self.entries:
            if not e[2]:
                self.copy(e).start()

    def arrive(self, e):
        p, axis, sub = e
        got = sub + (axis,)
        chip = self.place.chip_at(got)
        at = self.slot(chip, p)
        i = self.entries.index(e)
        rcopy(at, at, self.send.at[i], self.recv.at[i], self.place.next_dev(axis)).wait_recv()
        for n in self.entries:
            if n[0] == p and n[2] == got:
                self.copy(n).start()
        return chip, p

    def hops(self, n):
        return [e for e in self.entries if len(e[2]) == n]

    def finish(self):
        for e in self.entries:
            self.copy(e).wait_send()


def barrier_signal(place):
    sem = pltpu.get_barrier_semaphore()
    for r in range(1, N):
        pl.semaphore_signal(sem, inc=1, device_id=((place.me + r) % N,), device_id_type=MESH)


def barrier_wait():
    pl.semaphore_wait(pltpu.get_barrier_semaphore(), N - 1)


def head_places(kind_ref):
    pos, zeros, ones = [], 0, 8
    for n in range(N):
        k = kind_ref[n]
        pos.append(jnp.where(k == 0, zeros, ones))
        zeros, ones = zeros + 1 - k, ones + k
    return pos


class Exchange:
    def __init__(self, place, src, dst, send, recv):
        self.place, self.src, self.dst, self.send, self.recv = place, src, dst, send, recv

    def copies(self):
        me = self.place.me
        for r in range(1, N):
            to = (me + r) % N
            yield rcopy(self.src(to), self.dst(me), self.send(r), self.recv(r), to)

    def start(self):
        for cp in self.copies():
            cp.start()

    def wait(self):
        for r in range(1, N):
            at = self.dst((self.place.me + N - r) % N)
            rcopy(at, at, self.send(r), self.recv(r), self.place.me).wait_recv()

    def finish(self):
        for cp in self.copies():
            cp.wait_send()


def gather_heads(recv_at, pos, b, m):
    pa, pb = pos[2 * m], pos[2 * m + 1]
    k, j = b // 2, b % 2
    a = recv_at(j, 2 * (pa % 8) + k)
    c = recv_at(j, 2 * (pb % 8) + k)
    return pair_halves(a, pa // 8, c, pb // 8)


def span(tab):
    return lambda p: pl.ds(tab[p], tab[p + 1] - tab[p])


def centre(xb):
    xf = xb.astype(F32)
    cen = xf - jnp.mean(xf, axis=-1, keepdims=True)
    rstd = lax.rsqrt(jnp.mean(cen * cen, axis=-1, keepdims=True) + LN_EPS)
    return xf, cen * rstd, rstd


class Marks:
    def __init__(self):
        self.cur = None

    def __call__(self, name):
        if self.cur is not None:
            self.cur.__exit__(None, None, None)
        self.cur = None
        if name is not None:
            self.cur = jax.named_scope(name)
            self.cur.__enter__()


def layer_kernel(kind_ref, x_ref, dy_ref, gamma_ref, beta_ref, bout_ref, bqkv_ref, wqkv_hbm, wout_hbm,
                 y_ref, dx_ref, small_ref, dwg_ref, dwo_ref,
                 hg_ref, out_ref, wout_ref, wp_ref, do_ref, dog_ref, w_ref, bias_ref, qkv_ref, dqkv_ref, qt_ref, dot_ref,
                 dkt_ref, dvt_ref, s_f, p_f, ds_f, s_g, p_g, ds_g, so_ref, sd_ref, ro_ref, rd_ref, o_nat, dqkv_nat,
                 dwp_ref, dws_ref, part_ref, px_ref, acc_ref, rs0_ref, rs1_ref, rs2_ref, sm_ref,
                 loc, sib_send, sib_recv, h_send, h_recv, do_send, do_recv, o_send, o_recv, d_send, d_recv,
                 s_send, s_recv, w_send, w_recv, g_send, g_recv, ws_send, ws_recv, gs_send, gs_recv, r_send, r_recv):
    pc = Place()
    mk, mj = Marks(), Marks()
    barrier_signal(pc)

    def w_load(r):
        return pltpu.make_async_copy(wqkv_hbm.at[r * T:(r + 1) * T], dqkv_nat, loc.at[r])

    wo_load = pltpu.make_async_copy(wout_hbm, wout_ref, loc.at[2])
    w_load(0).start()
    wo_load.start()
    gamma = gamma_ref[...].reshape(1, D).astype(F32)
    beta = beta_ref[...].reshape(1, D).astype(F32)
    bout = bout_ref[...].reshape(1, D).astype(F32)
    bqkv = bqkv_ref[...].reshape(1, D3).astype(F32)

    def rows_of(core):
        return pl.ds(pl.multiple_of(core * L, L), L)

    def norm(xb):
        return (centre(xb)[1] * gamma + beta).astype(BF)

    def sib_copy(j):
        return rcopy(out_ref.at[j], hg_ref.at[pc.chip, j, rows_of(pc.core)], sib_send.at[j], sib_recv.at[j], pc.sib)

    for j in range(2):
        out_ref[j] = norm(x_ref[2 * (1 - pc.core) + j])
    for j in range(2):
        hg_ref[pc.chip, j, rows_of(pc.core)] = norm(x_ref[2 * pc.core + j])
    mk('barrier')
    barrier_wait()
    for j in range(2):
        sib_copy(j).start()

    h_rows, w_rows, o_rows = span(H_ROWS), span(W_ROWS), span(O_ROWS)

    def h_tree(j):
        slot = lambda c, p: hg_ref.at[c, j, h_rows(p)]
        return Tree(pc, lambda p: slot(pc.chip, p), slot, h_send.at[j], h_recv.at[j])

    def sib_arrive(j):
        at = hg_ref.at[pc.chip, j, rows_of(1 - pc.core)]
        rcopy(at, at, sib_send.at[j], sib_recv.at[j], pc.sib).wait_recv()

    do_out = do_ref.reshape(N, 2, L, L)

    def swap(src, dst, send, recv, j):
        return Exchange(pc, lambda t: src(t, j), lambda t: dst.at[j, t], lambda r: send.at[j, r], lambda r: recv.at[j, r])

    def do_swap(j):
        return swap(lambda t, j: do_out.at[t, j], dog_ref, do_send, do_recv, j)

    def o_swap(j):
        return swap(lambda t, j: so_ref.at[j, t], ro_ref, o_send, o_recv, j)

    def d_swap(j):
        return swap(lambda t, j: sd_ref.at[j, t], rd_ref, d_send, d_recv, j)

    mk('sibwait')
    trees = [h_tree(0), h_tree(1)]
    sib_arrive(0)
    trees[0].start_own()
    pos = head_places(kind_ref)
    perm = []
    for j in range(N):
        v = 0
        for n in range(1, N):
            v = v + jnp.where(pos[n] == j, n, 0)
        perm.append(v)
    f = g = 0
    for c in R8:
        f = f + jnp.where(pc.chip == c, perm[c], 0)
        g = g + jnp.where(pc.chip == c, perm[8 + c], 0)
    mk('dO_mm')
    wo_load.wait()
    dy_all = dy_ref[...].reshape(T, D)
    for c in R4:
        for u in range(2):
            wp_ref[u * L:u * L + 64] = wout_ref[perm[2 * c + u]]
            wp_ref[u * L + 64:u * L + L] = wout_ref[perm[8 + 2 * c + u]]
        d = dot_nt(dy_all, wp_ref[...]).astype(BF)
        for u in range(2):
            do_ref[2 * c + u] = d[:, u * L:(u + 1) * L].reshape(4, L, L)
    mk('t0_h0')
    for e in trees[0].hops(0):
        trees[0].arrive(e)
    mk('wsel')
    do_swap(0).start()
    for j in range(2):
        dog_ref[j, pc.me] = do_out[pc.me, j]

    def w_cols(t, k, head):
        out = None
        for m in R8:
            cur = dqkv_nat[k * L:(k + 1) * L, t * D + m * L:t * D + (m + 1) * L]
            out = cur if out is None else jnp.where(head // 2 == m, cur, out)
        return out

    for r in range(2):
        w_load(r).wait()
        for t in R3:
            for k in R4:
                w_ref[r * T + k * L:r * T + (k + 1) * L, t * L:(t + 1) * L] = pair_halves(
                    w_cols(t, k, f), f % 2, w_cols(t, k, g), g % 2)
        if r == 0:
            w_load(1).start()
    for t in R3:
        halves = []
        for head in (f, g):
            out = None
            for m in R8:
                cur = bqkv[:, t * D + m * L:t * D + (m + 1) * L]
                out = cur if out is None else jnp.where(head // 2 == m, cur, out)
            halves += [out, head % 2]
        bias_ref[:, t * L:(t + 1) * L] = jnp.broadcast_to(pair_halves(*halves), (8, L))
    dwp_ref[...] = jnp.zeros_like(dwp_ref)
    mk('t0_h1')
    for e in trees[0].hops(1):
        trees[0].arrive(e)
    sib_arrive(1)
    trees[1].start_own()

    lane = lax.broadcasted_iota(jnp.int32, (QB, L), 1)
    row_i = lax.broadcasted_iota(jnp.int32, (QB, QB), 0)
    col_i = lax.broadcasted_iota(jnp.int32, (QB, QB), 1)

    def head_block(j, i, hd):
        s_ref, p_ref, ds_ref = ((s_f, p_f, ds_f), (s_g, p_g, ds_g))[hd]
        first = 0 if hd == 0 else max(0, i - 2)
        blocks = range(first, i + 1)
        mine = (lane < 64) if hd == 0 else (lane >= 64)
        qi = qkv_ref[i * QB:(i + 1) * QB, 0:L] * BF(0.125)
        doi = dog_ref[j, 2 * i:2 * i + 2].reshape(QB, L)
        qm = jnp.where(mine, qi, BF(0))
        dom = jnp.where(mine, doi, BF(0))
        k_at = lambda kb: qkv_ref[kb * QB:(kb + 1) * QB, L:2 * L]
        v_at = lambda kb: qkv_ref[kb * QB:(kb + 1) * QB, 2 * L:3 * L]
        at = lambda kb: slice((kb - first) * QB, (kb - first + 1) * QB)
        mx = None
        for kb in blocks:
            s = dot_nt(qm, k_at(kb))
            if kb == i:
                s = jnp.where(col_i <= row_i, s, NEG_BIG)
            if hd == 1 and kb == i - 2:
                s = jnp.where(col_i > row_i, s, NEG_BIG)
            s_ref[:, at(kb)] = s
            cur = jnp.maximum(s[:, :L], s[:, L:])
            mx = cur if mx is None else jnp.maximum(mx, cur)
        m = jnp.max(mx, axis=1, keepdims=True)
        ls = None
        for kb in blocks:
            e = jnp.exp(s_ref[:, at(kb)] - m)
            s_ref[:, at(kb)] = e
            cur = e[:, :L] + e[:, L:]
            ls = cur if ls is None else ls + cur
        rl = 1.0 / jnp.sum(ls, axis=1, keepdims=True)
        acc = None
        for kb in blocks:
            p_ = s_ref[:, at(kb)] * rl
            s_ref[:, at(kb)] = p_
            pb = p_.astype(BF)
            p_ref[:, at(kb)] = pb
            cur = dot_nn(pb, v_at(kb))
            acc = cur if acc is None else acc + cur
        dsum = jnp.sum(dom.astype(F32) * acc, axis=1, keepdims=True)
        dq = None
        for kb in blocks:
            dp = dot_nt(dom, v_at(kb)).astype(BF).astype(F32)
            ds = (s_ref[:, at(kb)] * (dp - dsum)).astype(BF)
            ds_ref[:, at(kb)] = ds
            cur = dot_nn(ds, k_at(kb))
            dq = cur if dq is None else dq + cur
        hr = slice(hd * 64, hd * 64 + 64)
        n = len(blocks) * QB
        keys = slice(first * QB, first * QB + n)
        dvt_ref[hr, keys] += dot_nn(dot_ref[hr, i * QB:(i + 1) * QB], p_ref[:, :n])
        dkt_ref[hr, keys] += dot_nn(qt_ref[hr, i * QB:(i + 1) * QB], ds_ref[:, :n])
        return acc, dq * 0.125

    def batch_step(j, carry):
        mj('t_h2')
        last = h_tree(j)
        for e in last.hops(2):
            last.arrive(e)
        do_swap(j).wait()

        @pl.when(j == 1)
        def _():
            o_swap(0).start()
            d_swap(0).start()

        def qkv_step(r, c):
            rows = hg_ref[pl.ds(2 * r, 2), j].reshape(T, D)
            out = dot_nn(rows, w_ref[...]) + bias_ref[0:1, :]
            qkv_ref[pl.ds(pl.multiple_of(r * T, T), T), :] = out.astype(BF)
            return c

        mj('qkv')
        lax.fori_loop(0, 4, qkv_step, 0)

        mj('when')
        @pl.when(j == 0)
        def _():
            for e in trees[1].hops(0):
                trees[1].arrive(e)
            do_swap(1).start()

        mj('transp')
        for i in R8:
            qs = qkv_ref[i * QB:(i + 1) * QB, 0:L] * BF(0.125)
            qt_ref[:, i * QB:(i + 1) * QB] = qs.T
            dot_ref[:, i * QB:(i + 1) * QB] = dog_ref[j, 2 * i:2 * i + 2].reshape(QB, L).T
        dkt_ref[...] = jnp.zeros_like(dkt_ref)
        dvt_ref[...] = jnp.zeros_like(dvt_ref)
        for i in R8:
            mj('att')
            of, dqf = head_block(j, i, 0)
            og, dqg = head_block(j, i, 1)
            o = jnp.where(lane < 64, of, og).astype(BF)
            dq = jnp.where(lane < 64, dqf, dqg).astype(BF)
            for u in range(2):
                so_ref[j, 2 * i + u] = o[u * L:(u + 1) * L]
                sd_ref[j, 2 * i + u, 0] = dq[u * L:(u + 1) * L]
            dqkv_ref[i * QB:(i + 1) * QB, 0:L] = dq

        mj('when')
        @pl.when(j == 0)
        def _():
            for e in trees[1].hops(1):
                trees[1].arrive(e)

        mj('dkdv')
        for t, src in ((1, dkt_ref), (2, dvt_ref)):
            for n in range(N):
                d = src[:, n * L:(n + 1) * L].T.astype(BF)
                sd_ref[j, n, t] = d
                dqkv_ref[n * L:(n + 1) * L, t * L:(t + 1) * L] = d
        ro_ref[j, pc.me] = so_ref[j, pc.me]
        rd_ref[j, pc.me] = sd_ref[j, pc.me]

        @pl.when(j == 1)
        def _():
            o_swap(1).start()

        def dw_step(r, c):
            cols = pl.ds(pl.multiple_of(r * QB, QB), QB)
            dwp_ref[cols, :] += dot_tn(hg_ref[:, j, :, cols].reshape(S, QB), dqkv_ref[...])
            return c

        mj('dw')
        lax.fori_loop(0, 4, dw_step, 0)
        dwp_ref[D:D + 1, :] += jnp.sum(dqkv_ref[...].astype(F32), axis=0, keepdims=True)
        mj(None)
        return carry

    mk(None)
    lax.fori_loop(0, 2, batch_step, 0)
    d_swap(1).start()

    def half_of(core):
        return dwp_ref.at[pl.ds(pl.multiple_of(core * HR, 8), HR)]

    sends = []

    def to_sib(n, src, dst, send, recv):
        cp = rcopy(src, dst, send.at[n], recv.at[n], pc.sib)
        cp.start()
        sends.append(cp)
        return cp

    mk('half_start')
    half = to_sib(2, half_of(1 - pc.core), dws_ref, sib_send, sib_recv)
    mk('tree_fin')
    for j in range(2):
        trees[j].finish()
        do_swap(j).finish()
    w_flat = hg_ref.reshape(2 * S, D)
    w_loads = [pltpu.make_async_copy(wqkv_hbm.at[:, t * D:(t + 1) * D], w_flat.at[t * D:(t + 1) * D], loc.at[3 + t]) for t in R3]
    for cp in w_loads:
        cp.start()
    mk('o_wait')
    for j in range(2):
        o_swap(j).wait()
    for b in R4:
        for m in R8:
            o_nat[b * L:(b + 1) * L, m * L:(m + 1) * L] = gather_heads(lambda j, q: ro_ref[j, q], pos, b, m)

    def wout_part(core, c):
        cols = pl.ds(pl.multiple_of(core * T + c * QB, QB), QB)
        return dot_tn(o_nat[:, cols], dy_all)

    mk('part')
    for c in range(2):
        part_ref[c * QB:(c + 1) * QB] = wout_part(1 - pc.core, c)
    xp = to_sib(3, part_ref, px_ref, sib_send, sib_recv)
    for c in range(2):
        acc_ref[4 * c:4 * c + 4] = wout_part(pc.core, c).reshape(4, 64, D)
    mk('xp_wait')
    xp.wait_recv()
    acc_ref[...] += px_ref[...].reshape(8, 64, D)

    bufs = (rs0_ref, rs1_ref, rs2_ref)

    def reduce_step(s, wait):
        for p in R3:
            order = [(p + j) % 3 for j in R3]
            for i, sub in enumerate(subsets(order[s + 1:])):
                n = p * 7 + (0, 4, 6)[s] + i
                dst = bufs[s].at[i, o_rows(p)]
                if not wait:
                    cp = rcopy(acc_ref.at[pc.chip_at((order[s],) + sub), o_rows(p)], dst,
                               r_send.at[n], r_recv.at[n], pc.next_dev(order[s]))
                    cp.start()
                    sends.append(cp)
                else:
                    rcopy(dst, dst, r_send.at[n], r_recv.at[n], pc.sib).wait_recv()
                    acc_ref[pc.chip_at(sub), o_rows(p)] += bufs[s][i, o_rows(p)]

    mk('rs0_send')
    reduce_step(0, False)
    mk('half_wait')
    half.wait_recv()
    dws_ref[...] += half_of(pc.core)[...]

    def w_slot(c, p, core=pc.core):
        return dwg_ref.at[c, core, w_rows(p)]

    def g_slot(c, p, core=pc.core):
        return dwo_ref.at[core, c, o_rows(p)]

    wtree = Tree(pc, lambda p: dws_ref.at[w_rows(p)], w_slot, w_send, w_recv)
    wtree.start_own()
    keep_w = pltpu.make_async_copy(dws_ref, dwg_ref.at[pc.chip, pc.core], loc.at[0])
    keep_w.start()
    for p in R3:
        to_sib(p, dws_ref.at[w_rows(p)], w_slot(pc.chip, p), ws_send, ws_recv)

    def pass_on(tree, slot, n, send, recv):
        for e in tree.hops(n):
            c, p = tree.arrive(e)
            to_sib(3 + tree.entries.index(e), slot(c, p), slot(c, p), send, recv)

    mk('y')
    dbo = jnp.zeros((1, D), F32)
    for b in R4:
        rows = slice(b * L, (b + 1) * L)
        y_ref[b] = (x_ref[b].astype(F32) + dot_nn(o_nat[rows], wout_ref.reshape(D, D)[...]) + bout).astype(BF)
        dbo += jnp.sum(dy_ref[b].astype(F32), axis=0, keepdims=True)
    mk('rs0_wait')
    reduce_step(0, True)
    reduce_step(1, False)
    mk('d_wait')
    for j in range(2):
        d_swap(j).wait()

    def spread(b, c):
        rows = pl.ds(pl.multiple_of(b * L, L), L)
        for m in R8:
            for t in R3:
                dqkv_nat[rows, t * D + m * L:t * D + (m + 1) * L] = gather_heads(lambda j, q: rd_ref[j, q, t], pos, b, m)
        return c

    mk('spread')
    lax.fori_loop(0, 4, spread, 0)
    mk('rs1_wait')
    reduce_step(1, True)
    reduce_step(2, False)
    mk('wload_wait')
    for cp in w_loads:
        cp.wait()
    mk('rs2_wait')
    reduce_step(2, True)
    gtree = Tree(pc, lambda p: acc_ref.at[pc.chip, o_rows(p)], g_slot, g_send, g_recv)
    gtree.start_own()
    keep_g = pltpu.make_async_copy(acc_ref.at[pc.chip], dwo_ref.at[pc.core, pc.chip], loc.at[1])
    keep_g.start()
    for p in R3:
        to_sib(p, acc_ref.at[pc.chip, o_rows(p)], g_slot(pc.chip, p), gs_send, gs_recv)
    mk('w_h0')
    pass_on(wtree, w_slot, 0, ws_send, ws_recv)

    def back(b, c):
        dg, db = c
        rows = pl.ds(pl.multiple_of(b * L, L), L)
        _, xhat, rstd = centre(x_ref[b])
        dh = None
        for t in R3:
            cur = dot_nt(dqkv_nat[rows, t * D:(t + 1) * D], w_flat[t * D:(t + 1) * D])
            dh = cur if dh is None else dh + cur
        dh = dh.astype(BF).astype(F32)
        dxh = dh * gamma
        m1 = jnp.mean(dxh, axis=-1, keepdims=True)
        m2 = jnp.mean(dxh * xhat, axis=-1, keepdims=True)
        dx_ref[b] = (dy_ref[b].astype(F32) + rstd * (dxh - m1 - xhat * m2)).astype(BF)
        return dg + jnp.sum(dh * xhat, axis=0, keepdims=True), db + jnp.sum(dh, axis=0, keepdims=True)

    mk('dh')
    zero = jnp.zeros((1, D), F32)
    dg, db = lax.fori_loop(0, 4, back, (zero, zero))
    row = lax.broadcasted_iota(jnp.int32, (8, D), 0)
    sm_ref[pc.me] = jnp.where(row == 0, dg, jnp.where(row == 1, db, jnp.where(row == 2, dbo, 0.0)))
    s_swap = Exchange(pc, lambda t: sm_ref.at[pc.me], lambda t: sm_ref.at[t], lambda r: s_send.at[r], lambda r: s_recv.at[r])
    s_swap.start()
    mk('g_h0')
    pass_on(gtree, g_slot, 0, gs_send, gs_recv)
    mk('w_h1')
    pass_on(wtree, w_slot, 1, ws_send, ws_recv)
    mk('g_h1')
    pass_on(gtree, g_slot, 1, gs_send, gs_recv)
    mk('s_wait')
    s_swap.wait()
    tot = sm_ref[0]
    for n in range(1, N):
        tot = tot + sm_ref[n]
    small_ref[...] = tot
    mk('g_h2')
    pass_on(gtree, g_slot, 2, gs_send, gs_recv)
    mk('w_h2')
    pass_on(wtree, w_slot, 2, ws_send, ws_recv)
    mk('sib_waits')
    for tree, slot, send, recv in ((wtree, w_slot, ws_send, ws_recv), (gtree, g_slot, gs_send, gs_recv)):
        for p in R3:
            at = slot(pc.chip, p, 1 - pc.core)
            rcopy(at, at, send.at[p], recv.at[p], pc.sib).wait_recv()
        for i, (p, axis, sub) in enumerate(tree.entries):
            at = slot(pc.chip_at(sub + (axis,)), p, 1 - pc.core)
            rcopy(at, at, send.at[3 + i], recv.at[3 + i], pc.sib).wait_recv()
        tree.finish()
    mk('final')
    for j in range(2):
        sib_copy(j).wait_send()
        o_swap(j).finish()
        d_swap(j).finish()
    s_swap.finish()
    for cp in sends:
        cp.wait_send()
    keep_w.wait()
    keep_g.wait()
    mk(None)


def layer_call(kind, x, dy, gamma, beta, bout, bqkv, wqkv, wout):
    vm, sm, hb = (pl.BlockSpec(memory_space=m) for m in (pltpu.VMEM, pltpu.SMEM, pl.ANY))
    sem = pltpu.SemaphoreType.DMA
    tok = jax.ShapeDtypeStruct((4, L, D), BF)

    def pair(*n):
        return [sem(n), sem(n)]

    def bf(*n):
        return pltpu.VMEM(n, BF)

    def ff(*n):
        return pltpu.VMEM(n, F32)

    band = 3 * QB
    return pl.pallas_call(
        layer_kernel,
        out_shape=(tok, tok, jax.ShapeDtypeStruct((8, D), F32), jax.ShapeDtypeStruct((8, 2, HR, W3), F32),
                   jax.ShapeDtypeStruct((2, 8, 64, D), F32)),
        in_specs=[sm] + [vm] * 6 + [hb, hb],
        out_specs=(vm, vm, vm, hb, hb),
        scratch_shapes=[
            bf(8, 2, QB, D), bf(2, L, D), bf(N, 64, D), bf(QB, D), bf(8, 4, L, L), bf(2, N, L, L), bf(D, W3), ff(8, W3),
            bf(S, W3), bf(S, W3), bf(L, S), bf(L, S), ff(L, S), ff(L, S),
            ff(QB, S), bf(QB, S), bf(QB, S), ff(QB, band), bf(QB, band), bf(QB, band),
            bf(2, N, L, L), bf(2, N, 3, L, L), bf(2, N, L, L), bf(2, N, 3, L, L), bf(T, D), bf(T, D3),
            ff(DR, W3), ff(HR, W3), ff(T, D), ff(T, D), ff(8, 64, D),
            ff(4, 64, D), ff(2, 64, D), ff(1, 64, D), ff(N, 8, D), sem((6,))]
        + pair(4) + pair(2, 21) + pair(2, N) + pair(2, N) + pair(2, N) + pair(N)
        + pair(21) + pair(21) + pair(24) + pair(24) + pair(21),
        compiler_params=pltpu.CompilerParams(vmem_limit_bytes=VMEM_CAP, collective_id=0, has_side_effects=True),
        name="layer",
    )(kind, x, dy, gamma, beta, bout, bqkv, wqkv, wout)


def unpack_kernel(kind_ref, dw_hbm, dwo_hbm, y_in, dx_in, small_ref,
                  out_hbm, wo_hbm, y_out, dx_out, bias_ref, dg_ref, db_ref, dbo_ref,
                  in_ref, ob_ref, bias_in, wo_ref, y_ref, dx_ref, in_sem, out_sem, pass_in, pass_out):
    pos = head_places(kind_ref)

    def rows(r):
        return pl.ds(pl.multiple_of(r * L, L), L)

    def load(r):
        return pltpu.make_async_copy(dw_hbm.at[:, rows(r)], in_ref.at[r], in_sem.at[r])

    def store(r):
        return pltpu.make_async_copy(ob_ref.at[r], out_hbm.at[rows(r)], out_sem.at[r])

    def through(i):
        src, buf, dst = ((dwo_hbm, wo_ref, wo_hbm), (y_in, y_ref, y_out), (dx_in, dx_ref, dx_out))[i]
        return pltpu.make_async_copy(src, buf, pass_in.at[i]), pltpu.make_async_copy(buf, dst, pass_out.at[i])

    bias_load = pltpu.make_async_copy(dw_hbm.at[:, D:D + 8], bias_in, pass_in.at[3])
    for r in R3:
        load(r).start()
    bias_load.start()
    for i in R3:
        through(i)[0].start()

    def pick(read, t, m):
        pa, pb = pos[2 * m], pos[2 * m + 1]
        cols = slice(t * L, (t + 1) * L)
        a, b = read(pa % 8, cols), read(pb % 8, cols)
        lane = lax.broadcasted_iota(jnp.int32, a.shape, 1)
        a = jnp.where(pa // 8 == 1, pltpu.roll(a, 64, 1), a)
        b = jnp.where(pb // 8 == 0, pltpu.roll(b, 64, 1), b)
        return jnp.where(lane < 64, a, b)

    def step(r, c):
        load(r).wait()

        @pl.when(r < 5)
        def _():
            load(r + 3).start()

        for t in R3:
            for m in R8:
                ob_ref[r, :, t * D + m * L:t * D + (m + 1) * L] = pick(lambda q, cols: in_ref[r, q, :, cols], t, m)
        store(r).start()
        return c

    lax.fori_loop(0, 8, step, 0)
    for i in R3:
        get, put = through(i)
        get.wait()
        put.start()
    bias_load.wait()
    for t in R3:
        for m in R8:
            bias_ref[t * D + m * L:t * D + (m + 1) * L] = pick(lambda q, cols: bias_in[q, :, cols], t, m)[0]
    dg_ref[...] = small_ref[0]
    db_ref[...] = small_ref[1]
    dbo_ref[...] = small_ref[2]
    for r in R8:
        store(r).wait()
    for i in R3:
        through(i)[1].wait()


def unpack_call(kind, dwg, dwo, small, y, dx):
    vm, sm, hb = (pl.BlockSpec(memory_space=m) for m in (pltpu.VMEM, pltpu.SMEM, pl.ANY))
    sem = pltpu.SemaphoreType.DMA
    vec = jax.ShapeDtypeStruct((D,), F32)
    tok = jax.ShapeDtypeStruct((4, L, D), BF)
    return pl.pallas_call(
        unpack_kernel,
        in_specs=[sm, hb, hb, hb, hb, vm],
        out_specs=[hb, hb, hb, hb, vm, vm, vm, vm],
        out_shape=[jax.ShapeDtypeStruct((D, D3), F32), jax.ShapeDtypeStruct((D, D), F32), tok, tok,
                   jax.ShapeDtypeStruct((D3,), F32), vec, vec, vec],
        scratch_shapes=[
            pltpu.VMEM((8, 8, L, W3), F32), pltpu.VMEM((8, L, D3), F32), pltpu.VMEM((8, 8, W3), F32),
            pltpu.VMEM((D, D), F32), pltpu.VMEM((4, L, D), BF), pltpu.VMEM((4, L, D), BF),
            sem((8,)), sem((8,)), sem((4,)), sem((3,))],
        compiler_params=pltpu.CompilerParams(vmem_limit_bytes=VMEM_CAP),
        name="unpack",
    )(kind, dwg, dwo, y, dx, small)


def solution(mesh):
    tok_spec = P(None, "sp", None)

    def local_block(x, d_y, ln_gamma, ln_beta, w_qkv, b_qkv, w_out, b_out, head_kind):
        y, dx, small, dwg, dwo = layer_call(head_kind, x, d_y, ln_gamma, ln_beta, b_out, b_qkv, w_qkv, w_out.reshape(N, 64, D))
        dw, dwout, y, dx, dbias, dg, db, dbo = unpack_call(
            head_kind, dwg.reshape(8, DR, W3), dwo.reshape(D, D), small, y, dx)
        return y, dx, dg, db, dw, dbias, dwout, dbo

    return jax.shard_map(
        local_block, mesh=mesh,
        in_specs=(tok_spec, tok_spec, P(), P(), P(), P(), P(), P(), P()),
        out_specs=(tok_spec, tok_spec, P(), P(), P(), P(), P(), P()), check_vma=False)
```

```python
import functools
import math

import jax
import jax.numpy as jnp
from jax import lax
from jax.experimental import pallas as pl
from jax.experimental.pallas import tpu as pltpu
from jax.sharding import PartitionSpec as P

LN_EPS = 1e-5
NEG_BIG = -1e30
BF = jnp.bfloat16
F32 = jnp.float32
QB = 256
L = 128
W3 = 384
T = 512
D = 1024
DR = 1040
HR = 520
N = 16
R3, R4, R8 = range(3), range(4), range(8)
MESH = pl.DeviceIdType.MESH
H_ROWS = (0, 96, 176, 256)
W_ROWS = (0, 176, 352, 520)
O_ROWS = (0, 24, 48, 64)
S = 2048
D3 = 3072
VMEM_CAP = 63 * D * D


def dot_nn(a, b):
    return lax.dot_general(a, b, (((1,), (0,)), ((), ())), preferred_element_type=F32)


def dot_nt(a, b):
    return lax.dot_general(a, b, (((1,), (1,)), ((), ())), preferred_element_type=F32)


def dot_tn(a, b):
    return lax.dot_general(a, b, (((0,), (0,)), ((), ())), preferred_element_type=F32)


def swap_halves(a):
    return jnp.concatenate([a[:, 64:], a[:, :64]], axis=1)


def pair_halves(a, a_half, b, b_half):
    lane = lax.broadcasted_iota(jnp.int32, a.shape, 1)
    a = jnp.where(a_half == 1, swap_halves(a), a)
    b = jnp.where(b_half == 0, swap_halves(b), b)
    return jnp.where(lane < 64, a, b)


class Place:
    def __init__(self):
        self.me = lax.axis_index("sp")
        self.core, self.chip = self.me % 2, self.me // 2
        self.sib = self.me + 1 - 2 * self.core
        bits = (self.chip % 2, self.chip // 2 % 2, self.chip // 4)
        self.step = [(1 - 2 * v) * w for v, w in zip(bits, (1, 2, 4))]

    def chip_at(self, axes):
        out = self.chip
        for a in axes:
            out = out + self.step[a]
        return out

    def next_dev(self, axis):
        return self.me + 2 * self.step[axis]


def rcopy(src, dst, send, recv, dev):
    return pltpu.make_async_remote_copy(
        src_ref=src, dst_ref=dst, send_sem=send, recv_sem=recv, device_id=(dev,), device_id_type=MESH)


def subsets(axes):
    out = [()]
    for a in axes:
        out += [v + (a,) for v in out]
    return out


class Tree:
    def __init__(self, place, own, slot, seven, send, recv):
        self.place, self.own, self.slot, self.seven, self.send, self.recv = place, own, slot, seven, send, recv
        self.entries = []
        for s in R3:
            for p in R3:
                order = [(p + j) % 3 for j in R3]
                for sub in subsets(order[:s]):
                    self.entries.append((p, order[s], sub))

    def copy(self, e):
        p, axis, sub = e
        i = self.entries.index(e)
        at = self.slot(self.place.chip_at(sub), p)
        return rcopy(at if sub else self.own(p), at, self.send, self.recv.at[i], self.place.next_dev(axis))

    def start_own(self):
        for e in self.entries:
            if not e[2]:
                self.copy(e).start()

    def arrive(self, e):
        p, axis, sub = e
        got = sub + (axis,)
        chip = self.place.chip_at(got)
        at = self.slot(chip, p)
        i = self.entries.index(e)
        rcopy(at, at, self.send, self.recv.at[i], self.place.next_dev(axis)).wait_recv()
        for n in self.entries:
            if n[0] == p and n[2] == got:
                self.copy(n).start()
        return chip, p

    def hops(self, n):
        return [e for e in self.entries if len(e[2]) == n]

    def finish(self):
        rcopy(self.seven, self.seven, self.send, self.recv.at[0], self.place.me).wait_send()


def barrier_signal(place):
    sem = pltpu.get_barrier_semaphore()
    for r in range(1, N):
        pl.semaphore_signal(sem, inc=1, device_id=((place.me + r) % N,), device_id_type=MESH)


def barrier_wait():
    pl.semaphore_wait(pltpu.get_barrier_semaphore(), N - 1)


def head_places(kind_ref):
    pos, zeros, ones = [], 0, 8
    for n in range(N):
        k = kind_ref[n]
        pos.append(jnp.where(k == 0, zeros, ones))
        zeros, ones = zeros + 1 - k, ones + k
    return pos


class Exchange:
    def __init__(self, place, src, dst, rest, send, recv):
        self.place, self.src, self.dst, self.send, self.recv = place, src, dst, send, recv
        self.rest = rest

    def start(self):
        me = self.place.me
        for r in range(1, N):
            to = (me + r) % N
            rcopy(self.src(to), self.dst(me), self.send, self.recv, to).start()

    def wait(self):
        rcopy(self.rest, self.rest, self.send, self.recv, self.place.me).wait_recv()

    def finish(self):
        rcopy(self.rest, self.rest, self.send, self.recv, self.place.me).wait_send()


def gather_heads(recv_at, pos, b, m):
    pa, pb = pos[2 * m], pos[2 * m + 1]
    k, j = b // 2, b % 2
    a = recv_at(j, 2 * (pa % 8) + k)
    c = recv_at(j, 2 * (pb % 8) + k)
    return pair_halves(a, pa // 8, c, pb // 8)


def span(tab):
    return lambda p: pl.ds(tab[p], tab[p + 1] - tab[p])


def centre(xb):
    xf = xb.astype(F32)
    cen = xf - jnp.mean(xf, axis=-1, keepdims=True)
    rstd = lax.rsqrt(jnp.mean(cen * cen, axis=-1, keepdims=True) + LN_EPS)
    return xf, cen * rstd, rstd


class Marks:
    def __init__(self):
        self.cur = None

    def __call__(self, name):
        if self.cur is not None:
            self.cur.__exit__(None, None, None)
        self.cur = None
        if name is not None:
            self.cur = jax.named_scope(name)
            self.cur.__enter__()


def layer_kernel(kind_ref, x_ref, dy_ref, gamma_ref, beta_ref, bout_ref, bqkv_ref, wqkv_hbm, wout_hbm,
                 y_ref, dx_ref, small_ref, dwg_ref, dwo_ref,
                 hg_ref, out_ref, wout_ref, wp_ref, do_ref, dog_ref, w_ref, bias_ref, qkv_ref, dqkv_ref, qt_ref, dot_ref,
                 dkt_ref, dvt_ref, s_f, p_f, ds_f, s_g, p_g, ds_g, so_ref, sd_ref, ro_ref, rd_ref, o_nat, dqkv_nat,
                 dwp_ref, dws_ref, part_ref, px_ref, acc_ref, rs0_ref, rs1_ref, rs2_ref, sm_ref,
                 loc, sib_send, sib_recv, h_send, h_recv, do_send, do_recv, o_send, o_recv, d_send, d_recv,
                 s_send, s_recv, w_send, w_recv, g_send, g_recv, ws_send, ws_recv, gs_send, gs_recv, r_send, r_recv):
    pc = Place()
    mk, mj = Marks(), Marks()
    barrier_signal(pc)

    def w_load(r):
        return pltpu.make_async_copy(wqkv_hbm.at[r * T:(r + 1) * T], dqkv_nat, loc.at[r])

    wo_load = pltpu.make_async_copy(wout_hbm, wout_ref, loc.at[2])
    w_load(0).start()
    wo_load.start()
    gamma = gamma_ref[...].reshape(1, D).astype(F32)
    beta = beta_ref[...].reshape(1, D).astype(F32)
    bout = bout_ref[...].reshape(1, D).astype(F32)
    bqkv = bqkv_ref[...].reshape(1, D3).astype(F32)

    def rows_of(core):
        return pl.ds(pl.multiple_of(core * L, L), L)

    def norm(xb):
        return (centre(xb)[1] * gamma + beta).astype(BF)

    def sib_copy(j):
        return rcopy(out_ref.at[j], hg_ref.at[pc.chip, j, rows_of(pc.core)], sib_send.at[j], sib_recv.at[j], pc.sib)

    for j in range(2):
        out_ref[j] = norm(x_ref[2 * (1 - pc.core) + j])
    for j in range(2):
        hg_ref[pc.chip, j, rows_of(pc.core)] = norm(x_ref[2 * pc.core + j])
    mk('barrier')
    barrier_wait()
    for j in range(2):
        sib_copy(j).start()

    h_rows, w_rows, o_rows = span(H_ROWS), span(W_ROWS), span(O_ROWS)

    def h_tree(j):
        slot = lambda c, p: hg_ref.at[c, j, h_rows(p)]
        return Tree(pc, lambda p: slot(pc.chip, p), slot, hg_ref.at[0:7, j], h_send.at[j], h_recv.at[j])

    def sib_arrive(j):
        at = hg_ref.at[pc.chip, j, rows_of(1 - pc.core)]
        rcopy(at, at, sib_send.at[j], sib_recv.at[j], pc.sib).wait_recv()

    do_out = do_ref.reshape(N, 2, L, L)

    def swap(src, dst, send, recv, j):
        return Exchange(pc, lambda t: src(t, j), lambda t: dst.at[j, t], dst.at[j, 0:N - 1], send.at[j], recv.at[j])

    def do_swap(j):
        return swap(lambda t, j: do_out.at[t, j], dog_ref, do_send, do_recv, j)

    def o_swap(j):
        return swap(lambda t, j: so_ref.at[j, t], ro_ref, o_send, o_recv, j)

    def d_swap(j):
        return swap(lambda t, j: sd_ref.at[j, t], rd_ref, d_send, d_recv, j)

    mk('sibwait')
    trees = [h_tree(0), h_tree(1)]
    sib_arrive(0)
    trees[0].start_own()
    pos = head_places(kind_ref)
    perm = []
    for j in range(N):
        v = 0
        for n in range(1, N):
            v = v + jnp.where(pos[n] == j, n, 0)
        perm.append(v)
    f = g = 0
    for c in R8:
        f = f + jnp.where(pc.chip == c, perm[c], 0)
        g = g + jnp.where(pc.chip == c, perm[8 + c], 0)
    mk('dO_mm')
    wo_load.wait()
    dy_all = dy_ref[...].reshape(T, D)
    for c in R4:
        for u in range(2):
            wp_ref[u * L:u * L + 64] = wout_ref[perm[2 * c + u]]
            wp_ref[u * L + 64:u * L + L] = wout_ref[perm[8 + 2 * c + u]]
        d = dot_nt(dy_all, wp_ref[...]).astype(BF)
        for u in range(2):
            do_ref[2 * c + u] = d[:, u * L:(u + 1) * L].reshape(4, L, L)
    mk('t0_h0')
    for e in trees[0].hops(0):
        trees[0].arrive(e)
    mk('wsel')
    do_swap(0).start()
    for j in range(2):
        dog_ref[j, pc.me] = do_out[pc.me, j]

    def w_cols(t, k, head):
        out = None
        for m in R8:
            cur = dqkv_nat[k * L:(k + 1) * L, t * D + m * L:t * D + (m + 1) * L]
            out = cur if out is None else jnp.where(head // 2 == m, cur, out)
        return out

    for r in range(2):
        w_load(r).wait()
        for t in R3:
            for k in R4:
                w_ref[r * T + k * L:r * T + (k + 1) * L, t * L:(t + 1) * L] = pair_halves(
                    w_cols(t, k, f), f % 2, w_cols(t, k, g), g % 2)
        if r == 0:
            w_load(1).start()
    for t in R3:
        halves = []
        for head in (f, g):
            out = None
            for m in R8:
                cur = bqkv[:, t * D + m * L:t * D + (m + 1) * L]
                out = cur if out is None else jnp.where(head // 2 == m, cur, out)
            halves += [out, head % 2]
        bias_ref[:, t * L:(t + 1) * L] = jnp.broadcast_to(pair_halves(*halves), (8, L))
    dwp_ref[...] = jnp.zeros_like(dwp_ref)
    mk('t0_h1')
    for e in trees[0].hops(1):
        trees[0].arrive(e)
    sib_arrive(1)
    trees[1].start_own()

    lane = lax.broadcasted_iota(jnp.int32, (QB, L), 1)
    row_i = lax.broadcasted_iota(jnp.int32, (QB, QB), 0)
    col_i = lax.broadcasted_iota(jnp.int32, (QB, QB), 1)

    def head_block(j, i, hd):
        s_ref, p_ref, ds_ref = ((s_f, p_f, ds_f), (s_g, p_g, ds_g))[hd]
        first = 0 if hd == 0 else max(0, i - 2)
        blocks = range(first, i + 1)
        mine = (lane < 64) if hd == 0 else (lane >= 64)
        qi = qkv_ref[i * QB:(i + 1) * QB, 0:L] * BF(0.125)
        doi = dog_ref[j, 2 * i:2 * i + 2].reshape(QB, L)
        qm = jnp.where(mine, qi, BF(0))
        dom = jnp.where(mine, doi, BF(0))
        k_at = lambda kb: qkv_ref[kb * QB:(kb + 1) * QB, L:2 * L]
        v_at = lambda kb: qkv_ref[kb * QB:(kb + 1) * QB, 2 * L:3 * L]
        at = lambda kb: slice((kb - first) * QB, (kb - first + 1) * QB)
        mx = None
        for kb in blocks:
            s = dot_nt(qm, k_at(kb))
            if kb == i:
                s = jnp.where(col_i <= row_i, s, NEG_BIG)
            if hd == 1 and kb == i - 2:
                s = jnp.where(col_i > row_i, s, NEG_BIG)
            s_ref[:, at(kb)] = s
            cur = jnp.maximum(s[:, :L], s[:, L:])
            mx = cur if mx is None else jnp.maximum(mx, cur)
        m = jnp.max(mx, axis=1, keepdims=True)
        ls = None
        for kb in blocks:
            e = jnp.exp(s_ref[:, at(kb)] - m)
            s_ref[:, at(kb)] = e
            cur = e[:, :L] + e[:, L:]
            ls = cur if ls is None else ls + cur
        rl = 1.0 / jnp.sum(ls, axis=1, keepdims=True)
        acc = None
        for kb in blocks:
            p_ = s_ref[:, at(kb)] * rl
            s_ref[:, at(kb)] = p_
            pb = p_.astype(BF)
            p_ref[:, at(kb)] = pb
            cur = dot_nn(pb, v_at(kb))
            acc = cur if acc is None else acc + cur
        dsum = jnp.sum(dom.astype(F32) * acc, axis=1, keepdims=True)
        dq = None
        for kb in blocks:
            dp = dot_nt(dom, v_at(kb)).astype(BF).astype(F32)
            ds = (s_ref[:, at(kb)] * (dp - dsum)).astype(BF)
            ds_ref[:, at(kb)] = ds
            cur = dot_nn(ds, k_at(kb))
            dq = cur if dq is None else dq + cur
        hr = slice(hd * 64, hd * 64 + 64)
        n = len(blocks) * QB
        keys = slice(first * QB, first * QB + n)
        dvt_ref[hr, keys] += dot_nn(dot_ref[hr, i * QB:(i + 1) * QB], p_ref[:, :n])
        dkt_ref[hr, keys] += dot_nn(qt_ref[hr, i * QB:(i + 1) * QB], ds_ref[:, :n])
        return acc, dq * 0.125

    def batch_step(j, carry):
        mj('t_h2')
        last = h_tree(j)
        for e in last.hops(2):
            last.arrive(e)
        do_swap(j).wait()

        @pl.when(j == 1)
        def _():
            o_swap(0).start()
            d_swap(0).start()

        def qkv_step(r, c):
            rows = hg_ref[pl.ds(2 * r, 2), j].reshape(T, D)
            out = dot_nn(rows, w_ref[...]) + bias_ref[0:1, :]
            qkv_ref[pl.ds(pl.multiple_of(r * T, T), T), :] = out.astype(BF)
            return c

        mj('qkv')
        lax.fori_loop(0, 4, qkv_step, 0)

        mj('when')
        @pl.when(j == 0)
        def _():
            for e in trees[1].hops(0):
                trees[1].arrive(e)
            do_swap(1).start()

        mj('transp')
        for i in R8:
            qs = qkv_ref[i * QB:(i + 1) * QB, 0:L] * BF(0.125)
            qt_ref[:, i * QB:(i + 1) * QB] = qs.T
            dot_ref[:, i * QB:(i + 1) * QB] = dog_ref[j, 2 * i:2 * i + 2].reshape(QB, L).T
        dkt_ref[...] = jnp.zeros_like(dkt_ref)
        dvt_ref[...] = jnp.zeros_like(dvt_ref)
        for i in R8:
            mj('att')
            of, dqf = head_block(j, i, 0)
            og, dqg = head_block(j, i, 1)
            o = jnp.where(lane < 64, of, og).astype(BF)
            dq = jnp.where(lane < 64, dqf, dqg).astype(BF)
            for u in range(2):
                so_ref[j, 2 * i + u] = o[u * L:(u + 1) * L]
                sd_ref[j, 2 * i + u, 0] = dq[u * L:(u + 1) * L]
            dqkv_ref[i * QB:(i + 1) * QB, 0:L] = dq

        mj('when')
        @pl.when(j == 0)
        def _():
            for e in trees[1].hops(1):
                trees[1].arrive(e)

        mj('dkdv')
        for t, src in ((1, dkt_ref), (2, dvt_ref)):
            for n in range(N):
                d = src[:, n * L:(n + 1) * L].T.astype(BF)
                sd_ref[j, n, t] = d
                dqkv_ref[n * L:(n + 1) * L, t * L:(t + 1) * L] = d
        ro_ref[j, pc.me] = so_ref[j, pc.me]
        rd_ref[j, pc.me] = sd_ref[j, pc.me]

        @pl.when(j == 1)
        def _():
            o_swap(1).start()

        def dw_step(r, c):
            cols = pl.ds(pl.multiple_of(r * QB, QB), QB)
            dwp_ref[cols, :] += dot_tn(hg_ref[:, j, :, cols].reshape(S, QB), dqkv_ref[...])
            return c

        mj('dw')
        lax.fori_loop(0, 4, dw_step, 0)
        dwp_ref[D:D + 1, :] += jnp.sum(dqkv_ref[...].astype(F32), axis=0, keepdims=True)
        mj(None)
        return carry

    mk(None)
    lax.fori_loop(0, 2, batch_step, 0)

    def half_of(core):
        return dwp_ref.at[pl.ds(pl.multiple_of(core * HR, 8), HR)]

    def to_sib(n, src, dst, send, recv):
        cp = rcopy(src, dst, send.at[n], recv.at[n], pc.sib)
        cp.start()
        return cp

    half = to_sib(2, half_of(1 - pc.core), dws_ref, sib_send, sib_recv)
    mk('tree_fin')
    for j in range(2):
        trees[j].finish()
        do_swap(j).finish()
    w_flat = hg_ref.reshape(2 * S, D)
    w_loads = [pltpu.make_async_copy(wqkv_hbm.at[:, t * D:(t + 1) * D], w_flat.at[t * D:(t + 1) * D], loc.at[3 + t]) for t in R3]
    for cp in w_loads:
        cp.start()
    mk('o_wait')
    for j in range(2):
        o_swap(j).wait()
    d_swap(1).start()
    for b in R4:
        for m in R8:
            o_nat[b * L:(b + 1) * L, m * L:(m + 1) * L] = gather_heads(lambda j, q: ro_ref[j, q], pos, b, m)

    def wout_part(core, c):
        cols = pl.ds(pl.multiple_of(core * T + c * QB, QB), QB)
        return dot_tn(o_nat[:, cols], dy_all)

    mk('part')
    for c in range(2):
        part_ref[c * QB:(c + 1) * QB] = wout_part(1 - pc.core, c)
    xp = to_sib(3, part_ref, px_ref, sib_send, sib_recv)
    for c in range(2):
        acc_ref[4 * c:4 * c + 4] = wout_part(pc.core, c).reshape(4, 64, D)
    mk('xp_wait')
    xp.wait_recv()
    acc_ref[...] += px_ref[...].reshape(8, 64, D)

    bufs = (rs0_ref, rs1_ref, rs2_ref)

    def reduce_step(s, wait):
        for p in R3:
            order = [(p + j) % 3 for j in R3]
            if wait:
                at = bufs[s].at[:, o_rows(p)]
                rcopy(at, at, r_send.at[0], r_recv.at[s * 3 + p], pc.sib).wait_recv()
            for i, sub in enumerate(subsets(order[s + 1:])):
                if wait:
                    acc_ref[pc.chip_at(sub), o_rows(p)] += bufs[s][i, o_rows(p)]
                else:
                    rcopy(acc_ref.at[pc.chip_at((order[s],) + sub), o_rows(p)], bufs[s].at[i, o_rows(p)],
                          r_send.at[0], r_recv.at[s * 3 + p], pc.next_dev(order[s])).start()

    reduce_step(0, False)
    half.wait_recv()
    dws_ref[...] += half_of(pc.core)[...]

    def w_slot(c, p, core=pc.core):
        return dwg_ref.at[c, core, w_rows(p)]

    def g_slot(c, p, core=pc.core):
        return dwo_ref.at[core, c, o_rows(p)]

    wtree = Tree(pc, lambda p: dws_ref.at[w_rows(p)], w_slot, dwg_ref.at[0:7, pc.core], w_send.at[0], w_recv)
    wtree.start_own()
    keep_w = pltpu.make_async_copy(dws_ref, dwg_ref.at[pc.chip, pc.core], loc.at[0])
    keep_w.start()
    for p in R3:
        to_sib(0, dws_ref.at[w_rows(p)], w_slot(pc.chip, p), ws_send, ws_recv)

    def pass_on(tree, slot, n, send, recv):
        for e in tree.hops(n):
            c, p = tree.arrive(e)
            to_sib(0, slot(c, p), slot(c, p), send, recv)

    mk('y')
    dbo = jnp.zeros((1, D), F32)
    for b in R4:
        rows = slice(b * L, (b + 1) * L)
        y_ref[b] = (x_ref[b].astype(F32) + dot_nn(o_nat[rows], wout_ref.reshape(D, D)[...]) + bout).astype(BF)
        dbo += jnp.sum(dy_ref[b].astype(F32), axis=0, keepdims=True)
    mk('rs0_wait')
    reduce_step(0, True)
    reduce_step(1, False)
    mk('d_wait')
    for j in range(2):
        d_swap(j).wait()

    def spread(b, c):
        rows = pl.ds(pl.multiple_of(b * L, L), L)
        for m in R8:
            for t in R3:
                dqkv_nat[rows, t * D + m * L:t * D + (m + 1) * L] = gather_heads(lambda j, q: rd_ref[j, q, t], pos, b, m)
        return c

    def back(b, c):
        dg, db = c
        rows = pl.ds(pl.multiple_of(b * L, L), L)
        _, xhat, rstd = centre(x_ref[b])
        dh = None
        for t in R3:
            cur = dot_nt(dqkv_nat[rows, t * D:(t + 1) * D], w_flat[t * D:(t + 1) * D])
            dh = cur if dh is None else dh + cur
        dh = dh.astype(BF).astype(F32)
        dxh = dh * gamma
        m1 = jnp.mean(dxh, axis=-1, keepdims=True)
        m2 = jnp.mean(dxh * xhat, axis=-1, keepdims=True)
        dx_ref[b] = (dy_ref[b].astype(F32) + rstd * (dxh - m1 - xhat * m2)).astype(BF)
        return dg + jnp.sum(dh * xhat, axis=0, keepdims=True), db + jnp.sum(dh, axis=0, keepdims=True)

    mk('spread')
    lax.fori_loop(0, 4, spread, 0)
    mk('w_h0')
    pass_on(wtree, w_slot, 0, ws_send, ws_recv)
    mk('rs1_wait')
    reduce_step(1, True)
    reduce_step(2, False)
    mk('wload_wait')
    for cp in w_loads:
        cp.wait()
    mk('dh1')
    dgb = lax.fori_loop(0, 2, back, (jnp.zeros((1, D), F32), jnp.zeros((1, D), F32)))
    mk('rs2_wait')
    reduce_step(2, True)
    gtree = Tree(pc, lambda p: acc_ref.at[pc.chip, o_rows(p)], g_slot, dwo_ref.at[pc.core, 0:7], g_send.at[0], g_recv)
    gtree.start_own()
    keep_g = pltpu.make_async_copy(acc_ref.at[pc.chip], dwo_ref.at[pc.core, pc.chip], loc.at[1])
    keep_g.start()
    for p in R3:
        to_sib(0, acc_ref.at[pc.chip, o_rows(p)], g_slot(pc.chip, p), gs_send, gs_recv)

    mk('dh2')
    dg, db = lax.fori_loop(2, 4, back, dgb)
    row = lax.broadcasted_iota(jnp.int32, (8, D), 0)
    sm_ref[pc.me] = jnp.where(row == 0, dg, jnp.where(row == 1, db, jnp.where(row == 2, dbo, 0.0)))
    s_swap = Exchange(pc, lambda t: sm_ref.at[pc.me], lambda t: sm_ref.at[t], sm_ref.at[0:N - 1], s_send.at[0], s_recv.at[0])
    s_swap.start()
    mk('g_h0')
    pass_on(gtree, g_slot, 0, gs_send, gs_recv)
    mk('w_h1')
    pass_on(wtree, w_slot, 1, ws_send, ws_recv)
    mk('g_h1')
    pass_on(gtree, g_slot, 1, gs_send, gs_recv)
    mk('s_wait')
    s_swap.wait()
    tot = sm_ref[0]
    for n in range(1, N):
        tot = tot + sm_ref[n]
    small_ref[...] = tot
    mk('g_h2')
    pass_on(gtree, g_slot, 2, gs_send, gs_recv)
    mk('w_h2')
    pass_on(wtree, w_slot, 2, ws_send, ws_recv)
    mk('sib_waits')
    for tree, at, got, send, recv in (
            (wtree, dwg_ref.at[:, pc.core], dwg_ref.at[:, 1 - pc.core], ws_send, ws_recv),
            (gtree, dwo_ref.at[pc.core], dwo_ref.at[1 - pc.core], gs_send, gs_recv)):
        rcopy(got, got, send.at[0], recv.at[0], pc.sib).wait_recv()
        rcopy(at, at, send.at[0], recv.at[0], pc.sib).wait_send()
        tree.finish()
    mk('final')
    for j in range(2):
        sib_copy(j).wait_send()
        o_swap(j).finish()
        d_swap(j).finish()
    s_swap.finish()
    half.wait_send()
    xp.wait_send()
    rcopy(acc_ref.at[0:7], acc_ref.at[0:7], r_send.at[0], r_recv.at[0], pc.sib).wait_send()
    keep_w.wait()
    keep_g.wait()
    mk(None)


def layer_call(kind, x, dy, gamma, beta, bout, bqkv, wqkv, wout):
    vm, sm, hb = (pl.BlockSpec(memory_space=m) for m in (pltpu.VMEM, pltpu.SMEM, pl.ANY))
    sem = pltpu.SemaphoreType.DMA
    tok = jax.ShapeDtypeStruct((4, L, D), BF)

    def pair(*n):
        return [sem(n), sem(n)]

    def bf(*n):
        return pltpu.VMEM(n, BF)

    def ff(*n):
        return pltpu.VMEM(n, F32)

    band = 3 * QB
    return pl.pallas_call(
        layer_kernel,
        out_shape=(tok, tok, jax.ShapeDtypeStruct((8, D), F32), jax.ShapeDtypeStruct((8, 2, HR, W3), F32),
                   jax.ShapeDtypeStruct((2, 8, 64, D), F32)),
        in_specs=[sm] + [vm] * 6 + [hb, hb],
        out_specs=(vm, vm, vm, hb, hb),
        scratch_shapes=[
            bf(8, 2, QB, D), bf(2, L, D), bf(N, 64, D), bf(QB, D), bf(8, 4, L, L), bf(2, N, L, L), bf(D, W3), ff(8, W3),
            bf(S, W3), bf(S, W3), bf(L, S), bf(L, S), ff(L, S), ff(L, S),
            ff(QB, S), bf(QB, S), bf(QB, S), ff(QB, band), bf(QB, band), bf(QB, band),
            bf(2, N, L, L), bf(2, N, 3, L, L), bf(2, N, L, L), bf(2, N, 3, L, L), bf(T, D), bf(T, D3),
            ff(DR, W3), ff(HR, W3), ff(T, D), ff(T, D), ff(8, 64, D),
            ff(4, 64, D), ff(2, 64, D), ff(1, 64, D), ff(N, 8, D), sem((6,))]
        + pair(4) + [sem((2,)), sem((2, 21))] + pair(2) + pair(2) + pair(2) + pair(1)
        + [sem((1,)), sem((21,))] + [sem((1,)), sem((21,))] + pair(1) + pair(1) + [sem((1,)), sem((9,))],
        compiler_params=pltpu.CompilerParams(vmem_limit_bytes=VMEM_CAP, collective_id=0, has_side_effects=True),
        name="layer",
    )(kind, x, dy, gamma, beta, bout, bqkv, wqkv, wout)


def unpack_kernel(kind_ref, dw_hbm, dwo_hbm, y_in, dx_in, small_ref,
                  out_hbm, wo_hbm, y_out, dx_out, bias_ref, dg_ref, db_ref, dbo_ref,
                  in_ref, ob_ref, bias_in, wo_ref, y_ref, dx_ref, in_sem, out_sem, pass_in, pass_out):
    pos = head_places(kind_ref)

    def rows(r):
        return pl.ds(pl.multiple_of(r * L, L), L)

    def load(r):
        return pltpu.make_async_copy(dw_hbm.at[:, rows(r)], in_ref.at[r], in_sem.at[r])

    def store(r):
        return pltpu.make_async_copy(ob_ref.at[r], out_hbm.at[rows(r)], out_sem.at[r])

    def through(i):
        src, buf, dst = ((dwo_hbm, wo_ref, wo_hbm), (y_in, y_ref, y_out), (dx_in, dx_ref, dx_out))[i]
        return pltpu.make_async_copy(src, buf, pass_in.at[i]), pltpu.make_async_copy(buf, dst, pass_out.at[i])

    bias_load = pltpu.make_async_copy(dw_hbm.at[:, D:D + 8], bias_in, pass_in.at[3])
    for r in R3:
        load(r).start()
    bias_load.start()
    for i in R3:
        through(i)[0].start()

    def pick(read, t, m):
        pa, pb = pos[2 * m], pos[2 * m + 1]
        cols = slice(t * L, (t + 1) * L)
        a, b = read(pa % 8, cols), read(pb % 8, cols)
        lane = lax.broadcasted_iota(jnp.int32, a.shape, 1)
        a = jnp.where(pa // 8 == 1, pltpu.roll(a, 64, 1), a)
        b = jnp.where(pb // 8 == 0, pltpu.roll(b, 64, 1), b)
        return jnp.where(lane < 64, a, b)

    def step(r, c):
        load(r).wait()

        @pl.when(r < 5)
        def _():
            load(r + 3).start()

        for t in R3:
            for m in R8:
                ob_ref[r, :, t * D + m * L:t * D + (m + 1) * L] = pick(lambda q, cols: in_ref[r, q, :, cols], t, m)
        store(r).start()
        return c

    lax.fori_loop(0, 8, step, 0)
    for i in R3:
        get, put = through(i)
        get.wait()
        put.start()
    bias_load.wait()
    for t in R3:
        for m in R8:
            bias_ref[t * D + m * L:t * D + (m + 1) * L] = pick(lambda q, cols: bias_in[q, :, cols], t, m)[0]
    dg_ref[...] = small_ref[0]
    db_ref[...] = small_ref[1]
    dbo_ref[...] = small_ref[2]
    for r in R8:
        store(r).wait()
    for i in R3:
        through(i)[1].wait()


def unpack_call(kind, dwg, dwo, small, y, dx):
    vm, sm, hb = (pl.BlockSpec(memory_space=m) for m in (pltpu.VMEM, pltpu.SMEM, pl.ANY))
    sem = pltpu.SemaphoreType.DMA
    vec = jax.ShapeDtypeStruct((D,), F32)
    tok = jax.ShapeDtypeStruct((4, L, D), BF)
    return pl.pallas_call(
        unpack_kernel,
        in_specs=[sm, hb, hb, hb, hb, vm],
        out_specs=[hb, hb, hb, hb, vm, vm, vm, vm],
        out_shape=[jax.ShapeDtypeStruct((D, D3), F32), jax.ShapeDtypeStruct((D, D), F32), tok, tok,
                   jax.ShapeDtypeStruct((D3,), F32), vec, vec, vec],
        scratch_shapes=[
            pltpu.VMEM((8, 8, L, W3), F32), pltpu.VMEM((8, L, D3), F32), pltpu.VMEM((8, 8, W3), F32),
            pltpu.VMEM((D, D), F32), pltpu.VMEM((4, L, D), BF), pltpu.VMEM((4, L, D), BF),
            sem((8,)), sem((8,)), sem((4,)), sem((3,))],
        compiler_params=pltpu.CompilerParams(vmem_limit_bytes=VMEM_CAP),
        name="unpack",
    )(kind, dwg, dwo, y, dx, small)


def solution(mesh):
    tok_spec = P(None, "sp", None)

    def local_block(x, d_y, ln_gamma, ln_beta, w_qkv, b_qkv, w_out, b_out, head_kind):
        y, dx, small, dwg, dwo = layer_call(head_kind, x, d_y, ln_gamma, ln_beta, b_out, b_qkv, w_qkv, w_out.reshape(N, 64, D))
        dw, dwout, y, dx, dbias, dg, db, dbo = unpack_call(
            head_kind, dwg.reshape(8, DR, W3), dwo.reshape(D, D), small, y, dx)
        return y, dx, dg, db, dw, dbias, dwout, dbo

    return jax.shard_map(
        local_block, mesh=mesh,
        in_specs=(tok_spec, tok_spec, P(), P(), P(), P(), P(), P(), P()),
        out_specs=(tok_spec, tok_spec, P(), P(), P(), P(), P(), P()), check_vma=False)
```

```python
import functools
import math

import jax
import jax.numpy as jnp
from jax import lax
from jax.experimental import pallas as pl
from jax.experimental.pallas import tpu as pltpu
from jax.sharding import PartitionSpec as P

LN_EPS = 1e-5
NEG_BIG = -1e30
BF = jnp.bfloat16
F32 = jnp.float32
QB = 256
L = 128
W3 = 384
T = 512
D = 1024
DR = 1040
HR = 520
N = 16
R3, R4, R8 = range(3), range(4), range(8)
MESH = pl.DeviceIdType.MESH
H_ROWS = (0, 96, 176, 256)
W_ROWS = (0, 176, 352, 520)
O_ROWS = (0, 24, 48, 64)
S = 2048
D3 = 3072
VMEM_CAP = 63 * D * D


def dot_nn(a, b):
    return lax.dot_general(a, b, (((1,), (0,)), ((), ())), preferred_element_type=F32)


def dot_nt(a, b):
    return lax.dot_general(a, b, (((1,), (1,)), ((), ())), preferred_element_type=F32)


def dot_tn(a, b):
    return lax.dot_general(a, b, (((0,), (0,)), ((), ())), preferred_element_type=F32)


def swap_halves(a):
    return jnp.concatenate([a[:, 64:], a[:, :64]], axis=1)


def pair_halves(a, a_half, b, b_half):
    lane = lax.broadcasted_iota(jnp.int32, a.shape, 1)
    a = jnp.where(a_half == 1, swap_halves(a), a)
    b = jnp.where(b_half == 0, swap_halves(b), b)
    return jnp.where(lane < 64, a, b)


class Place:
    def __init__(self):
        self.me = lax.axis_index("sp")
        self.core, self.chip = self.me % 2, self.me // 2
        self.sib = self.me + 1 - 2 * self.core
        bits = (self.chip % 2, self.chip // 2 % 2, self.chip // 4)
        self.step = [(1 - 2 * v) * w for v, w in zip(bits, (1, 2, 4))]

    def chip_at(self, axes):
        out = self.chip
        for a in axes:
            out = out + self.step[a]
        return out

    def next_dev(self, axis):
        return self.me + 2 * self.step[axis]


def rcopy(src, dst, send, recv, dev):
    return pltpu.make_async_remote_copy(
        src_ref=src, dst_ref=dst, send_sem=send, recv_sem=recv, device_id=(dev,), device_id_type=MESH)


def subsets(axes):
    out = [()]
    for a in axes:
        out += [v + (a,) for v in out]
    return out


class Tree:
    def __init__(self, place, own, slot, seven, send, recv):
        self.place, self.own, self.slot, self.seven, self.send, self.recv = place, own, slot, seven, send, recv
        self.entries = []
        for s in R3:
            for p in R3:
                order = [(p + j) % 3 for j in R3]
                for sub in subsets(order[:s]):
                    self.entries.append((p, order[s], sub))

    def copy(self, e):
        p, axis, sub = e
        i = self.entries.index(e)
        at = self.slot(self.place.chip_at(sub), p)
        return rcopy(at if sub else self.own(p), at, self.send, self.recv.at[i], self.place.next_dev(axis))

    def start_own(self, levels=R3):
        for e in self.hops(0):
            if (e[1] - e[0]) % 3 in levels:
                self.copy(e).start()

    def arrive(self, e):
        p, axis, sub = e
        got = sub + (axis,)
        chip = self.place.chip_at(got)
        at = self.slot(chip, p)
        i = self.entries.index(e)
        rcopy(at, at, self.send, self.recv.at[i], self.place.next_dev(axis)).wait_recv()
        for n in self.entries:
            if n[0] == p and n[2] == got:
                self.copy(n).start()
        return chip, p

    def hops(self, n):
        return [e for e in self.entries if len(e[2]) == n]

    def finish(self):
        rcopy(self.seven, self.seven, self.send, self.recv.at[0], self.place.me).wait_send()


def barrier_signal(place):
    sem = pltpu.get_barrier_semaphore()
    for r in range(1, N):
        pl.semaphore_signal(sem, inc=1, device_id=((place.me + r) % N,), device_id_type=MESH)


def barrier_wait():
    pl.semaphore_wait(pltpu.get_barrier_semaphore(), N - 1)


def head_places(kind_ref):
    pos, zeros, ones = [], 0, 8
    for n in range(N):
        k = kind_ref[n]
        pos.append(jnp.where(k == 0, zeros, ones))
        zeros, ones = zeros + 1 - k, ones + k
    return pos


class Exchange:
    def __init__(self, place, src, dst, rest, send, recv):
        self.place, self.src, self.dst, self.send, self.recv = place, src, dst, send, recv
        self.rest = rest

    def start(self, first=1, end=N):
        me = self.place.me
        for r in range(first, end):
            to = (me + r) % N
            rcopy(self.src(to), self.dst(me), self.send, self.recv, to).start()

    def wait(self):
        rcopy(self.rest, self.rest, self.send, self.recv, self.place.me).wait_recv()

    def finish(self):
        rcopy(self.rest, self.rest, self.send, self.recv, self.place.me).wait_send()


def gather_heads(recv_at, pos, b, m):
    pa, pb = pos[2 * m], pos[2 * m + 1]
    k, j = b // 2, b % 2
    a = recv_at(j, 2 * (pa % 8) + k)
    c = recv_at(j, 2 * (pb % 8) + k)
    return pair_halves(a, pa // 8, c, pb // 8)


def span(tab):
    return lambda p: pl.ds(tab[p], tab[p + 1] - tab[p])


def centre(xb):
    xf = xb.astype(F32)
    cen = xf - jnp.mean(xf, axis=-1, keepdims=True)
    rstd = lax.rsqrt(jnp.mean(cen * cen, axis=-1, keepdims=True) + LN_EPS)
    return xf, cen * rstd, rstd


class Marks:
    def __init__(self):
        self.cur = None

    def __call__(self, name):
        if self.cur is not None:
            self.cur.__exit__(None, None, None)
        self.cur = None
        if name is not None:
            self.cur = jax.named_scope(name)
            self.cur.__enter__()


def layer_kernel(kind_ref, x_ref, dy_ref, gamma_ref, beta_ref, bout_ref, bqkv_ref, wqkv_hbm, wout_hbm,
                 y_ref, dx_ref, small_ref, dwg_ref, dwo_ref,
                 hg_ref, out_ref, wout_ref, wp_ref, do_ref, dog_ref, w_ref, bias_ref, qkv_ref, dqkv_ref, qt_ref, dot_ref,
                 dkt_ref, dvt_ref, s_f, p_f, ds_f, s_g, p_g, ds_g, so_ref, sd_ref, ro_ref, rd_ref, o_nat, dqkv_nat,
                 dwp_ref, dws_ref, part_ref, px_ref, acc_ref, rs0_ref, rs1_ref, rs2_ref, sm_ref, sm_out,
                 loc, sib_send, sib_recv, h_send, h_recv, do_send, do_recv, o_send, o_recv, d_send, d_recv,
                 s_send, s_recv, w_send, w_recv, g_send, g_recv, ws_send, ws_recv, gs_send, gs_recv, r_send, r_recv):
    pc = Place()
    mk, mj = Marks(), Marks()
    barrier_signal(pc)

    def w_load(r):
        return pltpu.make_async_copy(wqkv_hbm.at[r * T:(r + 1) * T], dqkv_nat, loc.at[r])

    wo_load = pltpu.make_async_copy(wout_hbm, wout_ref, loc.at[2])
    w_load(0).start()
    wo_load.start()
    gamma = gamma_ref[...].reshape(1, D).astype(F32)
    beta = beta_ref[...].reshape(1, D).astype(F32)
    bout = bout_ref[...].reshape(1, D).astype(F32)
    bqkv = bqkv_ref[...].reshape(1, D3).astype(F32)

    def rows_of(core):
        return pl.ds(pl.multiple_of(core * L, L), L)

    def norm(xb):
        return (centre(xb)[1] * gamma + beta).astype(BF)

    def sib_copy(j):
        return rcopy(out_ref.at[j], hg_ref.at[pc.chip, j, rows_of(pc.core)], sib_send.at[j], sib_recv.at[j], pc.sib)

    for j in range(2):
        out_ref[j] = norm(x_ref[2 * (1 - pc.core) + j])
    for j in range(2):
        hg_ref[pc.chip, j, rows_of(pc.core)] = norm(x_ref[2 * pc.core + j])
    mk('barrier')
    barrier_wait()
    for j in range(2):
        sib_copy(j).start()

    h_rows, w_rows, o_rows = span(H_ROWS), span(W_ROWS), span(O_ROWS)

    def h_tree(j):
        slot = lambda c, p: hg_ref.at[c, j, h_rows(p)]
        return Tree(pc, lambda p: slot(pc.chip, p), slot, hg_ref.at[0:7, j], h_send.at[j], h_recv.at[j])

    def sib_arrive(j):
        at = hg_ref.at[pc.chip, j, rows_of(1 - pc.core)]
        rcopy(at, at, sib_send.at[j], sib_recv.at[j], pc.sib).wait_recv()

    do_out = do_ref.reshape(N, 2, L, L)

    def swap(src, dst, send, recv, j):
        return Exchange(pc, lambda t: src(t, j), lambda t: dst.at[j, t], dst.at[j, 0:N - 1], send.at[j], recv.at[j])

    def do_swap(j):
        return swap(lambda t, j: do_out.at[t, j], dog_ref, do_send, do_recv, j)

    def o_swap(j):
        return swap(lambda t, j: so_ref.at[j, t], ro_ref, o_send, o_recv, j)

    def d_swap(j):
        return swap(lambda t, j: sd_ref.at[j, t], rd_ref, d_send, d_recv, j)

    mk('sibwait')
    trees = [h_tree(0), h_tree(1)]
    sib_arrive(0)
    trees[0].start_own()
    pos = head_places(kind_ref)
    perm = []
    for j in range(N):
        v = 0
        for n in range(1, N):
            v = v + jnp.where(pos[n] == j, n, 0)
        perm.append(v)
    f = g = 0
    for c in R8:
        f = f + jnp.where(pc.chip == c, perm[c], 0)
        g = g + jnp.where(pc.chip == c, perm[8 + c], 0)
    mk('dO_mm')
    wo_load.wait()
    dy_all = dy_ref[...].reshape(T, D)
    for c in R4:
        for u in range(2):
            wp_ref[u * L:u * L + 64] = wout_ref[perm[2 * c + u]]
            wp_ref[u * L + 64:u * L + L] = wout_ref[perm[8 + 2 * c + u]]
        d = dot_nt(dy_all, wp_ref[...]).astype(BF)
        for u in range(2):
            do_ref[2 * c + u] = d[:, u * L:(u + 1) * L].reshape(4, L, L)
    mk('t0_h0')
    for e in trees[0].hops(0):
        trees[0].arrive(e)
    mk('wsel')
    do_swap(0).start()
    for j in range(2):
        dog_ref[j, pc.me] = do_out[pc.me, j]

    def w_cols(t, k, head):
        out = None
        for m in R8:
            cur = dqkv_nat[k * L:(k + 1) * L, t * D + m * L:t * D + (m + 1) * L]
            out = cur if out is None else jnp.where(head // 2 == m, cur, out)
        return out

    for r in range(2):
        w_load(r).wait()
        for t in R3:
            for k in R4:
                w_ref[r * T + k * L:r * T + (k + 1) * L, t * L:(t + 1) * L] = pair_halves(
                    w_cols(t, k, f), f % 2, w_cols(t, k, g), g % 2)
        if r == 0:
            w_load(1).start()
    for t in R3:
        halves = []
        for head in (f, g):
            out = None
            for m in R8:
                cur = bqkv[:, t * D + m * L:t * D + (m + 1) * L]
                out = cur if out is None else jnp.where(head // 2 == m, cur, out)
            halves += [out, head % 2]
        bias_ref[:, t * L:(t + 1) * L] = jnp.broadcast_to(pair_halves(*halves), (8, L))
    dwp_ref[...] = jnp.zeros_like(dwp_ref)
    mk('t0_h1')
    for e in trees[0].hops(1):
        trees[0].arrive(e)
    sib_arrive(1)
    trees[1].start_own()

    lane = lax.broadcasted_iota(jnp.int32, (QB, L), 1)
    row_i = lax.broadcasted_iota(jnp.int32, (QB, QB), 0)
    col_i = lax.broadcasted_iota(jnp.int32, (QB, QB), 1)

    def head_block(j, i, hd):
        s_ref, p_ref, ds_ref = ((s_f, p_f, ds_f), (s_g, p_g, ds_g))[hd]
        first = 0 if hd == 0 else max(0, i - 2)
        blocks = range(first, i + 1)
        mine = (lane < 64) if hd == 0 else (lane >= 64)
        qi = qkv_ref[i * QB:(i + 1) * QB, 0:L] * BF(0.125)
        doi = dog_ref[j, 2 * i:2 * i + 2].reshape(QB, L)
        qm = jnp.where(mine, qi, BF(0))
        dom = jnp.where(mine, doi, BF(0))
        k_at = lambda kb: qkv_ref[kb * QB:(kb + 1) * QB, L:2 * L]
        v_at = lambda kb: qkv_ref[kb * QB:(kb + 1) * QB, 2 * L:3 * L]
        at = lambda kb: slice((kb - first) * QB, (kb - first + 1) * QB)
        mx = None
        for kb in blocks:
            s = dot_nt(qm, k_at(kb))
            if kb == i:
                s = jnp.where(col_i <= row_i, s, NEG_BIG)
            if hd == 1 and kb == i - 2:
                s = jnp.where(col_i > row_i, s, NEG_BIG)
            s_ref[:, at(kb)] = s
            cur = jnp.maximum(s[:, :L], s[:, L:])
            mx = cur if mx is None else jnp.maximum(mx, cur)
        m = jnp.max(mx, axis=1, keepdims=True)
        ls = None
        for kb in blocks:
            e = jnp.exp(s_ref[:, at(kb)] - m)
            s_ref[:, at(kb)] = e
            cur = e[:, :L] + e[:, L:]
            ls = cur if ls is None else ls + cur
        rl = 1.0 / jnp.sum(ls, axis=1, keepdims=True)
        acc = None
        for kb in blocks:
            p_ = s_ref[:, at(kb)] * rl
            s_ref[:, at(kb)] = p_
            pb = p_.astype(BF)
            p_ref[:, at(kb)] = pb
            cur = dot_nn(pb, v_at(kb))
            acc = cur if acc is None else acc + cur
        dsum = jnp.sum(dom.astype(F32) * acc, axis=1, keepdims=True)
        dq = None
        for kb in blocks:
            dp = dot_nt(dom, v_at(kb)).astype(BF).astype(F32)
            ds = (s_ref[:, at(kb)] * (dp - dsum)).astype(BF)
            ds_ref[:, at(kb)] = ds
            cur = dot_nn(ds, k_at(kb))
            dq = cur if dq is None else dq + cur
        hr = slice(hd * 64, hd * 64 + 64)
        n = len(blocks) * QB
        keys = slice(first * QB, first * QB + n)
        dvt_ref[hr, keys] += dot_nn(dot_ref[hr, i * QB:(i + 1) * QB], p_ref[:, :n])
        dkt_ref[hr, keys] += dot_nn(qt_ref[hr, i * QB:(i + 1) * QB], ds_ref[:, :n])
        return acc, dq * 0.125

    def batch_step(j, carry):
        mj('t_h2')
        last = h_tree(j)
        for e in last.hops(2):
            last.arrive(e)
        do_swap(j).wait()

        @pl.when(j == 1)
        def _():
            o_swap(0).start()
            d_swap(0).start()

        def qkv_step(r, c):
            rows = hg_ref[pl.ds(2 * r, 2), j].reshape(T, D)
            out = dot_nn(rows, w_ref[...]) + bias_ref[0:1, :]
            qkv_ref[pl.ds(pl.multiple_of(r * T, T), T), :] = out.astype(BF)
            return c

        mj('qkv')
        lax.fori_loop(0, 4, qkv_step, 0)

        mj('transp')
        for i in R8:
            qs = qkv_ref[i * QB:(i + 1) * QB, 0:L] * BF(0.125)
            qt_ref[:, i * QB:(i + 1) * QB] = qs.T
            dot_ref[:, i * QB:(i + 1) * QB] = dog_ref[j, 2 * i:2 * i + 2].reshape(QB, L).T
        dkt_ref[...] = jnp.zeros_like(dkt_ref)
        dvt_ref[...] = jnp.zeros_like(dvt_ref)
        for i in R8:
            mj('att')
            of, dqf = head_block(j, i, 0)
            og, dqg = head_block(j, i, 1)
            o = jnp.where(lane < 64, of, og).astype(BF)
            dq = jnp.where(lane < 64, dqf, dqg).astype(BF)
            for u in range(2):
                so_ref[j, 2 * i + u] = o[u * L:(u + 1) * L]
                sd_ref[j, 2 * i + u, 0] = dq[u * L:(u + 1) * L]
            dqkv_ref[i * QB:(i + 1) * QB, 0:L] = dq
            mj('when3')
            if i == 3:
                @pl.when(j == 0)
                def _():
                    for e in trees[1].hops(0):
                        trees[1].arrive(e)
                    do_swap(1).start()

        mj('dkdv')
        for t, src in ((1, dkt_ref), (2, dvt_ref)):
            for n in range(N):
                d = src[:, n * L:(n + 1) * L].T.astype(BF)
                sd_ref[j, n, t] = d
                dqkv_ref[n * L:(n + 1) * L, t * L:(t + 1) * L] = d
        ro_ref[j, pc.me] = so_ref[j, pc.me]
        rd_ref[j, pc.me] = sd_ref[j, pc.me]

        mj('when')
        @pl.when(j == 0)
        def _():
            for e in trees[1].hops(1):
                trees[1].arrive(e)

        @pl.when(j == 1)
        def _():
            o_swap(1).start()

        def dw_step(r, c):
            cols = pl.ds(pl.multiple_of(r * QB, QB), QB)
            dwp_ref[cols, :] += dot_tn(hg_ref[:, j, :, cols].reshape(S, QB), dqkv_ref[...])
            return c

        mj('dw')
        lax.fori_loop(0, 4, dw_step, 0)
        dwp_ref[D:D + 1, :] += jnp.sum(dqkv_ref[...].astype(F32), axis=0, keepdims=True)
        mj(None)
        return carry

    mk(None)
    lax.fori_loop(0, 2, batch_step, 0)

    def half_of(core):
        return dwp_ref.at[pl.ds(pl.multiple_of(core * HR, 8), HR)]

    def to_sib(n, src, dst, send, recv):
        cp = rcopy(src, dst, send.at[n], recv.at[n], pc.sib)
        cp.start()
        return cp

    half = to_sib(2, half_of(1 - pc.core), dws_ref, sib_send, sib_recv)
    mk('tree_fin')
    for j in range(2):
        trees[j].finish()
        do_swap(j).finish()
    w_flat = hg_ref.reshape(2 * S, D)
    w_loads = [pltpu.make_async_copy(wqkv_hbm.at[:, t * D:(t + 1) * D], w_flat.at[t * D:(t + 1) * D], loc.at[3 + t]) for t in R3]
    for cp in w_loads:
        cp.start()
    half.wait_recv()
    dws_ref[...] += half_of(pc.core)[...]

    def w_slot(c, p, core=pc.core):
        return dwg_ref.at[c, core, w_rows(p)]

    def g_slot(c, p, core=pc.core):
        return dwo_ref.at[core, c, o_rows(p)]

    wtree = Tree(pc, lambda p: dws_ref.at[w_rows(p)], w_slot, dwg_ref.at[0:7, pc.core], w_send.at[0], w_recv)
    wtree.start_own((0,))
    keep_w = pltpu.make_async_copy(dws_ref, dwg_ref.at[pc.chip, pc.core], loc.at[0])
    keep_w.start()
    for p in R3:
        to_sib(0, dws_ref.at[w_rows(p)], w_slot(pc.chip, p), ws_send, ws_recv)

    mk('o_wait')
    for j in range(2):
        o_swap(j).wait()
    for b in R4:
        for m in R8:
            o_nat[b * L:(b + 1) * L, m * L:(m + 1) * L] = gather_heads(lambda j, q: ro_ref[j, q], pos, b, m)

    def wout_part(core, c):
        cols = pl.ds(pl.multiple_of(core * T + c * QB, QB), QB)
        return dot_tn(o_nat[:, cols], dy_all)

    mk('part')
    for c in range(2):
        part_ref[c * QB:(c + 1) * QB] = wout_part(1 - pc.core, c)
    xp = to_sib(3, part_ref, px_ref, sib_send, sib_recv)
    for c in range(2):
        acc_ref[4 * c:4 * c + 4] = wout_part(pc.core, c).reshape(4, 64, D)
    mk('xp_wait')
    xp.wait_recv()
    acc_ref[...] += px_ref[...].reshape(8, 64, D)

    bufs = (rs0_ref, rs1_ref, rs2_ref)

    def reduce_step(s, wait):
        for p in R3:
            order = [(p + j) % 3 for j in R3]
            if wait:
                at = bufs[s].at[:, o_rows(p)]
                rcopy(at, at, r_send.at[0], r_recv.at[s * 3 + p], pc.sib).wait_recv()
            for i, sub in enumerate(subsets(order[s + 1:])):
                if wait:
                    acc_ref[pc.chip_at(sub), o_rows(p)] += bufs[s][i, o_rows(p)]
                else:
                    rcopy(acc_ref.at[pc.chip_at((order[s],) + sub), o_rows(p)], bufs[s].at[i, o_rows(p)],
                          r_send.at[0], r_recv.at[s * 3 + p], pc.next_dev(order[s])).start()

    reduce_step(0, False)
    wtree.start_own((1, 2))
    def pass_on(tree, slot, n, send, recv):
        for e in tree.hops(n):
            c, p = tree.arrive(e)
            to_sib(0, slot(c, p), slot(c, p), send, recv)

    mk('y')
    dbo = jnp.zeros((1, D), F32)
    for b in R4:
        rows = slice(b * L, (b + 1) * L)
        y_ref[b] = (x_ref[b].astype(F32) + dot_nn(o_nat[rows], wout_ref.reshape(D, D)[...]) + bout).astype(BF)
        dbo += jnp.sum(dy_ref[b].astype(F32), axis=0, keepdims=True)
    mk('rs0_wait')
    reduce_step(0, True)
    reduce_step(1, False)
    mk('d_start')
    d_swap(1).start(1, 9)
    mk('rs1_wait')
    reduce_step(1, True)
    reduce_step(2, False)
    d_swap(1).start(9)
    mk('rs2_wait')
    reduce_step(2, True)
    gtree = Tree(pc, lambda p: acc_ref.at[pc.chip, o_rows(p)], g_slot, dwo_ref.at[pc.core, 0:7], g_send.at[0], g_recv)
    gtree.start_own()
    keep_g = pltpu.make_async_copy(acc_ref.at[pc.chip], dwo_ref.at[pc.core, pc.chip], loc.at[1])
    keep_g.start()
    for p in R3:
        to_sib(0, acc_ref.at[pc.chip, o_rows(p)], g_slot(pc.chip, p), gs_send, gs_recv)

    mk('w_h0')
    pass_on(wtree, w_slot, 0, ws_send, ws_recv)
    for j in range(2):
        d_swap(j).wait()

    def spread(b, c):
        rows = pl.ds(pl.multiple_of(b * L, L), L)
        for m in R8:
            for t in R3:
                dqkv_nat[rows, t * D + m * L:t * D + (m + 1) * L] = gather_heads(lambda j, q: rd_ref[j, q, t], pos, b, m)
        return c

    def back(b, c):
        dg, db = c
        rows = pl.ds(pl.multiple_of(b * L, L), L)
        _, xhat, rstd = centre(x_ref[b])
        dh = None
        for t in R3:
            cur = dot_nt(dqkv_nat[rows, t * D:(t + 1) * D], w_flat[t * D:(t + 1) * D])
            dh = cur if dh is None else dh + cur
        dh = dh.astype(BF).astype(F32)
        dxh = dh * gamma
        m1 = jnp.mean(dxh, axis=-1, keepdims=True)
        m2 = jnp.mean(dxh * xhat, axis=-1, keepdims=True)
        dx_ref[b] = (dy_ref[b].astype(F32) + rstd * (dxh - m1 - xhat * m2)).astype(BF)
        return dg + jnp.sum(dh * xhat, axis=0, keepdims=True), db + jnp.sum(dh, axis=0, keepdims=True)

    mk('spread')
    lax.fori_loop(0, 4, spread, 0)
    mk('wload_wait')
    for cp in w_loads:
        cp.wait()
    mk('dh1')
    dgb = lax.fori_loop(0, 2, back, (jnp.zeros((1, D), F32), jnp.zeros((1, D), F32)))
    mk('g_h0')
    pass_on(gtree, g_slot, 0, gs_send, gs_recv)
    mk('dh2')
    dg, db = lax.fori_loop(2, 4, back, dgb)
    row = lax.broadcasted_iota(jnp.int32, (4, D), 0)
    sm_out[...] = jnp.where(row == 0, dg, jnp.where(row == 1, db, jnp.where(row == 2, dbo, 0.0)))
    sm_ref[pc.me] = sm_out[...]
    s_swap = Exchange(pc, lambda t: sm_out, lambda t: sm_ref.at[t], sm_ref.at[0:N - 1], s_send.at[0], s_recv.at[0])
    s_swap.start()
    mk('w_h1')
    pass_on(wtree, w_slot, 1, ws_send, ws_recv)
    mk('g_h1')
    pass_on(gtree, g_slot, 1, gs_send, gs_recv)
    mk('s_wait')
    s_swap.wait()
    tot = sm_ref[0]
    for n in range(1, N):
        tot = tot + sm_ref[n]
    small_ref[...] = tot
    mk('g_h2')
    pass_on(gtree, g_slot, 2, gs_send, gs_recv)
    mk('w_h2')
    pass_on(wtree, w_slot, 2, ws_send, ws_recv)
    mk('sib_waits')
    for tree, at, got, send, recv in (
            (wtree, dwg_ref.at[:, pc.core], dwg_ref.at[:, 1 - pc.core], ws_send, ws_recv),
            (gtree, dwo_ref.at[pc.core], dwo_ref.at[1 - pc.core], gs_send, gs_recv)):
        rcopy(got, got, send.at[0], recv.at[0], pc.sib).wait_recv()
        rcopy(at, at, send.at[0], recv.at[0], pc.sib).wait_send()
        tree.finish()
    mk('final')
    for j in range(2):
        sib_copy(j).wait_send()
        o_swap(j).finish()
        d_swap(j).finish()
    s_swap.finish()
    half.wait_send()
    xp.wait_send()
    rcopy(acc_ref.at[0:7], acc_ref.at[0:7], r_send.at[0], r_recv.at[0], pc.sib).wait_send()
    keep_w.wait()
    keep_g.wait()
    mk(None)


def layer_call(kind, x, dy, gamma, beta, bout, bqkv, wqkv, wout):
    vm, sm, hb = (pl.BlockSpec(memory_space=m) for m in (pltpu.VMEM, pltpu.SMEM, pl.ANY))
    sem = pltpu.SemaphoreType.DMA
    tok = jax.ShapeDtypeStruct((4, L, D), BF)

    def pair(*n):
        return [sem(n), sem(n)]

    def bf(*n):
        return pltpu.VMEM(n, BF)

    def ff(*n):
        return pltpu.VMEM(n, F32)

    band = 3 * QB
    return pl.pallas_call(
        layer_kernel,
        out_shape=(tok, tok, jax.ShapeDtypeStruct((4, D), F32), jax.ShapeDtypeStruct((8, 2, HR, W3), F32),
                   jax.ShapeDtypeStruct((2, 8, 64, D), F32)),
        in_specs=[sm] + [vm] * 6 + [hb, hb],
        out_specs=(vm, vm, vm, hb, hb),
        scratch_shapes=[
            bf(8, 2, QB, D), bf(2, L, D), bf(N, 64, D), bf(QB, D), bf(8, 4, L, L), bf(2, N, L, L), bf(D, W3), ff(8, W3),
            bf(S, W3), bf(S, W3), bf(L, S), bf(L, S), ff(L, S), ff(L, S),
            ff(QB, S), bf(QB, S), bf(QB, S), ff(QB, band), bf(QB, band), bf(QB, band),
            bf(2, N, L, L), bf(2, N, 3, L, L), bf(2, N, L, L), bf(2, N, 3, L, L), bf(T, D), bf(T, D3),
            ff(DR, W3), ff(HR, W3), ff(T, D), ff(T, D), ff(8, 64, D),
            ff(4, 64, D), ff(2, 64, D), ff(1, 64, D), ff(N, 4, D), ff(4, D), sem((6,))]
        + pair(4) + [sem((2,)), sem((2, 21))] + pair(2) + pair(2) + pair(2) + pair(1)
        + [sem((1,)), sem((21,))] + [sem((1,)), sem((21,))] + pair(1) + pair(1) + [sem((1,)), sem((9,))],
        compiler_params=pltpu.CompilerParams(vmem_limit_bytes=VMEM_CAP, collective_id=0, has_side_effects=True),
        name="layer",
    )(kind, x, dy, gamma, beta, bout, bqkv, wqkv, wout)


def unpack_kernel(kind_ref, dw_hbm, dwo_hbm, y_in, dx_in, small_ref,
                  out_hbm, wo_hbm, y_out, dx_out, bias_ref, dg_ref, db_ref, dbo_ref,
                  in_ref, ob_ref, bias_in, wo_ref, y_ref, dx_ref, in_sem, out_sem, pass_in, pass_out):
    pos = head_places(kind_ref)

    def rows(r):
        return pl.ds(pl.multiple_of(r * L, L), L)

    def load(r):
        return pltpu.make_async_copy(dw_hbm.at[:, rows(r)], in_ref.at[r], in_sem.at[r])

    def store(r):
        return pltpu.make_async_copy(ob_ref.at[r], out_hbm.at[rows(r)], out_sem.at[r])

    def through(i):
        src, buf, dst = ((dwo_hbm, wo_ref, wo_hbm), (y_in, y_ref, y_out), (dx_in, dx_ref, dx_out))[i]
        return pltpu.make_async_copy(src, buf, pass_in.at[i]), pltpu.make_async_copy(buf, dst, pass_out.at[i])

    bias_load = pltpu.make_async_copy(dw_hbm.at[:, D:D + 8], bias_in, pass_in.at[3])
    for r in R3:
        load(r).start()
    bias_load.start()
    for i in R3:
        through(i)[0].start()

    def pick(read, t, m):
        pa, pb = pos[2 * m], pos[2 * m + 1]
        cols = slice(t * L, (t + 1) * L)
        a, b = read(pa % 8, cols), read(pb % 8, cols)
        lane = lax.broadcasted_iota(jnp.int32, a.shape, 1)
        a = jnp.where(pa // 8 == 1, pltpu.roll(a, 64, 1), a)
        b = jnp.where(pb // 8 == 0, pltpu.roll(b, 64, 1), b)
        return jnp.where(lane < 64, a, b)

    def step(r, c):
        load(r).wait()

        @pl.when(r < 5)
        def _():
            load(r + 3).start()

        for t in R3:
            for m in R8:
                ob_ref[r, :, t * D + m * L:t * D + (m + 1) * L] = pick(lambda q, cols: in_ref[r, q, :, cols], t, m)
        store(r).start()
        return c

    lax.fori_loop(0, 8, step, 0)
    for i in R3:
        get, put = through(i)
        get.wait()
        put.start()
    bias_load.wait()
    for t in R3:
        for m in R8:
            bias_ref[t * D + m * L:t * D + (m + 1) * L] = pick(lambda q, cols: bias_in[q, :, cols], t, m)[0]
    for i, ref in enumerate((dg_ref, db_ref, dbo_ref)):
        ref[...] = small_ref[i]
    for r in R8:
        store(r).wait()
    for i in R3:
        through(i)[1].wait()


def unpack_call(kind, dwg, dwo, small, y, dx):
    vm, sm, hb = (pl.BlockSpec(memory_space=m) for m in (pltpu.VMEM, pltpu.SMEM, pl.ANY))
    sem = pltpu.SemaphoreType.DMA
    vec = jax.ShapeDtypeStruct((D,), F32)
    tok = jax.ShapeDtypeStruct((4, L, D), BF)
    return pl.pallas_call(
        unpack_kernel,
        in_specs=[sm, hb, hb, hb, hb, vm],
        out_specs=[hb, hb, hb, hb, vm, vm, vm, vm],
        out_shape=[jax.ShapeDtypeStruct((D, D3), F32), jax.ShapeDtypeStruct((D, D), F32), tok, tok,
                   jax.ShapeDtypeStruct((D3,), F32), vec, vec, vec],
        scratch_shapes=[
            pltpu.VMEM((8, 8, L, W3), F32), pltpu.VMEM((8, L, D3), F32), pltpu.VMEM((8, 8, W3), F32),
            pltpu.VMEM((D, D), F32), pltpu.VMEM((4, L, D), BF), pltpu.VMEM((4, L, D), BF),
            sem((8,)), sem((8,)), sem((4,)), sem((3,))],
        compiler_params=pltpu.CompilerParams(vmem_limit_bytes=VMEM_CAP),
        name="unpack",
    )(kind, dwg, dwo, y, dx, small)


def solution(mesh):
    tok_spec = P(None, "sp", None)

    def local_block(x, d_y, ln_gamma, ln_beta, w_qkv, b_qkv, w_out, b_out, head_kind):
        y, dx, small, dwg, dwo = layer_call(head_kind, x, d_y, ln_gamma, ln_beta, b_out, b_qkv, w_qkv, w_out.reshape(N, 64, D))
        dw, dwout, y, dx, dbias, dg, db, dbo = unpack_call(
            head_kind, dwg.reshape(8, DR, W3), dwo.reshape(D, D), small, y, dx)
        return y, dx, dg, db, dw, dbias, dwout, dbo

    return jax.shard_map(
        local_block, mesh=mesh,
        in_specs=(tok_spec, tok_spec, P(), P(), P(), P(), P(), P(), P()),
        out_specs=(tok_spec, tok_spec, P(), P(), P(), P(), P(), P()), check_vma=False)
```

```python
import functools
import math

import jax
import jax.numpy as jnp
from jax import lax
from jax.experimental import pallas as pl
from jax.experimental.pallas import tpu as pltpu
from jax.sharding import PartitionSpec as P

LN_EPS = 1e-5
NEG_BIG = -1e30
BF = jnp.bfloat16
F32 = jnp.float32
QB = 256
L = 128
W3 = 384
T = 512
D = 1024
DR = 1040
HR = 520
N = 16
R3, R4, R8 = range(3), range(4), range(8)
MESH = pl.DeviceIdType.MESH
H_ROWS = (0, 96, 176, 256)
W_ROWS = (0, 176, 352, 520)
O_ROWS = (0, 24, 48, 64)
S = 2048
D3 = 3072
VMEM_CAP = 63 * D * D


def dot_nn(a, b):
    return lax.dot_general(a, b, (((1,), (0,)), ((), ())), preferred_element_type=F32)


def dot_nt(a, b):
    return lax.dot_general(a, b, (((1,), (1,)), ((), ())), preferred_element_type=F32)


def dot_tn(a, b):
    return lax.dot_general(a, b, (((0,), (0,)), ((), ())), preferred_element_type=F32)


def swap_halves(a):
    return jnp.concatenate([a[:, 64:], a[:, :64]], axis=1)


def pair_halves(a, a_half, b, b_half):
    lane = lax.broadcasted_iota(jnp.int32, a.shape, 1)
    a = jnp.where(a_half == 1, swap_halves(a), a)
    b = jnp.where(b_half == 0, swap_halves(b), b)
    return jnp.where(lane < 64, a, b)


class Place:
    def __init__(self):
        self.me = lax.axis_index("sp")
        self.core, self.chip = self.me % 2, self.me // 2
        self.sib = self.me + 1 - 2 * self.core
        bits = (self.chip % 2, self.chip // 2 % 2, self.chip // 4)
        self.step = [(1 - 2 * v) * w for v, w in zip(bits, (1, 2, 4))]

    def chip_at(self, axes):
        out = self.chip
        for a in axes:
            out = out + self.step[a]
        return out

    def next_dev(self, axis):
        return self.me + 2 * self.step[axis]


def rcopy(src, dst, send, recv, dev):
    return pltpu.make_async_remote_copy(
        src_ref=src, dst_ref=dst, send_sem=send, recv_sem=recv, device_id=(dev,), device_id_type=MESH)


def subsets(axes):
    out = [()]
    for a in axes:
        out += [v + (a,) for v in out]
    return out


class Tree:
    def __init__(self, place, own, slot, seven, send, recv):
        self.place, self.own, self.slot, self.seven, self.send, self.recv = place, own, slot, seven, send, recv
        self.entries = []
        for s in R3:
            for p in R3:
                order = [(p + j) % 3 for j in R3]
                for sub in subsets(order[:s]):
                    self.entries.append((p, order[s], sub))

    def copy(self, e):
        p, axis, sub = e
        i = self.entries.index(e)
        at = self.slot(self.place.chip_at(sub), p)
        return rcopy(at if sub else self.own(p), at, self.send, self.recv.at[i], self.place.next_dev(axis))

    def start_own(self, levels=R3):
        for e in self.hops(0):
            if (e[1] - e[0]) % 3 in levels:
                self.copy(e).start()

    def arrive(self, e):
        p, axis, sub = e
        got = sub + (axis,)
        chip = self.place.chip_at(got)
        at = self.slot(chip, p)
        i = self.entries.index(e)
        rcopy(at, at, self.send, self.recv.at[i], self.place.next_dev(axis)).wait_recv()
        for n in self.entries:
            if n[0] == p and n[2] == got:
                self.copy(n).start()
        return chip, p

    def hops(self, n):
        return [e for e in self.entries if len(e[2]) == n]

    def finish(self):
        rcopy(self.seven, self.seven, self.send, self.recv.at[0], self.place.me).wait_send()


def barrier_signal(place):
    sem = pltpu.get_barrier_semaphore()
    for r in range(1, N):
        pl.semaphore_signal(sem, inc=1, device_id=((place.me + r) % N,), device_id_type=MESH)


def barrier_wait():
    pl.semaphore_wait(pltpu.get_barrier_semaphore(), N - 1)


def head_places(kind_ref):
    pos, zeros, ones = [], 0, 8
    for n in range(N):
        k = kind_ref[n]
        pos.append(jnp.where(k == 0, zeros, ones))
        zeros, ones = zeros + 1 - k, ones + k
    return pos


class Exchange:
    def __init__(self, place, src, dst, rest, send, recv):
        self.place, self.src, self.dst, self.send, self.recv = place, src, dst, send, recv
        self.rest = rest

    def start(self, first=1, end=N):
        me = self.place.me
        for r in range(first, end):
            to = (me + r) % N
            rcopy(self.src(to), self.dst(me), self.send, self.recv, to).start()

    def wait(self):
        rcopy(self.rest, self.rest, self.send, self.recv, self.place.me).wait_recv()

    def finish(self):
        rcopy(self.rest, self.rest, self.send, self.recv, self.place.me).wait_send()


def gather_heads(recv_at, pos, b, m):
    pa, pb = pos[2 * m], pos[2 * m + 1]
    k, j = b // 2, b % 2
    a = recv_at(j, 2 * (pa % 8) + k)
    c = recv_at(j, 2 * (pb % 8) + k)
    return pair_halves(a, pa // 8, c, pb // 8)


def span(tab):
    return lambda p: pl.ds(tab[p], tab[p + 1] - tab[p])


def centre(xb):
    xf = xb.astype(F32)
    cen = xf - jnp.mean(xf, axis=-1, keepdims=True)
    rstd = lax.rsqrt(jnp.mean(cen * cen, axis=-1, keepdims=True) + LN_EPS)
    return xf, cen * rstd, rstd


def layer_kernel(kind_ref, x_ref, dy_ref, gamma_ref, beta_ref, bout_ref, bqkv_ref, wqkv_hbm, wout_hbm,
                 y_ref, dx_ref, small_ref, dwg_ref, dwo_ref,
                 hg_ref, out_ref, wout_ref, wp_ref, do_ref, dog_ref, w_ref, bias_ref, qkv_ref, dqkv_ref, qt_ref, dot_ref,
                 dkt_ref, dvt_ref, s_f, p_f, ds_f, s_g, p_g, ds_g, so_ref, sd_ref, ro_ref, rd_ref, o_nat, dqkv_nat,
                 dwp_ref, dws_ref, part_ref, px_ref, acc_ref, rs0_ref, rs1_ref, rs2_ref, sm_ref, sm_out,
                 loc, sib_send, sib_recv, h_send, h_recv, do_send, do_recv, o_send, o_recv, d_send, d_recv,
                 s_send, s_recv, w_send, w_recv, g_send, g_recv, ws_send, ws_recv, gs_send, gs_recv, r_send, r_recv):
    pc = Place()
    barrier_signal(pc)

    def w_load(r):
        return pltpu.make_async_copy(wqkv_hbm.at[r * T:(r + 1) * T], dqkv_nat, loc.at[r])

    wo_load = pltpu.make_async_copy(wout_hbm, wout_ref, loc.at[2])
    w_load(0).start()
    wo_load.start()
    gamma = gamma_ref[...].reshape(1, D).astype(F32)
    beta = beta_ref[...].reshape(1, D).astype(F32)
    bout = bout_ref[...].reshape(1, D).astype(F32)
    bqkv = bqkv_ref[...].reshape(1, D3).astype(F32)

    def rows_of(core):
        return pl.ds(pl.multiple_of(core * L, L), L)

    def norm(xb):
        return (centre(xb)[1] * gamma + beta).astype(BF)

    def sib_copy(j):
        return rcopy(out_ref.at[j], hg_ref.at[pc.chip, j, rows_of(pc.core)], sib_send.at[j], sib_recv.at[j], pc.sib)

    for j in range(2):
        out_ref[j] = norm(x_ref[2 * (1 - pc.core) + j])
    for j in range(2):
        hg_ref[pc.chip, j, rows_of(pc.core)] = norm(x_ref[2 * pc.core + j])
    barrier_wait()
    for j in range(2):
        sib_copy(j).start()

    h_rows, w_rows, o_rows = span(H_ROWS), span(W_ROWS), span(O_ROWS)

    def h_tree(j):
        slot = lambda c, p: hg_ref.at[c, j, h_rows(p)]
        return Tree(pc, lambda p: slot(pc.chip, p), slot, hg_ref.at[0:7, j], h_send.at[j], h_recv.at[j])

    def sib_arrive(j):
        at = hg_ref.at[pc.chip, j, rows_of(1 - pc.core)]
        rcopy(at, at, sib_send.at[j], sib_recv.at[j], pc.sib).wait_recv()

    do_out = do_ref.reshape(N, 2, L, L)

    def swap(src, dst, send, recv, j):
        return Exchange(pc, lambda t: src(t, j), lambda t: dst.at[j, t], dst.at[j, 0:N - 1], send.at[j], recv.at[j])

    def do_swap(j):
        return swap(lambda t, j: do_out.at[t, j], dog_ref, do_send, do_recv, j)

    def o_swap(j):
        return swap(lambda t, j: so_ref.at[j, t], ro_ref, o_send, o_recv, j)

    def d_swap(j):
        return swap(lambda t, j: sd_ref.at[j, t], rd_ref, d_send, d_recv, j)

    trees = [h_tree(0), h_tree(1)]
    sib_arrive(0)
    trees[0].start_own()
    pos = head_places(kind_ref)
    perm = []
    for j in range(N):
        v = 0
        for n in range(1, N):
            v = v + jnp.where(pos[n] == j, n, 0)
        perm.append(v)
    f = g = 0
    for c in R8:
        f = f + jnp.where(pc.chip == c, perm[c], 0)
        g = g + jnp.where(pc.chip == c, perm[8 + c], 0)
    wo_load.wait()
    dy_all = dy_ref[...].reshape(T, D)
    for c in R4:
        for u in range(2):
            wp_ref[u * L:u * L + 64] = wout_ref[perm[2 * c + u]]
            wp_ref[u * L + 64:u * L + L] = wout_ref[perm[8 + 2 * c + u]]
        d = dot_nt(dy_all, wp_ref[...]).astype(BF)
        for u in range(2):
            do_ref[2 * c + u] = d[:, u * L:(u + 1) * L].reshape(4, L, L)
    for e in trees[0].hops(0):
        trees[0].arrive(e)
    do_swap(0).start()
    for j in range(2):
        dog_ref[j, pc.me] = do_out[pc.me, j]

    def w_cols(t, k, head):
        out = None
        for m in R8:
            cur = dqkv_nat[k * L:(k + 1) * L, t * D + m * L:t * D + (m + 1) * L]
            out = cur if out is None else jnp.where(head // 2 == m, cur, out)
        return out

    for r in range(2):
        w_load(r).wait()
        for t in R3:
            for k in R4:
                w_ref[r * T + k * L:r * T + (k + 1) * L, t * L:(t + 1) * L] = pair_halves(
                    w_cols(t, k, f), f % 2, w_cols(t, k, g), g % 2)
        if r == 0:
            w_load(1).start()
    for t in R3:
        halves = []
        for head in (f, g):
            out = None
            for m in R8:
                cur = bqkv[:, t * D + m * L:t * D + (m + 1) * L]
                out = cur if out is None else jnp.where(head // 2 == m, cur, out)
            halves += [out, head % 2]
        bias_ref[:, t * L:(t + 1) * L] = jnp.broadcast_to(pair_halves(*halves), (8, L))
    dwp_ref[...] = jnp.zeros_like(dwp_ref)
    for e in trees[0].hops(1):
        trees[0].arrive(e)
    sib_arrive(1)
    trees[1].start_own()

    lane = lax.broadcasted_iota(jnp.int32, (QB, L), 1)
    row_i = lax.broadcasted_iota(jnp.int32, (QB, QB), 0)
    col_i = lax.broadcasted_iota(jnp.int32, (QB, QB), 1)

    def head_block(j, i, hd):
        s_ref, p_ref, ds_ref = ((s_f, p_f, ds_f), (s_g, p_g, ds_g))[hd]
        first = 0 if hd == 0 else max(0, i - 2)
        blocks = range(first, i + 1)
        mine = (lane < 64) if hd == 0 else (lane >= 64)
        qi = qkv_ref[i * QB:(i + 1) * QB, 0:L] * BF(0.125)
        doi = dog_ref[j, 2 * i:2 * i + 2].reshape(QB, L)
        qm = jnp.where(mine, qi, BF(0))
        dom = jnp.where(mine, doi, BF(0))
        k_at = lambda kb: qkv_ref[kb * QB:(kb + 1) * QB, L:2 * L]
        v_at = lambda kb: qkv_ref[kb * QB:(kb + 1) * QB, 2 * L:3 * L]
        at = lambda kb: slice((kb - first) * QB, (kb - first + 1) * QB)
        mx = None
        for kb in blocks:
            s = dot_nt(qm, k_at(kb))
            if kb == i:
                s = jnp.where(col_i <= row_i, s, NEG_BIG)
            if hd == 1 and kb == i - 2:
                s = jnp.where(col_i > row_i, s, NEG_BIG)
            s_ref[:, at(kb)] = s
            cur = jnp.maximum(s[:, :L], s[:, L:])
            mx = cur if mx is None else jnp.maximum(mx, cur)
        m = jnp.max(mx, axis=1, keepdims=True)
        ls = None
        for kb in blocks:
            e = jnp.exp(s_ref[:, at(kb)] - m)
            s_ref[:, at(kb)] = e
            cur = e[:, :L] + e[:, L:]
            ls = cur if ls is None else ls + cur
        rl = 1.0 / jnp.sum(ls, axis=1, keepdims=True)
        acc = None
        for kb in blocks:
            p_ = s_ref[:, at(kb)] * rl
            s_ref[:, at(kb)] = p_
            pb = p_.astype(BF)
            p_ref[:, at(kb)] = pb
            cur = dot_nn(pb, v_at(kb))
            acc = cur if acc is None else acc + cur
        dsum = jnp.sum(dom.astype(F32) * acc, axis=1, keepdims=True)
        dq = None
        for kb in blocks:
            dp = dot_nt(dom, v_at(kb)).astype(BF).astype(F32)
            ds = (s_ref[:, at(kb)] * (dp - dsum)).astype(BF)
            ds_ref[:, at(kb)] = ds
            cur = dot_nn(ds, k_at(kb))
            dq = cur if dq is None else dq + cur
        hr = slice(hd * 64, hd * 64 + 64)
        n = len(blocks) * QB
        keys = slice(first * QB, first * QB + n)
        dvt_ref[hr, keys] += dot_nn(dot_ref[hr, i * QB:(i + 1) * QB], p_ref[:, :n])
        dkt_ref[hr, keys] += dot_nn(qt_ref[hr, i * QB:(i + 1) * QB], ds_ref[:, :n])
        return acc, dq * 0.125

    def batch_step(j, carry):
        last = h_tree(j)
        for e in last.hops(2):
            last.arrive(e)
        do_swap(j).wait()

        @pl.when(j == 1)
        def _():
            o_swap(0).start()
            d_swap(0).start()

        def qkv_step(r, c):
            rows = hg_ref[pl.ds(2 * r, 2), j].reshape(T, D)
            out = dot_nn(rows, w_ref[...]) + bias_ref[0:1, :]
            qkv_ref[pl.ds(pl.multiple_of(r * T, T), T), :] = out.astype(BF)
            return c

        lax.fori_loop(0, 4, qkv_step, 0)

        for i in R8:
            qs = qkv_ref[i * QB:(i + 1) * QB, 0:L] * BF(0.125)
            qt_ref[:, i * QB:(i + 1) * QB] = qs.T
            dot_ref[:, i * QB:(i + 1) * QB] = dog_ref[j, 2 * i:2 * i + 2].reshape(QB, L).T
        dkt_ref[...] = jnp.zeros_like(dkt_ref)
        dvt_ref[...] = jnp.zeros_like(dvt_ref)
        for i in R8:
            of, dqf = head_block(j, i, 0)
            og, dqg = head_block(j, i, 1)
            o = jnp.where(lane < 64, of, og).astype(BF)
            dq = jnp.where(lane < 64, dqf, dqg).astype(BF)
            for u in range(2):
                so_ref[j, 2 * i + u] = o[u * L:(u + 1) * L]
                sd_ref[j, 2 * i + u, 0] = dq[u * L:(u + 1) * L]
            dqkv_ref[i * QB:(i + 1) * QB, 0:L] = dq
            if i == 3:
                @pl.when(j == 0)
                def _():
                    for e in trees[1].hops(0):
                        trees[1].arrive(e)
                    do_swap(1).start()

        for t, src in ((1, dkt_ref), (2, dvt_ref)):
            for n in range(N):
                d = src[:, n * L:(n + 1) * L].T.astype(BF)
                sd_ref[j, n, t] = d
                dqkv_ref[n * L:(n + 1) * L, t * L:(t + 1) * L] = d
        ro_ref[j, pc.me] = so_ref[j, pc.me]
        rd_ref[j, pc.me] = sd_ref[j, pc.me]

        @pl.when(j == 0)
        def _():
            for e in trees[1].hops(1):
                trees[1].arrive(e)

        @pl.when(j == 1)
        def _():
            o_swap(1).start()

        def dw_step(r, c):
            cols = pl.ds(pl.multiple_of(r * QB, QB), QB)
            dwp_ref[cols, :] += dot_tn(hg_ref[:, j, :, cols].reshape(S, QB), dqkv_ref[...])
            return c

        lax.fori_loop(0, 4, dw_step, 0)
        dwp_ref[D:D + 1, :] += jnp.sum(dqkv_ref[...].astype(F32), axis=0, keepdims=True)
        return carry

    lax.fori_loop(0, 2, batch_step, 0)

    def half_of(core):
        return dwp_ref.at[pl.ds(pl.multiple_of(core * HR, 8), HR)]

    def to_sib(n, src, dst, send, recv):
        cp = rcopy(src, dst, send.at[n], recv.at[n], pc.sib)
        cp.start()
        return cp

    half = to_sib(2, half_of(1 - pc.core), dws_ref, sib_send, sib_recv)
    for j in range(2):
        trees[j].finish()
        do_swap(j).finish()
    w_flat = hg_ref.reshape(2 * S, D)
    w_loads = [pltpu.make_async_copy(wqkv_hbm.at[:, t * D:(t + 1) * D], w_flat.at[t * D:(t + 1) * D], loc.at[3 + t]) for t in R3]
    for cp in w_loads:
        cp.start()
    half.wait_recv()
    dws_ref[...] += half_of(pc.core)[...]

    def w_slot(c, p, core=pc.core):
        return dwg_ref.at[c, core, w_rows(p)]

    def g_slot(c, p, core=pc.core):
        return dwo_ref.at[core, c, o_rows(p)]

    wtree = Tree(pc, lambda p: dws_ref.at[w_rows(p)], w_slot, dwg_ref.at[0:7, pc.core], w_send.at[0], w_recv)
    wtree.start_own((0,))
    keep_w = pltpu.make_async_copy(dws_ref, dwg_ref.at[pc.chip, pc.core], loc.at[0])
    keep_w.start()
    for p in R3:
        to_sib(0, dws_ref.at[w_rows(p)], w_slot(pc.chip, p), ws_send, ws_recv)

    for j in range(2):
        o_swap(j).wait()
    for b in R4:
        for m in R8:
            o_nat[b * L:(b + 1) * L, m * L:(m + 1) * L] = gather_heads(lambda j, q: ro_ref[j, q], pos, b, m)

    def wout_part(core, c):
        cols = pl.ds(pl.multiple_of(core * T + c * QB, QB), QB)
        return dot_tn(o_nat[:, cols], dy_all)

    for c in range(2):
        part_ref[c * QB:(c + 1) * QB] = wout_part(1 - pc.core, c)
    xp = to_sib(3, part_ref, px_ref, sib_send, sib_recv)
    for c in range(2):
        acc_ref[4 * c:4 * c + 4] = wout_part(pc.core, c).reshape(4, 64, D)
    xp.wait_recv()
    acc_ref[...] += px_ref[...].reshape(8, 64, D)

    bufs = (rs0_ref, rs1_ref, rs2_ref)

    def reduce_step(s, wait):
        for p in R3:
            order = [(p + j) % 3 for j in R3]
            if wait:
                at = bufs[s].at[:, o_rows(p)]
                rcopy(at, at, r_send.at[0], r_recv.at[s * 3 + p], pc.sib).wait_recv()
            for i, sub in enumerate(subsets(order[s + 1:])):
                if wait:
                    acc_ref[pc.chip_at(sub), o_rows(p)] += bufs[s][i, o_rows(p)]
                else:
                    rcopy(acc_ref.at[pc.chip_at((order[s],) + sub), o_rows(p)], bufs[s].at[i, o_rows(p)],
                          r_send.at[0], r_recv.at[s * 3 + p], pc.next_dev(order[s])).start()

    reduce_step(0, False)
    wtree.start_own((1, 2))
    def pass_on(tree, slot, n, send, recv):
        for e in tree.hops(n):
            c, p = tree.arrive(e)
            to_sib(0, slot(c, p), slot(c, p), send, recv)

    dbo = jnp.zeros((1, D), F32)
    for b in R4:
        rows = slice(b * L, (b + 1) * L)
        y_ref[b] = (x_ref[b].astype(F32) + dot_nn(o_nat[rows], wout_ref.reshape(D, D)[...]) + bout).astype(BF)
        dbo += jnp.sum(dy_ref[b].astype(F32), axis=0, keepdims=True)
    reduce_step(0, True)
    reduce_step(1, False)
    d_swap(1).start(1, 9)
    reduce_step(1, True)
    reduce_step(2, False)
    d_swap(1).start(9)
    reduce_step(2, True)
    gtree = Tree(pc, lambda p: acc_ref.at[pc.chip, o_rows(p)], g_slot, dwo_ref.at[pc.core, 0:7], g_send.at[0], g_recv)
    gtree.start_own()
    keep_g = pltpu.make_async_copy(acc_ref.at[pc.chip], dwo_ref.at[pc.core, pc.chip], loc.at[1])
    keep_g.start()
    for p in R3:
        to_sib(0, acc_ref.at[pc.chip, o_rows(p)], g_slot(pc.chip, p), gs_send, gs_recv)

    pass_on(wtree, w_slot, 0, ws_send, ws_recv)
    for j in range(2):
        d_swap(j).wait()

    def spread(b, c):
        rows = pl.ds(pl.multiple_of(b * L, L), L)
        for m in R8:
            for t in R3:
                dqkv_nat[rows, t * D + m * L:t * D + (m + 1) * L] = gather_heads(lambda j, q: rd_ref[j, q, t], pos, b, m)
        return c

    def back(b, c):
        dg, db = c
        rows = pl.ds(pl.multiple_of(b * L, L), L)
        _, xhat, rstd = centre(x_ref[b])
        dh = None
        for t in R3:
            cur = dot_nt(dqkv_nat[rows, t * D:(t + 1) * D], w_flat[t * D:(t + 1) * D])
            dh = cur if dh is None else dh + cur
        dh = dh.astype(BF).astype(F32)
        dxh = dh * gamma
        m1 = jnp.mean(dxh, axis=-1, keepdims=True)
        m2 = jnp.mean(dxh * xhat, axis=-1, keepdims=True)
        dx_ref[b] = (dy_ref[b].astype(F32) + rstd * (dxh - m1 - xhat * m2)).astype(BF)
        return dg + jnp.sum(dh * xhat, axis=0, keepdims=True), db + jnp.sum(dh, axis=0, keepdims=True)

    lax.fori_loop(0, 4, spread, 0)
    for cp in w_loads:
        cp.wait()
    dgb = lax.fori_loop(0, 2, back, (jnp.zeros((1, D), F32), jnp.zeros((1, D), F32)))
    pass_on(gtree, g_slot, 0, gs_send, gs_recv)
    dg, db = lax.fori_loop(2, 4, back, dgb)
    row = lax.broadcasted_iota(jnp.int32, (4, D), 0)
    sm_out[...] = jnp.where(row == 0, dg, jnp.where(row == 1, db, jnp.where(row == 2, dbo, 0.0)))
    sm_ref[pc.me] = sm_out[...]
    s_swap = Exchange(pc, lambda t: sm_out, lambda t: sm_ref.at[t], sm_ref.at[0:N - 1], s_send.at[0], s_recv.at[0])
    s_swap.start()
    pass_on(wtree, w_slot, 1, ws_send, ws_recv)
    pass_on(gtree, g_slot, 1, gs_send, gs_recv)
    s_swap.wait()
    tot = sm_ref[0]
    for n in range(1, N):
        tot = tot + sm_ref[n]
    small_ref[...] = tot
    pass_on(gtree, g_slot, 2, gs_send, gs_recv)
    pass_on(wtree, w_slot, 2, ws_send, ws_recv)
    for tree, at, got, send, recv in (
            (wtree, dwg_ref.at[:, pc.core], dwg_ref.at[:, 1 - pc.core], ws_send, ws_recv),
            (gtree, dwo_ref.at[pc.core], dwo_ref.at[1 - pc.core], gs_send, gs_recv)):
        rcopy(got, got, send.at[0], recv.at[0], pc.sib).wait_recv()
        rcopy(at, at, send.at[0], recv.at[0], pc.sib).wait_send()
        tree.finish()
    for j in range(2):
        sib_copy(j).wait_send()
        o_swap(j).finish()
        d_swap(j).finish()
    s_swap.finish()
    half.wait_send()
    xp.wait_send()
    rcopy(acc_ref.at[0:7], acc_ref.at[0:7], r_send.at[0], r_recv.at[0], pc.sib).wait_send()
    keep_w.wait()
    keep_g.wait()


def layer_call(kind, x, dy, gamma, beta, bout, bqkv, wqkv, wout):
    vm, sm, hb = (pl.BlockSpec(memory_space=m) for m in (pltpu.VMEM, pltpu.SMEM, pl.ANY))
    sem = pltpu.SemaphoreType.DMA
    tok = jax.ShapeDtypeStruct((4, L, D), BF)

    def pair(*n):
        return [sem(n), sem(n)]

    def bf(*n):
        return pltpu.VMEM(n, BF)

    def ff(*n):
        return pltpu.VMEM(n, F32)

    band = 3 * QB
    return pl.pallas_call(
        layer_kernel,
        out_shape=(tok, tok, jax.ShapeDtypeStruct((4, D), F32), jax.ShapeDtypeStruct((8, 2, HR, W3), F32),
                   jax.ShapeDtypeStruct((2, 8, 64, D), F32)),
        in_specs=[sm] + [vm] * 6 + [hb, hb],
        out_specs=(vm, vm, vm, hb, hb),
        scratch_shapes=[
            bf(8, 2, QB, D), bf(2, L, D), bf(N, 64, D), bf(QB, D), bf(8, 4, L, L), bf(2, N, L, L), bf(D, W3), ff(8, W3),
            bf(S, W3), bf(S, W3), bf(L, S), bf(L, S), ff(L, S), ff(L, S),
            ff(QB, S), bf(QB, S), bf(QB, S), ff(QB, band), bf(QB, band), bf(QB, band),
            bf(2, N, L, L), bf(2, N, 3, L, L), bf(2, N, L, L), bf(2, N, 3, L, L), bf(T, D), bf(T, D3),
            ff(DR, W3), ff(HR, W3), ff(T, D), ff(T, D), ff(8, 64, D),
            ff(4, 64, D), ff(2, 64, D), ff(1, 64, D), ff(N, 4, D), ff(4, D), sem((6,))]
        + pair(4) + [sem((2,)), sem((2, 21))] + pair(2) + pair(2) + pair(2) + pair(1)
        + [sem((1,)), sem((21,))] + [sem((1,)), sem((21,))] + pair(1) + pair(1) + [sem((1,)), sem((9,))],
        compiler_params=pltpu.CompilerParams(vmem_limit_bytes=VMEM_CAP, collective_id=0, has_side_effects=True),
        name="layer",
    )(kind, x, dy, gamma, beta, bout, bqkv, wqkv, wout)


def unpack_kernel(kind_ref, dw_hbm, dwo_hbm, y_in, dx_in, small_ref,
                  out_hbm, wo_hbm, y_out, dx_out, bias_ref, dg_ref, db_ref, dbo_ref,
                  in_ref, ob_ref, bias_in, wo_ref, y_ref, dx_ref, in_sem, out_sem, pass_in, pass_out):
    pos = head_places(kind_ref)

    def rows(r):
        return pl.ds(pl.multiple_of(r * 64, 64), 64)

    def load(r):
        return pltpu.make_async_copy(dw_hbm.at[:, rows(r)], in_ref.at[r], in_sem.at[r])

    def store(r):
        return pltpu.make_async_copy(ob_ref.at[r], out_hbm.at[rows(r)], out_sem.at[r])

    chain = ((dwo_hbm, wo_ref, wo_hbm), (y_in, y_ref, y_out), (dx_in, dx_ref, dx_out))

    def get(i):
        return pltpu.make_async_copy(chain[i][0], chain[i][1], pass_in.at[i])

    def put(i):
        return pltpu.make_async_copy(chain[i][1], chain[i][2], pass_out.at[i])

    bias_load = pltpu.make_async_copy(dw_hbm.at[:, D:D + 8], bias_in, pass_in.at[3])
    for r in R8:
        load(r).start()
    bias_load.start()

    def pick(read, t, m):
        pa, pb = pos[2 * m], pos[2 * m + 1]
        cols = slice(t * L, (t + 1) * L)
        a, b = read(pa % 8, cols), read(pb % 8, cols)
        lane = lax.broadcasted_iota(jnp.int32, a.shape, 1)
        a = jnp.where(pa // 8 == 1, pltpu.roll(a, 64, 1), a)
        b = jnp.where(pb // 8 == 0, pltpu.roll(b, 64, 1), b)
        return jnp.where(lane < 64, a, b)

    def step(r, c):
        load(r).wait()

        @pl.when(r < 8)
        def _():
            load(r + 8).start()

        @pl.when(r == 2)
        def _():
            for i in R3:
                get(i).start()

        @pl.when(r == 8)
        def _():
            for i in R3:
                get(i).wait()
                put(i).start()

        for t in R3:
            for m in R8:
                ob_ref[r, :, t * D + m * L:t * D + (m + 1) * L] = pick(lambda q, cols: in_ref[r, q, :, cols], t, m)
        store(r).start()
        return c

    lax.fori_loop(0, N, step, 0)
    bias_load.wait()
    for t in R3:
        for m in R8:
            bias_ref[t * D + m * L:t * D + (m + 1) * L] = pick(lambda q, cols: bias_in[q, :, cols], t, m)[0]
    for i, ref in enumerate((dg_ref, db_ref, dbo_ref)):
        ref[...] = small_ref[i]
    for r in range(N):
        store(r).wait()
    for i in R3:
        put(i).wait()


def unpack_call(kind, dwg, dwo, small, y, dx):
    vm, sm, hb = (pl.BlockSpec(memory_space=m) for m in (pltpu.VMEM, pltpu.SMEM, pl.ANY))
    sem = pltpu.SemaphoreType.DMA
    vec = jax.ShapeDtypeStruct((D,), F32)
    tok = jax.ShapeDtypeStruct((4, L, D), BF)
    return pl.pallas_call(
        unpack_kernel,
        in_specs=[sm, hb, hb, hb, hb, vm],
        out_specs=[hb, hb, hb, hb, vm, vm, vm, vm],
        out_shape=[jax.ShapeDtypeStruct((D, D3), F32), jax.ShapeDtypeStruct((D, D), F32), tok, tok,
                   jax.ShapeDtypeStruct((D3,), F32), vec, vec, vec],
        scratch_shapes=[
            pltpu.VMEM((N, 8, 64, W3), F32), pltpu.VMEM((N, 64, D3), F32), pltpu.VMEM((8, 8, W3), F32),
            pltpu.VMEM((D, D), F32), pltpu.VMEM((4, L, D), BF), pltpu.VMEM((4, L, D), BF),
            sem((N,)), sem((N,)), sem((4,)), sem((3,))],
        compiler_params=pltpu.CompilerParams(vmem_limit_bytes=VMEM_CAP),
        name="unpack",
    )(kind, dwg, dwo, y, dx, small)


def solution(mesh):
    tok_spec = P(None, "sp", None)

    def local_block(x, d_y, ln_gamma, ln_beta, w_qkv, b_qkv, w_out, b_out, head_kind):
        y, dx, small, dwg, dwo = layer_call(head_kind, x, d_y, ln_gamma, ln_beta, b_out, b_qkv, w_qkv, w_out.reshape(N, 64, D))
        dw, dwout, y, dx, dbias, dg, db, dbo = unpack_call(
            head_kind, dwg.reshape(8, DR, W3), dwo.reshape(D, D), small, y, dx)
        return y, dx, dg, db, dw, dbias, dwout, dbo

    return jax.shard_map(
        local_block, mesh=mesh,
        in_specs=(tok_spec, tok_spec, P(), P(), P(), P(), P(), P(), P()),
        out_specs=(tok_spec, tok_spec, P(), P(), P(), P(), P(), P()), check_vma=False)
```

```python
import functools
import math

import jax
import jax.numpy as jnp
from jax import lax
from jax.experimental import pallas as pl
from jax.experimental.pallas import tpu as pltpu
from jax.sharding import PartitionSpec as P

LN_EPS = 1e-5
NEG_BIG = -1e30
BF = jnp.bfloat16
F32 = jnp.float32
QB = 256
L = 128
W3 = 384
T = 512
D = 1024
DR = 1040
HR = 520
N = 16
R2, R3, R4, R8 = range(2), range(3), range(4), range(8)
MESH = pl.DeviceIdType.MESH
H_ROWS = (0, 96, 176, 256)
W_ROWS = (0, 176, 352, 520)
O_ROWS = (0, 24, 48, 64)
S = 2048
D3 = 3072
VMEM_CAP = 63 * D * D


def dot_nn(a, b):
    return lax.dot_general(a, b, (((1,), (0,)), ((), ())), preferred_element_type=F32)


def dot_nt(a, b):
    return lax.dot_general(a, b, (((1,), (1,)), ((), ())), preferred_element_type=F32)


def dot_tn(a, b):
    return lax.dot_general(a, b, (((0,), (0,)), ((), ())), preferred_element_type=F32)


def swap_halves(a):
    return jnp.concatenate([a[:, 64:], a[:, :64]], axis=1)


def pair_halves(a, a_half, b, b_half):
    lane = lax.broadcasted_iota(jnp.int32, a.shape, 1)
    a = jnp.where(a_half == 1, swap_halves(a), a)
    b = jnp.where(b_half == 0, swap_halves(b), b)
    return jnp.where(lane < 64, a, b)


class Place:
    def __init__(self):
        self.me = lax.axis_index("sp")
        self.core, self.chip = self.me % 2, self.me // 2
        self.sib = self.me + 1 - 2 * self.core
        bits = (self.chip % 2, self.chip // 2 % 2, self.chip // 4)
        self.step = [(1 - 2 * v) * w for v, w in zip(bits, (1, 2, 4))]

    def chip_at(self, axes):
        out = self.chip
        for a in axes:
            out = out + self.step[a]
        return out

    def next_dev(self, axis):
        return self.me + 2 * self.step[axis]


def rcopy(src, dst, send, recv, dev):
    return pltpu.make_async_remote_copy(
        src_ref=src, dst_ref=dst, send_sem=send, recv_sem=recv, device_id=(dev,), device_id_type=MESH)


def subsets(axes):
    out = [()]
    for a in axes:
        out += [v + (a,) for v in out]
    return out


class Tree:
    def __init__(self, place, own, slot, seven, send, recv):
        self.place, self.own, self.slot, self.seven, self.send, self.recv = place, own, slot, seven, send, recv
        self.entries = []
        for s in R3:
            for p in R3:
                order = [(p + j) % 3 for j in R3]
                for sub in subsets(order[:s]):
                    self.entries.append((p, order[s], sub))

    def copy(self, e):
        p, axis, sub = e
        i = self.entries.index(e)
        at = self.slot(self.place.chip_at(sub), p)
        return rcopy(at if sub else self.own(p), at, self.send, self.recv.at[i], self.place.next_dev(axis))

    def start_own(self, levels=R3):
        for e in self.hops(0):
            if (e[1] - e[0]) % 3 in levels:
                self.copy(e).start()

    def arrive(self, e):
        p, axis, sub = e
        got = sub + (axis,)
        chip = self.place.chip_at(got)
        at = self.slot(chip, p)
        i = self.entries.index(e)
        rcopy(at, at, self.send, self.recv.at[i], self.place.next_dev(axis)).wait_recv()
        for n in self.entries:
            if n[0] == p and n[2] == got:
                self.copy(n).start()
        return chip, p

    def hops(self, n):
        return [e for e in self.entries if len(e[2]) == n]

    def finish(self):
        rcopy(self.seven, self.seven, self.send, self.recv.at[0], self.place.me).wait_send()


def barrier_signal(place):
    sem = pltpu.get_barrier_semaphore()
    for r in range(1, N):
        pl.semaphore_signal(sem, inc=1, device_id=((place.me + r) % N,), device_id_type=MESH)


def barrier_wait():
    pl.semaphore_wait(pltpu.get_barrier_semaphore(), N - 1)


def head_places(kind_ref):
    pos, zeros, ones = [], 0, 8
    for n in range(N):
        k = kind_ref[n]
        pos.append(jnp.where(k == 0, zeros, ones))
        zeros, ones = zeros + 1 - k, ones + k
    return pos


class Exchange:
    def __init__(self, place, src, dst, rest, send, recv):
        self.place, self.src, self.dst, self.send, self.recv = place, src, dst, send, recv
        self.rest = rest

    def start(self, first=1, end=N):
        me = self.place.me
        for r in range(first, end):
            to = (me + r) % N
            rcopy(self.src(to), self.dst(me), self.send, self.recv, to).start()

    def start_half(self, upper):
        me = self.place.me
        for r in range(1, N):
            to = (me + r) % N

            @pl.when(to // 8 == upper)
            def _():
                rcopy(self.src(to), self.dst(me), self.send, self.recv, to).start()

    def wait(self):
        rcopy(self.rest, self.rest, self.send, self.recv, self.place.me).wait_recv()

    def finish(self):
        rcopy(self.rest, self.rest, self.send, self.recv, self.place.me).wait_send()


def gather_heads(recv_at, pos, b, m):
    pa, pb = pos[2 * m], pos[2 * m + 1]
    k, j = b // 2, b % 2
    a = recv_at(j, 2 * (pa % 8) + k)
    c = recv_at(j, 2 * (pb % 8) + k)
    return pair_halves(a, pa // 8, c, pb // 8)


def span(tab):
    return lambda p: pl.ds(tab[p], tab[p + 1] - tab[p])


def centre(xb):
    xf = xb.astype(F32)
    cen = xf - jnp.mean(xf, axis=-1, keepdims=True)
    rstd = lax.rsqrt(jnp.mean(cen * cen, axis=-1, keepdims=True) + LN_EPS)
    return xf, cen * rstd, rstd


def layer_kernel(kind_ref, x_hbm, dy_hbm, gamma_ref, beta_ref, bout_ref, bqkv_ref, wqkv_hbm, wout_hbm,
                 y_hbm, dx_hbm, small_ref, dwg_ref, dwo_ref, x_ref, dy_ref, y_ref, dx_ref,
                 hg_ref, out_ref, wout_ref, wp_ref, do_ref, dog_ref, w_ref, bias_ref, qkv_ref, dqkv_ref, qt_ref, dot_ref,
                 dkt_ref, dvt_ref, s_f, p_f, ds_f, s_g, p_g, ds_g, so_ref, sd_ref, ro_ref, rd_ref, o_nat, dqkv_nat,
                 dwp_ref, dws_ref, part_ref, px_ref, acc_ref, rs0_ref, rs1_ref, rs2_ref, sm_ref, sm_out,
                 loc, sib_send, sib_recv, h_send, h_recv, do_send, do_recv, o_send, o_recv, d_send, d_recv,
                 s_send, s_recv, w_send, w_recv, g_send, g_recv, ws_send, ws_recv, gs_send, gs_recv, r_send, r_recv, io_sem):
    pc = Place()
    barrier_signal(pc)

    def w_load(r):
        return pltpu.make_async_copy(wqkv_hbm.at[r * T:(r + 1) * T], dqkv_nat, loc.at[r])

    wo_load = pltpu.make_async_copy(wout_hbm, wout_ref, loc.at[2])
    x_load, dy_load, y_put, dx_put = [
        pltpu.make_async_copy(a, b, io_sem.at[i]) for i, (a, b) in enumerate(
            ((x_hbm, x_ref), (dy_hbm, dy_ref), (y_ref, y_hbm), (dx_ref, dx_hbm)))]
    x_load.start()
    dy_load.start()
    w_load(0).start()
    wo_load.start()
    gamma = gamma_ref[...].reshape(1, D).astype(F32)
    beta = beta_ref[...].reshape(1, D).astype(F32)
    bout = bout_ref[...].reshape(1, D).astype(F32)
    bqkv = bqkv_ref[...].reshape(1, D3).astype(F32)

    def rows_of(core):
        return pl.ds(pl.multiple_of(core * L, L), L)

    def norm(xb):
        return (centre(xb)[1] * gamma + beta).astype(BF)

    def sib_copy(j):
        return rcopy(out_ref.at[j], hg_ref.at[pc.chip, j, rows_of(pc.core)], sib_send.at[j], sib_recv.at[j], pc.sib)

    x_load.wait()
    for j in R2:
        out_ref[j] = norm(x_ref[2 * (1 - pc.core) + j])
    for j in R2:
        hg_ref[pc.chip, j, rows_of(pc.core)] = norm(x_ref[2 * pc.core + j])
    barrier_wait()
    for j in R2:
        sib_copy(j).start()

    h_rows, w_rows, o_rows = span(H_ROWS), span(W_ROWS), span(O_ROWS)

    def h_tree(j):
        slot = lambda c, p: hg_ref.at[c, j, h_rows(p)]
        return Tree(pc, lambda p: slot(pc.chip, p), slot, hg_ref.at[0:7, j], h_send.at[j], h_recv.at[j])

    def sib_arrive(j):
        at = hg_ref.at[pc.chip, j, rows_of(1 - pc.core)]
        rcopy(at, at, sib_send.at[j], sib_recv.at[j], pc.sib).wait_recv()

    do_out = do_ref.reshape(N, 2, L, L)

    def swap(src, dst, send, recv, j):
        return Exchange(pc, lambda t: src(t, j), lambda t: dst.at[j, t], dst.at[j, 0:N - 1], send.at[j], recv.at[j])

    def do_swap(j):
        return swap(lambda t, j: do_out.at[t, j], dog_ref, do_send, do_recv, j)

    def o_swap(j):
        return swap(lambda t, j: so_ref.at[j, t], ro_ref, o_send, o_recv, j)

    def d_swap(j):
        return swap(lambda t, j: sd_ref.at[j, t], rd_ref, d_send, d_recv, j)

    trees = [h_tree(0), h_tree(1)]
    sib_arrive(0)
    trees[0].start_own()
    pos = head_places(kind_ref)
    perm = []
    for j in range(N):
        v = 0
        for n in range(1, N):
            v = v + jnp.where(pos[n] == j, n, 0)
        perm.append(v)
    f = g = 0
    for c in R8:
        f = f + jnp.where(pc.chip == c, perm[c], 0)
        g = g + jnp.where(pc.chip == c, perm[8 + c], 0)
    wo_load.wait()
    dy_load.wait()
    dy_all = dy_ref[...].reshape(T, D)
    for c in R4:
        for u in R2:
            wp_ref[u * L:u * L + 64] = wout_ref[perm[2 * c + u]]
            wp_ref[u * L + 64:u * L + L] = wout_ref[perm[8 + 2 * c + u]]
        d = dot_nt(dy_all, wp_ref[...]).astype(BF)
        for u in R2:
            do_ref[2 * c + u] = d[:, u * L:(u + 1) * L].reshape(4, L, L)
    for e in trees[0].hops(0):
        trees[0].arrive(e)
    do_swap(0).start()
    for j in R2:
        dog_ref[j, pc.me] = do_out[pc.me, j]

    def w_cols(t, k, head):
        out = None
        for m in R8:
            cur = dqkv_nat[k * L:(k + 1) * L, t * D + m * L:t * D + (m + 1) * L]
            out = cur if out is None else jnp.where(head // 2 == m, cur, out)
        return out

    for r in R2:
        w_load(r).wait()
        for t in R3:
            for k in R4:
                w_ref[r * T + k * L:r * T + (k + 1) * L, t * L:(t + 1) * L] = pair_halves(
                    w_cols(t, k, f), f % 2, w_cols(t, k, g), g % 2)
        if r == 0:
            w_load(1).start()
    for t in R3:
        halves = []
        for head in (f, g):
            out = None
            for m in R8:
                cur = bqkv[:, t * D + m * L:t * D + (m + 1) * L]
                out = cur if out is None else jnp.where(head // 2 == m, cur, out)
            halves += [out, head % 2]
        bias_ref[:, t * L:(t + 1) * L] = jnp.broadcast_to(pair_halves(*halves), (8, L))
    dwp_ref[...] = jnp.zeros_like(dwp_ref)
    for e in trees[0].hops(1):
        trees[0].arrive(e)
    sib_arrive(1)
    trees[1].start_own()

    lane = lax.broadcasted_iota(jnp.int32, (QB, L), 1)
    row_i = lax.broadcasted_iota(jnp.int32, (QB, QB), 0)
    col_i = lax.broadcasted_iota(jnp.int32, (QB, QB), 1)

    def head_block(j, i, hd):
        s_ref, p_ref, ds_ref = ((s_f, p_f, ds_f), (s_g, p_g, ds_g))[hd]
        first = 0 if hd == 0 else max(0, i - 2)
        blocks = range(first, i + 1)
        mine = (lane < 64) if hd == 0 else (lane >= 64)
        qi = qkv_ref[i * QB:(i + 1) * QB, 0:L] * BF(0.125)
        doi = dog_ref[j, 2 * i:2 * i + 2].reshape(QB, L)
        qm = jnp.where(mine, qi, BF(0))
        dom = jnp.where(mine, doi, BF(0))
        k_at = lambda kb: qkv_ref[kb * QB:(kb + 1) * QB, L:2 * L]
        v_at = lambda kb: qkv_ref[kb * QB:(kb + 1) * QB, 2 * L:3 * L]
        at = lambda kb: slice((kb - first) * QB, (kb - first + 1) * QB)
        mx = None
        for kb in blocks:
            s = dot_nt(qm, k_at(kb))
            if kb == i:
                s = jnp.where(col_i <= row_i, s, NEG_BIG)
            if hd == 1 and kb == i - 2:
                s = jnp.where(col_i > row_i, s, NEG_BIG)
            s_ref[:, at(kb)] = s
            cur = jnp.maximum(s[:, :L], s[:, L:])
            mx = cur if mx is None else jnp.maximum(mx, cur)
        m = jnp.max(mx, axis=1, keepdims=True)
        ls = None
        for kb in blocks:
            e = jnp.exp(s_ref[:, at(kb)] - m)
            s_ref[:, at(kb)] = e
            cur = e[:, :L] + e[:, L:]
            ls = cur if ls is None else ls + cur
        rl = 1.0 / jnp.sum(ls, axis=1, keepdims=True)
        acc = None
        for kb in blocks:
            p_ = s_ref[:, at(kb)] * rl
            s_ref[:, at(kb)] = p_
            pb = p_.astype(BF)
            p_ref[:, at(kb)] = pb
            cur = dot_nn(pb, v_at(kb))
            acc = cur if acc is None else acc + cur
        dsum = jnp.sum(dom.astype(F32) * acc, axis=1, keepdims=True)
        dq = None
        for kb in blocks:
            dp = dot_nt(dom, v_at(kb)).astype(BF).astype(F32)
            ds = (s_ref[:, at(kb)] * (dp - dsum)).astype(BF)
            ds_ref[:, at(kb)] = ds
            cur = dot_nn(ds, k_at(kb))
            dq = cur if dq is None else dq + cur
        hr = slice(hd * 64, hd * 64 + 64)
        n = len(blocks) * QB
        keys = slice(first * QB, first * QB + n)
        dvt_ref[hr, keys] += dot_nn(dot_ref[hr, i * QB:(i + 1) * QB], p_ref[:, :n])
        dkt_ref[hr, keys] += dot_nn(qt_ref[hr, i * QB:(i + 1) * QB], ds_ref[:, :n])
        return acc, dq * 0.125

    def batch_step(j, carry):
        last = h_tree(j)
        for e in last.hops(2):
            last.arrive(e)
        do_swap(j).wait()

        @pl.when(j == 1)
        def _():
            o_swap(0).start()
            d_swap(0).start()

        def qkv_step(r, c):
            rows = hg_ref[pl.ds(2 * r, 2), j].reshape(T, D)
            out = dot_nn(rows, w_ref[...]) + bias_ref[0:1, :]
            qkv_ref[pl.ds(pl.multiple_of(r * T, T), T), :] = out.astype(BF)
            return c

        lax.fori_loop(0, 4, qkv_step, 0)

        for i in R8:
            qs = qkv_ref[i * QB:(i + 1) * QB, 0:L] * BF(0.125)
            qt_ref[:, i * QB:(i + 1) * QB] = qs.T
            dot_ref[:, i * QB:(i + 1) * QB] = dog_ref[j, 2 * i:2 * i + 2].reshape(QB, L).T
        dkt_ref[...] = jnp.zeros_like(dkt_ref)
        dvt_ref[...] = jnp.zeros_like(dvt_ref)
        for i in R8:
            of, dqf = head_block(j, i, 0)
            og, dqg = head_block(j, i, 1)
            o = jnp.where(lane < 64, of, og).astype(BF)
            dq = jnp.where(lane < 64, dqf, dqg).astype(BF)
            for u in R2:
                so_ref[j, 2 * i + u] = o[u * L:(u + 1) * L]
                sd_ref[j, 2 * i + u, 0] = dq[u * L:(u + 1) * L]
            dqkv_ref[i * QB:(i + 1) * QB, 0:L] = dq
            if i == 3:
                @pl.when(j == 0)
                def _():
                    for e in trees[1].hops(0):
                        trees[1].arrive(e)
                    do_swap(1).start()

                @pl.when(j == 1)
                def _():
                    o_swap(1).start_half(0)

        for t, src in ((1, dkt_ref), (2, dvt_ref)):
            for n in range(N):
                d = src[:, n * L:(n + 1) * L].T.astype(BF)
                sd_ref[j, n, t] = d
                dqkv_ref[n * L:(n + 1) * L, t * L:(t + 1) * L] = d
        ro_ref[j, pc.me] = so_ref[j, pc.me]
        rd_ref[j, pc.me] = sd_ref[j, pc.me]

        @pl.when(j == 0)
        def _():
            for e in trees[1].hops(1):
                trees[1].arrive(e)

        @pl.when(j == 1)
        def _():
            o_swap(1).start_half(1)

        def dw_step(r, c):
            cols = pl.ds(pl.multiple_of(r * QB, QB), QB)
            dwp_ref[cols, :] += dot_tn(hg_ref[:, j, :, cols].reshape(S, QB), dqkv_ref[...])
            return c

        lax.fori_loop(0, 4, dw_step, 0)
        dwp_ref[D:D + 1, :] += jnp.sum(dqkv_ref[...].astype(F32), axis=0, keepdims=True)
        return carry

    lax.fori_loop(0, 2, batch_step, 0)

    def half_of(core):
        return dwp_ref.at[pl.ds(pl.multiple_of(core * HR, 8), HR)]

    def to_sib(n, src, dst, send, recv):
        cp = rcopy(src, dst, send.at[n], recv.at[n], pc.sib)
        cp.start()
        return cp

    half = to_sib(2, half_of(1 - pc.core), dws_ref, sib_send, sib_recv)
    for j in R2:
        trees[j].finish()
        do_swap(j).finish()
    w_flat = hg_ref.reshape(2 * S, D)
    w_loads = [pltpu.make_async_copy(wqkv_hbm.at[:, t * D:(t + 1) * D], w_flat.at[t * D:(t + 1) * D], loc.at[3 + t]) for t in R3]
    for cp in w_loads:
        cp.start()
    half.wait_recv()
    dws_ref[...] += half_of(pc.core)[...]

    def w_slot(c, p, core=pc.core):
        return dwg_ref.at[c, core, w_rows(p)]

    def g_slot(c, p, core=pc.core):
        return dwo_ref.at[core, c, o_rows(p)]

    wtree = Tree(pc, lambda p: dws_ref.at[w_rows(p)], w_slot, dwg_ref.at[0:7, pc.core], w_send.at[0], w_recv)
    wtree.start_own((0,))
    keep_w = pltpu.make_async_copy(dws_ref, dwg_ref.at[pc.chip, pc.core], loc.at[0])
    keep_w.start()
    for p in R3:
        to_sib(0, dws_ref.at[w_rows(p)], w_slot(pc.chip, p), ws_send, ws_recv)

    for j in R2:
        o_swap(j).wait()
    for b in R4:
        for m in R8:
            o_nat[b * L:(b + 1) * L, m * L:(m + 1) * L] = gather_heads(lambda j, q: ro_ref[j, q], pos, b, m)

    def wout_part(core, c):
        cols = pl.ds(pl.multiple_of(core * T + c * QB, QB), QB)
        return dot_tn(o_nat[:, cols], dy_all)

    for c in R2:
        part_ref[c * QB:(c + 1) * QB] = wout_part(1 - pc.core, c)
    xp = to_sib(3, part_ref, px_ref, sib_send, sib_recv)
    for c in R2:
        acc_ref[4 * c:4 * c + 4] = wout_part(pc.core, c).reshape(4, 64, D)
    xp.wait_recv()
    acc_ref[...] += px_ref[...].reshape(8, 64, D)

    bufs = (rs0_ref, rs1_ref, rs2_ref)

    def reduce_step(s, wait):
        for p in R3:
            order = [(p + j) % 3 for j in R3]
            if wait:
                at = bufs[s].at[:, o_rows(p)]
                rcopy(at, at, r_send.at[0], r_recv.at[s * 3 + p], pc.sib).wait_recv()
            for i, sub in enumerate(subsets(order[s + 1:])):
                if wait:
                    acc_ref[pc.chip_at(sub), o_rows(p)] += bufs[s][i, o_rows(p)]
                else:
                    rcopy(acc_ref.at[pc.chip_at((order[s],) + sub), o_rows(p)], bufs[s].at[i, o_rows(p)],
                          r_send.at[0], r_recv.at[s * 3 + p], pc.next_dev(order[s])).start()

    reduce_step(0, False)
    wtree.start_own((1, 2))
    def pass_on(tree, slot, n, send, recv):
        for e in tree.hops(n):
            c, p = tree.arrive(e)
            to_sib(0, slot(c, p), slot(c, p), send, recv)

    dbo = jnp.zeros((1, D), F32)
    for b in R4:
        rows = slice(b * L, (b + 1) * L)
        y_ref[b] = (x_ref[b].astype(F32) + dot_nn(o_nat[rows], wout_ref.reshape(D, D)[...]) + bout).astype(BF)
        dbo += jnp.sum(dy_ref[b].astype(F32), axis=0, keepdims=True)
    y_put.start()
    reduce_step(0, True)
    reduce_step(1, False)
    d_swap(1).start(1, 9)
    reduce_step(1, True)
    reduce_step(2, False)
    d_swap(1).start(9)
    reduce_step(2, True)
    gtree = Tree(pc, lambda p: acc_ref.at[pc.chip, o_rows(p)], g_slot, dwo_ref.at[pc.core, 0:7], g_send.at[0], g_recv)
    gtree.start_own()
    keep_g = pltpu.make_async_copy(acc_ref.at[pc.chip], dwo_ref.at[pc.core, pc.chip], loc.at[1])
    keep_g.start()
    for p in R3:
        to_sib(0, acc_ref.at[pc.chip, o_rows(p)], g_slot(pc.chip, p), gs_send, gs_recv)

    pass_on(wtree, w_slot, 0, ws_send, ws_recv)
    for j in R2:
        d_swap(j).wait()

    def spread(b, c):
        rows = pl.ds(pl.multiple_of(b * L, L), L)
        for m in R8:
            for t in R3:
                dqkv_nat[rows, t * D + m * L:t * D + (m + 1) * L] = gather_heads(lambda j, q: rd_ref[j, q, t], pos, b, m)
        return c

    def back(b, c):
        dg, db = c
        rows = pl.ds(pl.multiple_of(b * L, L), L)
        _, xhat, rstd = centre(x_ref[b])
        dh = None
        for t in R3:
            cur = dot_nt(dqkv_nat[rows, t * D:(t + 1) * D], w_flat[t * D:(t + 1) * D])
            dh = cur if dh is None else dh + cur
        dh = dh.astype(BF).astype(F32)
        dxh = dh * gamma
        m1 = jnp.mean(dxh, axis=-1, keepdims=True)
        m2 = jnp.mean(dxh * xhat, axis=-1, keepdims=True)
        dx_ref[b] = (dy_ref[b].astype(F32) + rstd * (dxh - m1 - xhat * m2)).astype(BF)
        return dg + jnp.sum(dh * xhat, axis=0, keepdims=True), db + jnp.sum(dh, axis=0, keepdims=True)

    lax.fori_loop(0, 4, spread, 0)
    for cp in w_loads:
        cp.wait()
    dgb = lax.fori_loop(0, 2, back, (jnp.zeros((1, D), F32), jnp.zeros((1, D), F32)))
    pass_on(gtree, g_slot, 0, gs_send, gs_recv)
    dg, db = lax.fori_loop(2, 4, back, dgb)
    dx_put.start()
    row = lax.broadcasted_iota(jnp.int32, (4, D), 0)
    sm_out[...] = jnp.where(row == 0, dg, jnp.where(row == 1, db, jnp.where(row == 2, dbo, 0.0)))
    sm_ref[pc.me] = sm_out[...]
    s_swap = Exchange(pc, lambda t: sm_out, lambda t: sm_ref.at[t], sm_ref.at[0:N - 1], s_send.at[0], s_recv.at[0])
    s_swap.start()
    pass_on(wtree, w_slot, 1, ws_send, ws_recv)
    pass_on(gtree, g_slot, 1, gs_send, gs_recv)
    s_swap.wait()
    tot = sm_ref[0]
    for n in range(1, N):
        tot = tot + sm_ref[n]
    small_ref[...] = tot
    pass_on(gtree, g_slot, 2, gs_send, gs_recv)
    pass_on(wtree, w_slot, 2, ws_send, ws_recv)
    for tree, at, got, send, recv in (
            (wtree, dwg_ref.at[:, pc.core], dwg_ref.at[:, 1 - pc.core], ws_send, ws_recv),
            (gtree, dwo_ref.at[pc.core], dwo_ref.at[1 - pc.core], gs_send, gs_recv)):
        rcopy(got, got, send.at[0], recv.at[0], pc.sib).wait_recv()
        rcopy(at, at, send.at[0], recv.at[0], pc.sib).wait_send()
        tree.finish()
    for j in R2:
        sib_copy(j).wait_send()
        o_swap(j).finish()
        d_swap(j).finish()
    s_swap.finish()
    half.wait_send()
    xp.wait_send()
    rcopy(acc_ref.at[0:7], acc_ref.at[0:7], r_send.at[0], r_recv.at[0], pc.sib).wait_send()
    for cp in (keep_w, keep_g, y_put, dx_put):
        cp.wait()


def layer_call(kind, x, dy, gamma, beta, bout, bqkv, wqkv, wout):
    vm, sm, hb = (pl.BlockSpec(memory_space=m) for m in (pltpu.VMEM, pltpu.SMEM, pl.ANY))
    sem = pltpu.SemaphoreType.DMA
    tok = jax.ShapeDtypeStruct((4, L, D), BF)

    def pair(*n):
        return [sem(n), sem(n)]

    def bf(*n):
        return pltpu.VMEM(n, BF)

    def ff(*n):
        return pltpu.VMEM(n, F32)

    band = 3 * QB
    return pl.pallas_call(
        layer_kernel,
        out_shape=(tok, tok, jax.ShapeDtypeStruct((4, D), F32), jax.ShapeDtypeStruct((8, 2, HR, W3), F32),
                   jax.ShapeDtypeStruct((2, 8, 64, D), F32)),
        in_specs=[sm, hb, hb] + [vm] * 4 + [hb, hb],
        out_specs=(hb, hb, vm, hb, hb),
        scratch_shapes=[bf(4, L, D)] * 4 + [
            bf(8, 2, QB, D), bf(2, L, D), bf(N, 64, D), bf(QB, D), bf(8, 4, L, L), bf(2, N, L, L), bf(D, W3), ff(8, W3),
            bf(S, W3), bf(S, W3), bf(L, S), bf(L, S), ff(L, S), ff(L, S),
            ff(QB, S), bf(QB, S), bf(QB, S), ff(QB, band), bf(QB, band), bf(QB, band),
            bf(2, N, L, L), bf(2, N, 3, L, L), bf(2, N, L, L), bf(2, N, 3, L, L), bf(T, D), bf(T, D3),
            ff(DR, W3), ff(HR, W3), ff(T, D), ff(T, D), ff(8, 64, D),
            ff(4, 64, D), ff(2, 64, D), ff(1, 64, D), ff(N, 4, D), ff(4, D), sem((6,))]
        + pair(4) + [sem((2,)), sem((2, 21))] + pair(2) + pair(2) + pair(2) + pair(1)
        + [sem((1,)), sem((21,))] + [sem((1,)), sem((21,))] + pair(1) + pair(1) + [sem((1,)), sem((9,)), sem((4,))],
        compiler_params=pltpu.CompilerParams(vmem_limit_bytes=VMEM_CAP, collective_id=0, has_side_effects=True),
        name="layer",
    )(kind, x, dy, gamma, beta, bout, bqkv, wqkv, wout)


def unpack_kernel(kind_ref, dw_hbm, dwo_hbm, y_in, dx_in, small_ref,
                  out_hbm, wo_hbm, y_out, dx_out, bias_ref, dg_ref, db_ref, dbo_ref,
                  in_ref, ob_ref, bias_in, wo_ref, y_ref, dx_ref, in_sem, out_sem, pass_in, pass_out):
    pos = head_places(kind_ref)

    def rows(r):
        return pl.ds(pl.multiple_of(r * 64, 64), 64)

    def load(r):
        return pltpu.make_async_copy(dw_hbm.at[:, rows(r)], in_ref.at[r], in_sem.at[r])

    def store(r):
        return pltpu.make_async_copy(ob_ref.at[r], out_hbm.at[rows(r)], out_sem.at[r])

    chain = ((dwo_hbm, wo_ref, wo_hbm), (y_in, y_ref, y_out), (dx_in, dx_ref, dx_out))

    def get(i):
        return pltpu.make_async_copy(chain[i][0], chain[i][1], pass_in.at[i])

    def put(i):
        return pltpu.make_async_copy(chain[i][1], chain[i][2], pass_out.at[i])

    bias_load = pltpu.make_async_copy(dw_hbm.at[:, D:D + 8], bias_in, pass_in.at[3])
    for r in R8:
        load(r).start()
    bias_load.start()

    def pick(read, t, m):
        pa, pb = pos[2 * m], pos[2 * m + 1]
        cols = slice(t * L, (t + 1) * L)
        a, b = read(pa % 8, cols), read(pb % 8, cols)
        lane = lax.broadcasted_iota(jnp.int32, a.shape, 1)
        a = jnp.where(pa // 8 == 1, pltpu.roll(a, 64, 1), a)
        b = jnp.where(pb // 8 == 0, pltpu.roll(b, 64, 1), b)
        return jnp.where(lane < 64, a, b)

    def step(r, c):
        load(r).wait()

        @pl.when(r < 8)
        def _():
            load(r + 8).start()

        @pl.when(r == 2)
        def _():
            for i in R3:
                get(i).start()

        @pl.when(r == 8)
        def _():
            for i in R3:
                get(i).wait()
                put(i).start()

        for t in R3:
            for m in R8:
                ob_ref[r, :, t * D + m * L:t * D + (m + 1) * L] = pick(lambda q, cols: in_ref[r, q, :, cols], t, m)
        store(r).start()
        return c

    lax.fori_loop(0, N, step, 0)
    bias_load.wait()
    for t in R3:
        for m in R8:
            bias_ref[t * D + m * L:t * D + (m + 1) * L] = pick(lambda q, cols: bias_in[q, :, cols], t, m)[0]
    for i, ref in enumerate((dg_ref, db_ref, dbo_ref)):
        ref[...] = small_ref[i]
    for r in range(N):
        store(r).wait()
    for i in R3:
        put(i).wait()


def unpack_call(kind, dwg, dwo, small, y, dx):
    vm, sm, hb = (pl.BlockSpec(memory_space=m) for m in (pltpu.VMEM, pltpu.SMEM, pl.ANY))
    sem = pltpu.SemaphoreType.DMA
    vec = jax.ShapeDtypeStruct((D,), F32)
    tok = jax.ShapeDtypeStruct((4, L, D), BF)
    return pl.pallas_call(
        unpack_kernel,
        in_specs=[sm, hb, hb, hb, hb, vm],
        out_specs=[hb, hb, hb, hb, vm, vm, vm, vm],
        out_shape=[jax.ShapeDtypeStruct((D, D3), F32), jax.ShapeDtypeStruct((D, D), F32), tok, tok,
                   jax.ShapeDtypeStruct((D3,), F32), vec, vec, vec],
        scratch_shapes=[
            pltpu.VMEM((N, 8, 64, W3), F32), pltpu.VMEM((N, 64, D3), F32), pltpu.VMEM((8, 8, W3), F32),
            pltpu.VMEM((D, D), F32), pltpu.VMEM((4, L, D), BF), pltpu.VMEM((4, L, D), BF),
            sem((N,)), sem((N,)), sem((4,)), sem((3,))],
        compiler_params=pltpu.CompilerParams(vmem_limit_bytes=VMEM_CAP),
        name="unpack",
    )(kind, dwg, dwo, y, dx, small)


def solution(mesh):
    tok_spec = P(None, "sp", None)

    def local_block(x, d_y, ln_gamma, ln_beta, w_qkv, b_qkv, w_out, b_out, head_kind):
        y, dx, small, dwg, dwo = layer_call(head_kind, x, d_y, ln_gamma, ln_beta, b_out, b_qkv, w_qkv, w_out.reshape(N, 64, D))
        dw, dwout, y, dx, dbias, dg, db, dbo = unpack_call(
            head_kind, dwg.reshape(8, DR, W3), dwo.reshape(D, D), small, y, dx)
        return y, dx, dg, db, dw, dbias, dwout, dbo

    return jax.shard_map(
        local_block, mesh=mesh,
        in_specs=(tok_spec, tok_spec, P(), P(), P(), P(), P(), P(), P()),
        out_specs=(tok_spec, tok_spec, P(), P(), P(), P(), P(), P()), check_vma=False)
```

```python
import functools
import math

import jax
import jax.numpy as jnp
from jax import lax
from jax.experimental import pallas as pl
from jax.experimental.pallas import tpu as pltpu
from jax.sharding import PartitionSpec as P

LN_EPS = 1e-5
NEG_BIG = -1e30
BF = jnp.bfloat16
F32 = jnp.float32
QB = 256
L = 128
W3 = 384
T = 512
D = 1024
DR = 1040
HR = 520
N = 16
R2, R3, R4, R8 = range(2), range(3), range(4), range(8)
MESH = pl.DeviceIdType.MESH
H_ROWS = (0, 96, 176, 256)
W_ROWS = (0, 176, 352, 520)
O_ROWS = (0, 24, 48, 64)
S = 2048
D3 = 3072
VMEM_CAP = 63 * D * D


def dot_nn(a, b):
    return lax.dot_general(a, b, (((1,), (0,)), ((), ())), preferred_element_type=F32)


def dot_nt(a, b):
    return lax.dot_general(a, b, (((1,), (1,)), ((), ())), preferred_element_type=F32)


def dot_tn(a, b):
    return lax.dot_general(a, b, (((0,), (0,)), ((), ())), preferred_element_type=F32)


def swap_halves(a):
    return jnp.concatenate([a[:, 64:], a[:, :64]], axis=1)


def pair_halves(a, a_half, b, b_half):
    lane = lax.broadcasted_iota(jnp.int32, a.shape, 1)
    a = jnp.where(a_half == 1, swap_halves(a), a)
    b = jnp.where(b_half == 0, swap_halves(b), b)
    return jnp.where(lane < 64, a, b)


class Place:
    def __init__(self):
        self.me = lax.axis_index("sp")
        self.core, self.chip = self.me % 2, self.me // 2
        self.sib = self.me + 1 - 2 * self.core
        bits = (self.chip % 2, self.chip // 2 % 2, self.chip // 4)
        self.step = [(1 - 2 * v) * w for v, w in zip(bits, (1, 2, 4))]

    def chip_at(self, axes):
        out = self.chip
        for a in axes:
            out = out + self.step[a]
        return out

    def next_dev(self, axis):
        return self.me + 2 * self.step[axis]


def rcopy(src, dst, send, recv, dev):
    return pltpu.make_async_remote_copy(
        src_ref=src, dst_ref=dst, send_sem=send, recv_sem=recv, device_id=(dev,), device_id_type=MESH)


def subsets(axes):
    out = [()]
    for a in axes:
        out += [v + (a,) for v in out]
    return out


class Tree:
    def __init__(self, place, own, slot, seven, send, recv):
        self.place, self.own, self.slot, self.seven, self.send, self.recv = place, own, slot, seven, send, recv
        self.entries = []
        for s in R3:
            for p in R3:
                order = [(p + j) % 3 for j in R3]
                for sub in subsets(order[:s]):
                    self.entries.append((p, order[s], sub))

    def copy(self, e):
        p, axis, sub = e
        i = self.entries.index(e)
        at = self.slot(self.place.chip_at(sub), p)
        return rcopy(at if sub else self.own(p), at, self.send, self.recv.at[i], self.place.next_dev(axis))

    def start_own(self, levels=R3):
        for e in self.hops(0):
            if (e[1] - e[0]) % 3 in levels:
                self.copy(e).start()

    def arrive(self, e):
        p, axis, sub = e
        got = sub + (axis,)
        chip = self.place.chip_at(got)
        at = self.slot(chip, p)
        i = self.entries.index(e)
        rcopy(at, at, self.send, self.recv.at[i], self.place.next_dev(axis)).wait_recv()
        for n in self.entries:
            if n[0] == p and n[2] == got:
                self.copy(n).start()
        return chip, p

    def hops(self, n):
        return [e for e in self.entries if len(e[2]) == n]

    def finish(self):
        rcopy(self.seven, self.seven, self.send, self.recv.at[0], self.place.me).wait_send()


def barrier_signal(place):
    sem = pltpu.get_barrier_semaphore()
    for r in range(1, N):
        pl.semaphore_signal(sem, inc=1, device_id=((place.me + r) % N,), device_id_type=MESH)


def barrier_wait():
    pl.semaphore_wait(pltpu.get_barrier_semaphore(), N - 1)


def head_places(kind_ref):
    pos, zeros, ones = [], 0, 8
    for n in range(N):
        k = kind_ref[n]
        pos.append(jnp.where(k == 0, zeros, ones))
        zeros, ones = zeros + 1 - k, ones + k
    return pos


class Exchange:
    def __init__(self, place, src, dst, rest, send, recv):
        self.place, self.src, self.dst, self.send, self.recv = place, src, dst, send, recv
        self.rest = rest

    def start(self, first=1, end=N):
        me = self.place.me
        for r in range(first, end):
            to = (me + r) % N
            rcopy(self.src(to), self.dst(me), self.send, self.recv, to).start()

    def start_half(self, upper):
        me = self.place.me
        for r in range(1, N):
            to = (me + r) % N

            @pl.when(to // 8 == upper)
            def _():
                rcopy(self.src(to), self.dst(me), self.send, self.recv, to).start()

    def wait(self):
        rcopy(self.rest, self.rest, self.send, self.recv, self.place.me).wait_recv()

    def finish(self):
        rcopy(self.rest, self.rest, self.send, self.recv, self.place.me).wait_send()


def gather_heads(recv_at, pos, b, m):
    pa, pb = pos[2 * m], pos[2 * m + 1]
    k, j = b // 2, b % 2
    a = recv_at(j, 2 * (pa % 8) + k)
    c = recv_at(j, 2 * (pb % 8) + k)
    return pair_halves(a, pa // 8, c, pb // 8)


def span(tab):
    return lambda p: pl.ds(tab[p], tab[p + 1] - tab[p])


def centre(xb):
    xf = xb.astype(F32)
    cen = xf - jnp.mean(xf, axis=-1, keepdims=True)
    rstd = lax.rsqrt(jnp.mean(cen * cen, axis=-1, keepdims=True) + LN_EPS)
    return xf, cen * rstd, rstd


def layer_kernel(kind_ref, x_hbm, dy_hbm, gamma_ref, beta_ref, bout_ref, bqkv_ref, wqkv_hbm, wout_hbm,
                 y_hbm, dx_hbm, small_ref, dwg_ref, dwo_ref, x_ref, dy_ref, y_ref, dx_ref,
                 hg_ref, out_ref, wout_ref, wp_ref, do_ref, dog_ref, w_ref, bias_ref, qkv_ref, dqkv_ref, qt_ref, dot_ref,
                 dkt_ref, dvt_ref, s_f, p_f, ds_f, s_g, p_g, ds_g, so_ref, sd_ref, ro_ref, rd_ref, o_nat, dqkv_nat,
                 dwp_ref, dws_ref, part_ref, px_ref, acc_ref, rs0_ref, rs1_ref, rs2_ref, sm_ref, sm_out,
                 loc, sib_send, sib_recv, h_send, h_recv, do_send, do_recv, o_send, o_recv, d_send, d_recv,
                 s_send, s_recv, w_send, w_recv, g_send, g_recv, ws_send, ws_recv, gs_send, gs_recv, r_send, r_recv, io_sem):
    pc = Place()
    barrier_signal(pc)

    def w_load(r):
        return pltpu.make_async_copy(wqkv_hbm.at[r * T:(r + 1) * T], dqkv_nat, loc.at[r])

    wo_load = pltpu.make_async_copy(wout_hbm, wout_ref, loc.at[2])
    x_load, dy_load, y_put, dx_put = [
        pltpu.make_async_copy(a, b, io_sem.at[i]) for i, (a, b) in enumerate(
            ((x_hbm, x_ref), (dy_hbm, dy_ref), (y_ref, y_hbm), (dx_ref, dx_hbm)))]
    x_load.start()
    dy_load.start()
    w_load(0).start()
    wo_load.start()
    gamma = gamma_ref[...].reshape(1, D).astype(F32)
    beta = beta_ref[...].reshape(1, D).astype(F32)
    bout = bout_ref[...].reshape(1, D).astype(F32)
    bqkv = bqkv_ref[...].reshape(1, D3).astype(F32)

    def rows_of(core):
        return pl.ds(pl.multiple_of(core * L, L), L)

    def norm(xb):
        return (centre(xb)[1] * gamma + beta).astype(BF)

    def sib_copy(j):
        return rcopy(out_ref.at[j], hg_ref.at[pc.chip, j, rows_of(pc.core)], sib_send.at[j], sib_recv.at[j], pc.sib)

    x_load.wait()
    for j in R2:
        out_ref[j] = norm(x_ref[2 * (1 - pc.core) + j])
    for j in R2:
        hg_ref[pc.chip, j, rows_of(pc.core)] = norm(x_ref[2 * pc.core + j])
    barrier_wait()
    for j in R2:
        sib_copy(j).start()

    h_rows, w_rows, o_rows = span(H_ROWS), span(W_ROWS), span(O_ROWS)

    def h_tree(j):
        slot = lambda c, p: hg_ref.at[c, j, h_rows(p)]
        return Tree(pc, lambda p: slot(pc.chip, p), slot, hg_ref.at[0:7, j], h_send.at[j], h_recv.at[j])

    def sib_arrive(j):
        at = hg_ref.at[pc.chip, j, rows_of(1 - pc.core)]
        rcopy(at, at, sib_send.at[j], sib_recv.at[j], pc.sib).wait_recv()

    do_out = do_ref.reshape(N, 2, L, L)

    def swap(src, dst, send, recv, j):
        return Exchange(pc, lambda t: src(t, j), lambda t: dst.at[j, t], dst.at[j, 0:N - 1], send.at[j], recv.at[j])

    def do_swap(j):
        return swap(lambda t, j: do_out.at[t, j], dog_ref, do_send, do_recv, j)

    def o_swap(j):
        return swap(lambda t, j: so_ref.at[j, t], ro_ref, o_send, o_recv, j)

    def d_swap(j):
        return swap(lambda t, j: sd_ref.at[j, t], rd_ref, d_send, d_recv, j)

    trees = [h_tree(0), h_tree(1)]
    sib_arrive(0)
    trees[0].start_own()
    pos = head_places(kind_ref)
    perm = []
    for j in range(N):
        v = 0
        for n in range(1, N):
            v = v + jnp.where(pos[n] == j, n, 0)
        perm.append(v)
    f = g = 0
    for c in R8:
        f = f + jnp.where(pc.chip == c, perm[c], 0)
        g = g + jnp.where(pc.chip == c, perm[8 + c], 0)
    wo_load.wait()
    dy_load.wait()
    dy_all = dy_ref[...].reshape(T, D)
    for c in R4:
        for u in R2:
            wp_ref[u * L:u * L + 64] = wout_ref[perm[2 * c + u]]
            wp_ref[u * L + 64:u * L + L] = wout_ref[perm[8 + 2 * c + u]]
        d = dot_nt(dy_all, wp_ref[...]).astype(BF)
        for u in R2:
            do_ref[2 * c + u] = d[:, u * L:(u + 1) * L].reshape(4, L, L)
    for e in trees[0].hops(0):
        trees[0].arrive(e)
    do_swap(0).start()
    for j in R2:
        dog_ref[j, pc.me] = do_out[pc.me, j]

    def w_cols(t, k, head):
        out = None
        for m in R8:
            cur = dqkv_nat[k * L:(k + 1) * L, t * D + m * L:t * D + (m + 1) * L]
            out = cur if out is None else jnp.where(head // 2 == m, cur, out)
        return out

    for r in R2:
        w_load(r).wait()
        for t in R3:
            for k in R4:
                w_ref[r * T + k * L:r * T + (k + 1) * L, t * L:(t + 1) * L] = pair_halves(
                    w_cols(t, k, f), f % 2, w_cols(t, k, g), g % 2)
        if r == 0:
            w_load(1).start()
    for t in R3:
        halves = []
        for head in (f, g):
            out = None
            for m in R8:
                cur = bqkv[:, t * D + m * L:t * D + (m + 1) * L]
                out = cur if out is None else jnp.where(head // 2 == m, cur, out)
            halves += [out, head % 2]
        bias_ref[:, t * L:(t + 1) * L] = jnp.broadcast_to(pair_halves(*halves), (8, L))
    dwp_ref[...] = jnp.zeros_like(dwp_ref)
    for e in trees[0].hops(1):
        trees[0].arrive(e)
    sib_arrive(1)
    trees[1].start_own()

    lane = lax.broadcasted_iota(jnp.int32, (QB, L), 1)
    row_i = lax.broadcasted_iota(jnp.int32, (QB, QB), 0)
    col_i = lax.broadcasted_iota(jnp.int32, (QB, QB), 1)

    def head_block(j, i, hd):
        s_ref, p_ref, ds_ref = ((s_f, p_f, ds_f), (s_g, p_g, ds_g))[hd]
        first = 0 if hd == 0 else max(0, i - 2)
        blocks = range(first, i + 1)
        mine = (lane < 64) if hd == 0 else (lane >= 64)
        qi = qkv_ref[i * QB:(i + 1) * QB, 0:L] * BF(0.125)
        doi = dog_ref[j, 2 * i:2 * i + 2].reshape(QB, L)
        qm = jnp.where(mine, qi, BF(0))
        dom = jnp.where(mine, doi, BF(0))
        k_at = lambda kb: qkv_ref[kb * QB:(kb + 1) * QB, L:2 * L]
        v_at = lambda kb: qkv_ref[kb * QB:(kb + 1) * QB, 2 * L:3 * L]
        at = lambda kb: slice((kb - first) * QB, (kb - first + 1) * QB)
        mx = None
        for kb in blocks:
            s = dot_nt(qm, k_at(kb))
            if kb == i:
                s = jnp.where(col_i <= row_i, s, NEG_BIG)
            if hd == 1 and kb == i - 2:
                s = jnp.where(col_i > row_i, s, NEG_BIG)
            s_ref[:, at(kb)] = s
            cur = jnp.maximum(s[:, :L], s[:, L:])
            mx = cur if mx is None else jnp.maximum(mx, cur)
        m = jnp.max(mx, axis=1, keepdims=True)
        ls = None
        for kb in blocks:
            e = jnp.exp(s_ref[:, at(kb)] - m)
            s_ref[:, at(kb)] = e
            cur = e[:, :L] + e[:, L:]
            ls = cur if ls is None else ls + cur
        rl = 1.0 / jnp.sum(ls, axis=1, keepdims=True)
        acc = None
        for kb in blocks:
            p_ = s_ref[:, at(kb)] * rl
            s_ref[:, at(kb)] = p_
            pb = p_.astype(BF)
            p_ref[:, at(kb)] = pb
            cur = dot_nn(pb, v_at(kb))
            acc = cur if acc is None else acc + cur
        dsum = jnp.sum(dom.astype(F32) * acc, axis=1, keepdims=True)
        dq = None
        for kb in blocks:
            dp = dot_nt(dom, v_at(kb)).astype(BF).astype(F32)
            ds = (s_ref[:, at(kb)] * (dp - dsum)).astype(BF)
            ds_ref[:, at(kb)] = ds
            cur = dot_nn(ds, k_at(kb))
            dq = cur if dq is None else dq + cur
        hr = slice(hd * 64, hd * 64 + 64)
        n = len(blocks) * QB
        keys = slice(first * QB, first * QB + n)
        dvt_ref[hr, keys] += dot_nn(dot_ref[hr, i * QB:(i + 1) * QB], p_ref[:, :n])
        dkt_ref[hr, keys] += dot_nn(qt_ref[hr, i * QB:(i + 1) * QB], ds_ref[:, :n])
        return acc, dq * 0.125

    def batch_step(j, carry):
        last = h_tree(j)
        for e in last.hops(2):
            last.arrive(e)
        do_swap(j).wait()

        @pl.when(j == 1)
        def _():
            o_swap(0).start()
            d_swap(0).start()

        def qkv_step(r, c):
            rows = hg_ref[pl.ds(2 * r, 2), j].reshape(T, D)
            out = dot_nn(rows, w_ref[...]) + bias_ref[0:1, :]
            qkv_ref[pl.ds(pl.multiple_of(r * T, T), T), :] = out.astype(BF)
            return c

        lax.fori_loop(0, 4, qkv_step, 0)

        for i in R8:
            qs = qkv_ref[i * QB:(i + 1) * QB, 0:L] * BF(0.125)
            qt_ref[:, i * QB:(i + 1) * QB] = qs.T
            dot_ref[:, i * QB:(i + 1) * QB] = dog_ref[j, 2 * i:2 * i + 2].reshape(QB, L).T
        dkt_ref[...] = jnp.zeros_like(dkt_ref)
        dvt_ref[...] = jnp.zeros_like(dvt_ref)
        for i in R8:
            of, dqf = head_block(j, i, 0)
            og, dqg = head_block(j, i, 1)
            o = jnp.where(lane < 64, of, og).astype(BF)
            dq = jnp.where(lane < 64, dqf, dqg).astype(BF)
            for u in R2:
                so_ref[j, 2 * i + u] = o[u * L:(u + 1) * L]
                sd_ref[j, 2 * i + u, 0] = dq[u * L:(u + 1) * L]
            dqkv_ref[i * QB:(i + 1) * QB, 0:L] = dq
            if i == 3:
                @pl.when(j == 0)
                def _():
                    for e in trees[1].hops(0):
                        trees[1].arrive(e)
                    do_swap(1).start()

                @pl.when(j == 1)
                def _():
                    o_swap(1).start_half(0)

        for t, src in ((1, dkt_ref), (2, dvt_ref)):
            for n in range(N):
                d = src[:, n * L:(n + 1) * L].T.astype(BF)
                sd_ref[j, n, t] = d
                dqkv_ref[n * L:(n + 1) * L, t * L:(t + 1) * L] = d
        ro_ref[j, pc.me] = so_ref[j, pc.me]
        rd_ref[j, pc.me] = sd_ref[j, pc.me]

        @pl.when(j == 1)
        def _():
            o_swap(1).start_half(1)

        def dw_step(r, c):
            cols = pl.ds(pl.multiple_of(r * QB, QB), QB)
            dwp_ref[cols, :] += dot_tn(hg_ref[:, j, :, cols].reshape(S, QB), dqkv_ref[...])
            return c

        lax.fori_loop(0, 4, dw_step, 0)

        @pl.when(j == 0)
        def _():
            for e in trees[1].hops(1):
                trees[1].arrive(e)

        dwp_ref[D:D + 1, :] += jnp.sum(dqkv_ref[...].astype(F32), axis=0, keepdims=True)
        return carry

    lax.fori_loop(0, 2, batch_step, 0)

    def half_of(core):
        return dwp_ref.at[pl.ds(pl.multiple_of(core * HR, 8), HR)]

    def to_sib(n, src, dst, send, recv):
        cp = rcopy(src, dst, send.at[n], recv.at[n], pc.sib)
        cp.start()
        return cp

    half = to_sib(2, half_of(1 - pc.core), dws_ref, sib_send, sib_recv)
    for j in R2:
        trees[j].finish()
        do_swap(j).finish()
    w_flat = hg_ref.reshape(2 * S, D)
    w_loads = [pltpu.make_async_copy(wqkv_hbm.at[:, t * D:(t + 1) * D], w_flat.at[t * D:(t + 1) * D], loc.at[3 + t]) for t in R3]
    for cp in w_loads:
        cp.start()
    half.wait_recv()
    dws_ref[...] += half_of(pc.core)[...]

    def w_slot(c, p, core=pc.core):
        return dwg_ref.at[c, core, w_rows(p)]

    def g_slot(c, p, core=pc.core):
        return dwo_ref.at[core, c, o_rows(p)]

    wtree = Tree(pc, lambda p: dws_ref.at[w_rows(p)], w_slot, dwg_ref.at[0:7, pc.core], w_send.at[0], w_recv)
    wtree.start_own((0,))
    keep_w = pltpu.make_async_copy(dws_ref, dwg_ref.at[pc.chip, pc.core], loc.at[0])
    keep_w.start()
    for p in R3:
        to_sib(0, dws_ref.at[w_rows(p)], w_slot(pc.chip, p), ws_send, ws_recv)

    for j in R2:
        o_swap(j).wait()
    for b in R4:
        for m in R8:
            o_nat[b * L:(b + 1) * L, m * L:(m + 1) * L] = gather_heads(lambda j, q: ro_ref[j, q], pos, b, m)

    def wout_part(core, c):
        cols = pl.ds(pl.multiple_of(core * T + c * QB, QB), QB)
        return dot_tn(o_nat[:, cols], dy_all)

    for c in R2:
        part_ref[c * QB:(c + 1) * QB] = wout_part(1 - pc.core, c)
    xp = to_sib(3, part_ref, px_ref, sib_send, sib_recv)
    for c in R2:
        acc_ref[4 * c:4 * c + 4] = wout_part(pc.core, c).reshape(4, 64, D)
    xp.wait_recv()
    acc_ref[...] += px_ref[...].reshape(8, 64, D)

    bufs = (rs0_ref, rs1_ref, rs2_ref)

    def reduce_step(s, wait):
        for p in R3:
            order = [(p + j) % 3 for j in R3]
            if wait:
                at = bufs[s].at[:, o_rows(p)]
                rcopy(at, at, r_send.at[0], r_recv.at[s * 3 + p], pc.sib).wait_recv()
            for i, sub in enumerate(subsets(order[s + 1:])):
                if wait:
                    acc_ref[pc.chip_at(sub), o_rows(p)] += bufs[s][i, o_rows(p)]
                else:
                    rcopy(acc_ref.at[pc.chip_at((order[s],) + sub), o_rows(p)], bufs[s].at[i, o_rows(p)],
                          r_send.at[0], r_recv.at[s * 3 + p], pc.next_dev(order[s])).start()

    reduce_step(0, False)
    wtree.start_own((1, 2))
    def pass_on(tree, slot, n, send, recv):
        for e in tree.hops(n):
            c, p = tree.arrive(e)
            to_sib(0, slot(c, p), slot(c, p), send, recv)

    dbo = jnp.zeros((1, D), F32)
    for b in R4:
        rows = slice(b * L, (b + 1) * L)
        y_ref[b] = (x_ref[b].astype(F32) + dot_nn(o_nat[rows], wout_ref.reshape(D, D)[...]) + bout).astype(BF)
        dbo += jnp.sum(dy_ref[b].astype(F32), axis=0, keepdims=True)
    y_put.start()
    reduce_step(0, True)
    reduce_step(1, False)
    d_swap(1).start(1, 9)
    reduce_step(1, True)
    reduce_step(2, False)
    d_swap(1).start(9)
    reduce_step(2, True)
    gtree = Tree(pc, lambda p: acc_ref.at[pc.chip, o_rows(p)], g_slot, dwo_ref.at[pc.core, 0:7], g_send.at[0], g_recv)
    gtree.start_own()
    keep_g = pltpu.make_async_copy(acc_ref.at[pc.chip], dwo_ref.at[pc.core, pc.chip], loc.at[1])
    keep_g.start()
    for p in R3:
        to_sib(0, acc_ref.at[pc.chip, o_rows(p)], g_slot(pc.chip, p), gs_send, gs_recv)

    pass_on(wtree, w_slot, 0, ws_send, ws_recv)
    for j in R2:
        d_swap(j).wait()

    def spread(b, c):
        rows = pl.ds(pl.multiple_of(b * L, L), L)
        for m in R8:
            for t in R3:
                dqkv_nat[rows, t * D + m * L:t * D + (m + 1) * L] = gather_heads(lambda j, q: rd_ref[j, q, t], pos, b, m)
        return c

    def back(b, c):
        dg, db = c
        rows = pl.ds(pl.multiple_of(b * L, L), L)
        _, xhat, rstd = centre(x_ref[b])
        dh = None
        for t in R3:
            cur = dot_nt(dqkv_nat[rows, t * D:(t + 1) * D], w_flat[t * D:(t + 1) * D])
            dh = cur if dh is None else dh + cur
        dh = dh.astype(BF).astype(F32)
        dxh = dh * gamma
        m1 = jnp.mean(dxh, axis=-1, keepdims=True)
        m2 = jnp.mean(dxh * xhat, axis=-1, keepdims=True)
        dx_ref[b] = (dy_ref[b].astype(F32) + rstd * (dxh - m1 - xhat * m2)).astype(BF)
        return dg + jnp.sum(dh * xhat, axis=0, keepdims=True), db + jnp.sum(dh, axis=0, keepdims=True)

    lax.fori_loop(0, 4, spread, 0)
    for cp in w_loads:
        cp.wait()
    dgb = lax.fori_loop(0, 2, back, (jnp.zeros((1, D), F32), jnp.zeros((1, D), F32)))
    pass_on(gtree, g_slot, 0, gs_send, gs_recv)
    dg, db = lax.fori_loop(2, 4, back, dgb)
    dx_put.start()
    row = lax.broadcasted_iota(jnp.int32, (4, D), 0)
    sm_out[...] = jnp.where(row == 0, dg, jnp.where(row == 1, db, jnp.where(row == 2, dbo, 0.0)))
    sm_ref[pc.me] = sm_out[...]
    s_swap = Exchange(pc, lambda t: sm_out, lambda t: sm_ref.at[t], sm_ref.at[0:N - 1], s_send.at[0], s_recv.at[0])
    s_swap.start()
    pass_on(wtree, w_slot, 1, ws_send, ws_recv)
    pass_on(gtree, g_slot, 1, gs_send, gs_recv)
    s_swap.wait()
    tot = sm_ref[0]
    for n in range(1, N):
        tot = tot + sm_ref[n]
    small_ref[...] = tot
    pass_on(gtree, g_slot, 2, gs_send, gs_recv)
    pass_on(wtree, w_slot, 2, ws_send, ws_recv)
    for tree, at, got, send, recv in (
            (wtree, dwg_ref.at[:, pc.core], dwg_ref.at[:, 1 - pc.core], ws_send, ws_recv),
            (gtree, dwo_ref.at[pc.core], dwo_ref.at[1 - pc.core], gs_send, gs_recv)):
        rcopy(got, got, send.at[0], recv.at[0], pc.sib).wait_recv()
        rcopy(at, at, send.at[0], recv.at[0], pc.sib).wait_send()
        tree.finish()
    for j in R2:
        sib_copy(j).wait_send()
        o_swap(j).finish()
        d_swap(j).finish()
    s_swap.finish()
    half.wait_send()
    xp.wait_send()
    rcopy(acc_ref.at[0:7], acc_ref.at[0:7], r_send.at[0], r_recv.at[0], pc.sib).wait_send()
    for cp in (keep_w, keep_g, y_put, dx_put):
        cp.wait()


def layer_call(kind, x, dy, gamma, beta, bout, bqkv, wqkv, wout):
    vm, sm, hb = (pl.BlockSpec(memory_space=m) for m in (pltpu.VMEM, pltpu.SMEM, pl.ANY))
    sem = pltpu.SemaphoreType.DMA
    tok = jax.ShapeDtypeStruct((4, L, D), BF)

    def pair(*n):
        return [sem(n), sem(n)]

    def bf(*n):
        return pltpu.VMEM(n, BF)

    def ff(*n):
        return pltpu.VMEM(n, F32)

    band = 3 * QB
    return pl.pallas_call(
        layer_kernel,
        out_shape=(tok, tok, jax.ShapeDtypeStruct((4, D), F32), jax.ShapeDtypeStruct((8, 2, HR, W3), F32),
                   jax.ShapeDtypeStruct((2, 8, 64, D), F32)),
        in_specs=[sm, hb, hb] + [vm] * 4 + [hb, hb],
        out_specs=(hb, hb, vm, hb, hb),
        scratch_shapes=[bf(4, L, D)] * 4 + [
            bf(8, 2, QB, D), bf(2, L, D), bf(N, 64, D), bf(QB, D), bf(8, 4, L, L), bf(2, N, L, L), bf(D, W3), ff(8, W3),
            bf(S, W3), bf(S, W3), bf(L, S), bf(L, S), ff(L, S), ff(L, S),
            ff(QB, S), bf(QB, S), bf(QB, S), ff(QB, band), bf(QB, band), bf(QB, band),
            bf(2, N, L, L), bf(2, N, 3, L, L), bf(2, N, L, L), bf(2, N, 3, L, L), bf(T, D), bf(T, D3),
            ff(DR, W3), ff(HR, W3), ff(T, D), ff(T, D), ff(8, 64, D),
            ff(4, 64, D), ff(2, 64, D), ff(1, 64, D), ff(N, 4, D), ff(4, D), sem((6,))]
        + pair(4) + [sem((2,)), sem((2, 21))] + pair(2) + pair(2) + pair(2) + pair(1)
        + [sem((1,)), sem((21,))] + [sem((1,)), sem((21,))] + pair(1) + pair(1) + [sem((1,)), sem((9,)), sem((4,))],
        compiler_params=pltpu.CompilerParams(vmem_limit_bytes=VMEM_CAP, collective_id=0, has_side_effects=True),
        name="layer",
    )(kind, x, dy, gamma, beta, bout, bqkv, wqkv, wout)


def unpack_kernel(kind_ref, dw_hbm, dwo_hbm, y_in, dx_in, small_ref,
                  out_hbm, wo_hbm, y_out, dx_out, bias_ref, dg_ref, db_ref, dbo_ref,
                  in_ref, ob_ref, bias_in, wo_ref, y_ref, dx_ref, in_sem, out_sem, pass_in, pass_out):
    pos = head_places(kind_ref)

    def rows(r):
        return pl.ds(pl.multiple_of(r * 64, 64), 64)

    def load(r):
        return pltpu.make_async_copy(dw_hbm.at[:, rows(r)], in_ref.at[r], in_sem.at[r])

    def store(r):
        return pltpu.make_async_copy(ob_ref.at[r], out_hbm.at[rows(r)], out_sem.at[r])

    chain = ((dwo_hbm, wo_ref, wo_hbm), (y_in, y_ref, y_out), (dx_in, dx_ref, dx_out))

    def get(i):
        return pltpu.make_async_copy(chain[i][0], chain[i][1], pass_in.at[i])

    def put(i):
        return pltpu.make_async_copy(chain[i][1], chain[i][2], pass_out.at[i])

    bias_load = pltpu.make_async_copy(dw_hbm.at[:, D:D + 8], bias_in, pass_in.at[3])
    for r in R8:
        load(r).start()
    bias_load.start()

    def pick(read, t, m):
        pa, pb = pos[2 * m], pos[2 * m + 1]
        cols = slice(t * L, (t + 1) * L)
        a, b = read(pa % 8, cols), read(pb % 8, cols)
        lane = lax.broadcasted_iota(jnp.int32, a.shape, 1)
        a = jnp.where(pa // 8 == 1, pltpu.roll(a, 64, 1), a)
        b = jnp.where(pb // 8 == 0, pltpu.roll(b, 64, 1), b)
        return jnp.where(lane < 64, a, b)

    def step(r, c):
        load(r).wait()

        @pl.when(r < 8)
        def _():
            load(r + 8).start()

        @pl.when(r == 2)
        def _():
            for i in R3:
                get(i).start()

        @pl.when(r == 8)
        def _():
            for i in R3:
                get(i).wait()
                put(i).start()

        for t in R3:
            for m in R8:
                ob_ref[r, :, t * D + m * L:t * D + (m + 1) * L] = pick(lambda q, cols: in_ref[r, q, :, cols], t, m)
        store(r).start()
        return c

    lax.fori_loop(0, N, step, 0)
    bias_load.wait()
    for t in R3:
        for m in R8:
            bias_ref[t * D + m * L:t * D + (m + 1) * L] = pick(lambda q, cols: bias_in[q, :, cols], t, m)[0]
    for i, ref in enumerate((dg_ref, db_ref, dbo_ref)):
        ref[...] = small_ref[i]
    for r in range(N):
        store(r).wait()
    for i in R3:
        put(i).wait()


def unpack_call(kind, dwg, dwo, small, y, dx):
    vm, sm, hb = (pl.BlockSpec(memory_space=m) for m in (pltpu.VMEM, pltpu.SMEM, pl.ANY))
    sem = pltpu.SemaphoreType.DMA
    vec = jax.ShapeDtypeStruct((D,), F32)
    tok = jax.ShapeDtypeStruct((4, L, D), BF)
    return pl.pallas_call(
        unpack_kernel,
        in_specs=[sm, hb, hb, hb, hb, vm],
        out_specs=[hb, hb, hb, hb, vm, vm, vm, vm],
        out_shape=[jax.ShapeDtypeStruct((D, D3), F32), jax.ShapeDtypeStruct((D, D), F32), tok, tok,
                   jax.ShapeDtypeStruct((D3,), F32), vec, vec, vec],
        scratch_shapes=[
            pltpu.VMEM((N, 8, 64, W3), F32), pltpu.VMEM((N, 64, D3), F32), pltpu.VMEM((8, 8, W3), F32),
            pltpu.VMEM((D, D), F32), pltpu.VMEM((4, L, D), BF), pltpu.VMEM((4, L, D), BF),
            sem((N,)), sem((N,)), sem((4,)), sem((3,))],
        compiler_params=pltpu.CompilerParams(vmem_limit_bytes=VMEM_CAP),
        name="unpack",
    )(kind, dwg, dwo, y, dx, small)


def solution(mesh):
    tok_spec = P(None, "sp", None)

    def local_block(x, d_y, ln_gamma, ln_beta, w_qkv, b_qkv, w_out, b_out, head_kind):
        y, dx, small, dwg, dwo = layer_call(head_kind, x, d_y, ln_gamma, ln_beta, b_out, b_qkv, w_qkv, w_out.reshape(N, 64, D))
        dw, dwout, y, dx, dbias, dg, db, dbo = unpack_call(
            head_kind, dwg.reshape(8, DR, W3), dwo.reshape(D, D), small, y, dx)
        return y, dx, dg, db, dw, dbias, dwout, dbo

    return jax.shard_map(
        local_block, mesh=mesh,
        in_specs=(tok_spec, tok_spec, P(), P(), P(), P(), P(), P(), P()),
        out_specs=(tok_spec, tok_spec, P(), P(), P(), P(), P(), P()), check_vma=False)
```
